512 devices in a mesh: mem: 16 (over z, core), tile: 32 (over y, x).
Axes of the slice: x: 4, y: 8, z: 8, core: 2. Of those that a mesh axis runs over, the one named last changes fastest.
Arguments:
- ensemble: float32 [512, 4, 1024, 128], P('mem', None, 'tile'), may hold values from -16 to 16
- diffusion: float32 [4, 1024, 128], P(None, 'tile'), may hold values from 0.04 to 0.12
- obs_cells: int32 [32, 16, 512], P('tile', 'mem'), may hold values from 0 to 3071
- obs_values: float32 [32, 16, 512], P('tile', 'mem'), may hold values from -6 to 6
- obs_weights: float32 [32, 16, 512], P('tile', 'mem'), may hold values from 12 to 36
Outputs:
- analysis: float32 [512, 4, 1024, 128], P('mem', None, 'tile')
The draws below stay inside these ranges and needn't reach their ends.
Inputs may be any that keep to these rules, and one draw needn't show every extreme that they name: `obs_cells`: index e below 1024 is cell e of the patch before (mem index minus one, cyclically, same tile); then come the patch's own 1024 cells, then those of the patch after.
All inputs are finite; a program needn't handle non-finite values.
Results may differ from the reference program's by a relative error of at most 0.019.
The reference program's roundings to bfloat16 on the way (of `background`, `predicted`, `wtotal` and `xpert`) count: a program that leaves them out, or rounds other values in their place, can miss the bound.
Values may be sent and summed in bfloat16 or wider, within the bound.
A program may use at most 64 MiB of HBM per device.

```python
import math
import jax
import jax.numpy as jnp
from jax import lax

K = 512
LEV = 4
NY = 128
PATCH = 1024
NOBS = 512
ITERS = 6
SUB = 3
CX = 32
NX = 1024
TILES = 32
SHARES = 16
N_MEM = 16
N_TILE = 32


def draw_ensemble(key, part):
    shape = (K, LEV, NX, NY)
    common_key = jax.random.fold_in(key, 17)
    member_key = jax.random.fold_in(key, 29)
    common = 4.0 * jax.random.normal(common_key, (1, LEV, NX, NY), jnp.float32)
    spread = 3.0 * jax.random.normal(member_key, shape, jnp.float32)
    return jnp.clip(common + spread, -16.0, 16.0)


def set_ends(entries, stream_key, least, largest):
    spot = [jax.random.randint(jax.random.fold_in(stream_key, axis), (), 0, length) for axis, length in enumerate(entries.shape)]
    longest = entries.shape.index(max(entries.shape))
    neighbour = spot[:longest] + [(spot[longest] + 1) % entries.shape[longest]] + spot[longest + 1:]
    return entries.at[tuple(spot)].set(least).at[tuple(neighbour)].set(largest)


def steps_of(key, dims, shards, low, largest):
    gain, own = 1.0, jax.random.fold_in(key, 6)
    for dim, parts in shards:
        draws = jnp.exp(jax.random.uniform(jax.random.fold_in(own, dim), (parts,), jnp.float32, low / len(shards), largest / len(shards)))
        gain = gain * jnp.repeat(draws, dims[dim] // parts).reshape([-1 if axis == dim else 1 for axis in range(len(dims))])
    return gain


def noise(rng, shape, scale, most, shards=(), kind=jnp.bfloat16):
    values = scale * jax.random.normal(rng, shape, jnp.float32)
    if shards:
        values = values * steps_of(rng, shape, shards, -0.22, 0.18)
    return jnp.clip(values, -most, most).astype(kind)


def setup_inputs(seed: int = 0) -> dict:
    keys = jax.random.split(jax.random.key(seed), 6)
    ensemble = draw_ensemble(jax.random.fold_in(keys[5], 71), 0)
    diffusion = jnp.clip(jnp.exp(math.log(0.12) - 1.0986123 * jax.random.uniform(keys[1], (LEV, NX, NY), jnp.float32) ** steps_of(keys[1], (LEV, NX, NY), ((1, 32),), -0.2, 0.2)), 0.04, 0.12)
    obs_cells = set_ends(jax.random.randint(keys[2], (TILES, SHARES, NOBS), 0, 3 * PATCH), jax.random.fold_in(keys[2], 1), 0, (3 * PATCH) - 1).astype(jnp.int32)
    obs_values = noise(keys[3], (TILES, SHARES, NOBS), 1.0, 6.0, ((0, 32), (1, 16)), jnp.float32)
    obs_weights = jnp.clip(jnp.exp(math.log(36.0) - 1.0986123 * jax.random.uniform(keys[4], (TILES, SHARES, NOBS), jnp.float32) ** steps_of(keys[4], (TILES, SHARES, NOBS), ((0, 32), (1, 16)), -0.2, 0.2)), 12.0, 36.0)
    return {"ensemble": ensemble, "diffusion": diffusion, "obs_cells": obs_cells, "obs_values": obs_values, "obs_weights": obs_weights}


advect = 0.3
vertical = 0.1

def stencil(padded, diffusion):
    extended = jnp.pad(padded, ((0, 0), (1, 1), (0, 0), (1, 1)))
    centre = extended[:, 1:-1, 1:-1, 1:-1]
    west_side = extended[:, 1:-1, :-2, 1:-1]
    east_side = extended[:, 1:-1, 2:, 1:-1]
    south_side = extended[:, 1:-1, 1:-1, :-2]
    north_side = extended[:, 1:-1, 1:-1, 2:]
    level_above = extended[:, 2:, 1:-1, 1:-1]
    level_below = extended[:, :-2, 1:-1, 1:-1]
    laplace = west_side + east_side + south_side + north_side - 4.0 * centre
    return centre + diffusion * laplace + advect * (west_side - centre) + vertical * (level_above + level_below - 2.0 * centre)

def analyse(cellwise, predicted, values, weights):
    members = cellwise.shape[0]
    identity = jnp.eye(members, dtype=jnp.float32)
    pfloat = predicted.astype(jnp.float32)
    pmean = lax.optimization_barrier(jnp.mean(pfloat, axis=0))
    ppert = pfloat - pmean
    innov = values - pmean
    left = (ppert * weights).astype(jnp.bfloat16)
    right = ppert.astype(jnp.bfloat16)
    gram = lax.dot_general(left, right, (((1,), (1,)), ((), ())), preferred_element_type=jnp.float32)
    cov = identity + gram / (members - 1.0)
    scale = 3.0 * jnp.trace(cov) / members
    yiter = cov / scale
    ziter = identity
    for repeat in range(ITERS):
        middle = 1.5 * identity - 0.5 * jnp.dot(ziter.astype(jnp.bfloat16), yiter.astype(jnp.bfloat16), preferred_element_type=jnp.float32)
        mbf = middle.astype(jnp.bfloat16)
        yiter = jnp.dot(yiter.astype(jnp.bfloat16), mbf, preferred_element_type=jnp.float32)
        ziter = jnp.dot(mbf, ziter.astype(jnp.bfloat16), preferred_element_type=jnp.float32)
    root = ziter / jnp.sqrt(scale)
    drive = jnp.dot(ppert, weights * innov, precision=lax.Precision.HIGHEST) / (members - 1.0)
    wmean = jnp.dot(root, jnp.dot(root, drive, precision=lax.Precision.HIGHEST), precision=lax.Precision.HIGHEST)
    wtotal = (root + wmean[:, None]).astype(jnp.bfloat16)
    cfloat = cellwise.astype(jnp.float32)
    xmean = lax.optimization_barrier(jnp.mean(cfloat, axis=0))
    xpert = (cfloat - xmean).astype(jnp.bfloat16)
    update = lax.dot_general(wtotal, xpert, (((0,), (0,)), ((), ())), preferred_element_type=jnp.float32)
    return xmean + update

def reference(ensemble, diffusion, obs_cells, obs_values, obs_weights):
    states = ensemble
    for repeat in range(SUB):
        padded = jnp.pad(states, ((0, 0), (0, 0), (1, 1), (0, 0)))
        states = stencil(padded, diffusion)
    background = states.astype(jnp.bfloat16)
    tiled = background.reshape(K, LEV, N_TILE, CX, NY).transpose(2, 0, 1, 3, 4).reshape(N_TILE, K, N_MEM, PATCH)

    def one_patch(number):
        tindex = number // N_MEM
        mindex = number % N_MEM
        own_tile = tiled[tindex]
        before = own_tile[:, (mindex + N_MEM - 1) % N_MEM]
        middle = own_tile[:, mindex]
        after = own_tile[:, (mindex + 1) % N_MEM]
        extended = jnp.concatenate([before, middle, after], axis=1)
        predicted = jnp.take(extended, obs_cells[tindex, mindex], axis=1)
        return analyse(middle, predicted, obs_values[tindex, mindex], obs_weights[tindex, mindex])
    result = lax.map(one_patch, jnp.arange(N_TILE * N_MEM, dtype=jnp.int32))
    result = result.reshape(N_TILE, N_MEM, K, PATCH).transpose(2, 0, 1, 3)
    result = result.reshape(K, N_TILE, LEV, CX, NY).transpose(0, 2, 1, 3, 4)
    return result.reshape(K, LEV, NX, NY)
```

```python
import functools

import jax
import jax.numpy as jnp
from jax import lax
from jax.experimental import pallas as pl
from jax.experimental.pallas import tpu as pltpu
from jax.sharding import PartitionSpec as P

ITERS = 6
SUB = 3
ADVECT = 0.3
VERTICAL = 0.1
PARTS = 16
LOCAL = 32
LEVELS = 4
ROWS = 32
LANES = 128
MEMBERS = 512
NOBS = 512
CHUNKS = 4
WIDE = 256
PITCH = 40
MESH = pl.DeviceIdType.MESH
F32 = jnp.float32
BF16 = jnp.bfloat16


def row_ids():
    return lax.broadcasted_iota(jnp.int32, (8, LANES), 0)


def place(tiles, source, target):
    first, last = source // 8, (source + 2) // 8
    shift = (target - source) % 8
    out = pltpu.roll(tiles[first], shift, 0) if shift else tiles[first]
    if last != first:
        other = pltpu.roll(tiles[last], shift, 0) if shift else tiles[last]
        out = jnp.where(row_ids() >= target + 8 * last - source, other, out)
    return out


def pack(pieces, base):
    rows = row_ids()
    out = []
    for block in range(3):
        acc = jnp.zeros((8, LANES), F32)
        for number, piece in enumerate(pieces):
            low, high = 3 * number - 8 * block, 3 * number + 3 - 8 * block
            if high <= 0 or low >= 8:
                continue
            shift = (3 * number - base) % 8
            moved = pltpu.roll(piece, shift, 0) if shift else piece
            acc = jnp.where((rows >= low) & (rows < high), moved, acc)
        out.append(acc)
    return out


def kernel(
    ens_hbm, dif_ref, cells_ref, values_ref, weights_ref, out_ref,
    ens, up_send, down_send, top_halo, low_halo, coef, turn,
    oc, cell_send, cell_recv, pred_send, pred_recv,
    ymat, zmat, mmat, root, drive, back_send, back_recv,
    load_sem, halo_ssem, halo_rsem, oc_ssem, oc_rsem, pred_ssem, pred_rsem,
    cell_ssem, cell_rsem, back_ssem, back_rsem,
):
    me = lax.axis_index("mem")
    tile = lax.axis_index("tile")
    tiles = lax.axis_size("tile")
    right, left = lax.rem(tile + 1, tiles), lax.rem(tile + tiles - 1, tiles)

    load = pltpu.make_async_copy(ens_hbm, ens, load_sem)
    load.start()
    barrier = pltpu.get_barrier_semaphore()
    for offset in range(1, PARTS):
        pl.semaphore_signal(
            barrier, inc=1, device_id={"mem": lax.rem(me + offset, PARTS)}, device_id_type=MESH
        )
    for other in (left, right):
        pl.semaphore_signal(barrier, inc=1, device_id={"tile": other}, device_id_type=MESH)
    load.wait()

    def pack_pair(pair, carry):
        tops, lows = [], []
        for half in range(2):
            for level in range(LEVELS):
                tops.append(ens[2 * pair + half, level, 0:8, :])
                lows.append(ens[2 * pair + half, level, ROWS - 8 : ROWS, :])
        for block, value in enumerate(pack(tops, 0)):
            up_send[pair, 8 * block : 8 * block + 8, :] = value
        for block, value in enumerate(pack(lows, 5)):
            down_send[pair, 8 * block : 8 * block + 8, :] = value
        return carry

    lax.fori_loop(0, LOCAL // 2, pack_pair, 0)
    tops = [dif_ref[level, 0:8, :] for level in range(LEVELS)]
    lows = [dif_ref[level, ROWS - 8 : ROWS, :] for level in range(LEVELS)]
    for block, value in enumerate(pack(tops, 0)):
        up_send[LOCAL // 2, 8 * block : 8 * block + 8, :] = value
    for block, value in enumerate(pack(lows, 5)):
        down_send[LOCAL // 2, 8 * block : 8 * block + 8, :] = value

    pl.semaphore_wait(barrier, PARTS + 1)

    def remote(source, target, ssem, rsem, device):
        return pltpu.make_async_remote_copy(
            src_ref=source, dst_ref=target, send_sem=ssem, recv_sem=rsem,
            device_id=device, device_id_type=MESH,
        )

    def oc_copy(offset):
        return remote(
            cells_ref.at[0], oc.at[me], oc_ssem.at[offset], oc_rsem.at[offset],
            {"mem": lax.rem(me + offset, PARTS)},
        )

    def pred_copy(offset):
        other = lax.rem(me + offset, PARTS)
        return remote(
            pred_send.at[other], pred_recv.at[me], pred_ssem.at[offset], pred_rsem.at[offset],
            {"mem": other},
        )

    def cell_copy(chunk, offset):
        other = lax.rem(me + offset, PARTS)
        return remote(
            cell_send.at[other, chunk], cell_recv.at[chunk, me],
            cell_ssem.at[chunk, offset], cell_rsem.at[chunk, offset], {"mem": other},
        )

    def back_copy(chunk, offset):
        other = lax.rem(me + offset, PARTS)
        return remote(
            back_send.at[chunk, other], back_recv.at[chunk, me],
            back_ssem.at[chunk, offset], back_rsem.at[chunk, offset], {"mem": other},
        )

    def each(action):
        def step(offset, carry):
            action(offset)
            return carry

        lax.fori_loop(1, PARTS, step, 0)

    to_right = remote(down_send, top_halo, halo_ssem.at[0], halo_rsem.at[0], {"tile": right})
    to_left = remote(up_send, low_halo, halo_ssem.at[1], halo_rsem.at[1], {"tile": left})
    to_right.start()
    to_left.start()
    each(lambda offset: oc_copy(offset).start())
    oc[me] = cells_ref[0]

    top_mask = jnp.where(tile > 0, 1.0, 0.0).astype(F32)
    low_mask = jnp.where(tile < tiles - 1, 1.0, 0.0).astype(F32)
    to_right.wait()
    to_left.wait()
    extra = [
        [halo[LOCAL // 2, 8 * block : 8 * block + 8, :] for block in range(3)]
        for halo in (top_halo, low_halo)
    ]
    lane = lax.broadcasted_iota(jnp.int32, (ROWS + 16, LANES), 1)
    for level in range(LEVELS):
        dif = jnp.concatenate(
            [place(extra[0], 3 * level, 5), dif_ref[level], place(extra[1], 3 * level, 0)], axis=0
        )
        coef[0, level] = 1.0 - ADVECT - 2.0 * VERTICAL - 4.0 * dif
        coef[1, level] = dif + ADVECT
        coef[2, level] = dif
        coef[3, level] = jnp.where(lane == 0, 0.0, dif)
        coef[4, level] = jnp.where(lane == LANES - 1, 0.0, dif)

    def forecast_pair(pair, carry):
        above = [top_halo[pair, 8 * block : 8 * block + 8, :] for block in range(3)]
        below = [low_halo[pair, 8 * block : 8 * block + 8, :] for block in range(3)]
        for half in range(2):
            member = 2 * pair + half
            states = []
            for level in range(LEVELS):
                at = 3 * (LEVELS * half + level)
                states.append(
                    jnp.concatenate(
                        [
                            place(above, at, 5) * top_mask,
                            ens[member, level],
                            place(below, at, 0) * low_mask,
                        ],
                        axis=0,
                    )
                )
            for repeat in range(SUB):
                updated = []
                for level in range(LEVELS):
                    state = states[level]
                    near = [states[n] for n in (level - 1, level + 1) if 0 <= n < LEVELS]
                    column = near[0] + near[1] if len(near) == 2 else near[0]
                    value = (
                        coef[0, level] * state
                        + coef[1, level] * pltpu.roll(state, 1, 0)
                        + coef[2, level] * pltpu.roll(state, ROWS + 15, 0)
                        + coef[3, level] * pltpu.roll(state, 1, 1)
                        + coef[4, level] * pltpu.roll(state, LANES - 1, 1)
                        + VERTICAL * column
                    )
                    if repeat < SUB - 1:
                        value = jnp.concatenate(
                            [
                                value[0:8] * top_mask,
                                value[8 : ROWS + 8],
                                value[ROWS + 8 :] * low_mask,
                            ],
                            axis=0,
                        )
                    updated.append(value)
                states = updated
            for level in range(LEVELS):
                for block in range(ROWS // 8):
                    first = (level * ROWS + 8 * block) * PITCH
                    turn[pl.ds(first + member, 8, stride=PITCH), :] = states[level][
                        8 * block + 8 : 8 * block + 16
                    ]
        return carry

    lax.fori_loop(0, LOCAL // 2, forecast_pair, 0)

    def to_cells(part, carry):
        for chunk in range(CHUNKS):
            for half in range(2):
                first = pl.multiple_of((part * 8 + 2 * chunk + half) * PITCH, 8)
                cell_send[part, chunk, :, half * LANES : (half + 1) * LANES] = turn[
                    pl.ds(first, LOCAL), :
                ].astype(BF16)
        return carry

    lax.fori_loop(0, PARTS, to_cells, 0)

    each(lambda offset: oc_copy(offset).wait())
    within = lax.broadcasted_iota(jnp.int32, (WIDE, NOBS), 0)

    def gather(offset, carry):
        part = lax.rem(me + offset, PARTS)
        index = oc[part]
        hot = jnp.where(within == jnp.bitwise_and(index, WIDE - 1), 1.0, 0.0).astype(BF16)
        group = jnp.broadcast_to(jnp.right_shift(index, 8), (LOCAL, NOBS))
        pieces = []
        for step in (PARTS - 1, 0, 1):
            other = lax.rem(part + step, PARTS)
            for chunk in range(CHUNKS):
                pieces.append(cell_send[other, chunk])
        found = jnp.dot(jnp.concatenate(pieces, axis=0), hot, preferred_element_type=F32)
        total = jnp.zeros((LOCAL, NOBS), F32)
        for number in range(3 * CHUNKS):
            total += jnp.where(
                group == number, found[LOCAL * number : LOCAL * number + LOCAL], 0.0
            )
        pred_send[part] = total.astype(BF16)
        pl.when(offset > 1)(lambda: pred_copy(offset - 1).start())
        return carry

    lax.fori_loop(1, PARTS + 1, gather, 0)
    for chunk in range(CHUNKS):
        each(lambda offset: cell_copy(chunk, offset).start())
        cell_recv[chunk, me] = cell_send[me, chunk]
    pred_recv[me] = pred_send[me]

    each(lambda offset: pred_copy(offset).wait())
    weights, values = weights_ref[0], values_ref[0]
    total = jnp.zeros((1, NOBS), F32)
    for part in range(PARTS):
        total += jnp.sum(pred_recv[part].astype(F32), axis=0, keepdims=True)
    pmean = total * (1.0 / MEMBERS)
    pull = weights * (values - pmean)
    for part in range(PARTS):
        rows = slice(LOCAL * part, LOCAL * part + LOCAL)
        ppert = pred_recv[part].astype(F32) - pmean
        ymat[rows, :] = (ppert * weights).astype(BF16)
        zmat[rows, :] = ppert.astype(BF16)
        drive[rows, :] = jnp.sum(ppert * pull, axis=1, keepdims=True) * (1.0 / (MEMBERS - 1.0))
    gram = lax.dot_general(
        zmat[...], ymat[...], (((1,), (1,)), ((), ())), preferred_element_type=F32
    )
    eye = jnp.where(
        lax.broadcasted_iota(jnp.int32, (MEMBERS, MEMBERS), 0)
        == lax.broadcasted_iota(jnp.int32, (MEMBERS, MEMBERS), 1),
        1.0,
        0.0,
    )
    root[...] = gram * (1.0 / (MEMBERS - 1.0)) + eye
    small = jnp.where(
        lax.broadcasted_iota(jnp.int32, (LANES, LANES), 0)
        == lax.broadcasted_iota(jnp.int32, (LANES, LANES), 1),
        1.0,
        0.0,
    )
    trace = jnp.zeros((1, 1), F32)
    for block in range(MEMBERS // LANES):
        part = slice(LANES * block, LANES * block + LANES)
        diagonal = jnp.sum(root[part, part] * small, axis=1, keepdims=True)
        trace += jnp.sum(diagonal, axis=0, keepdims=True)
    scale = trace * (3.0 / MEMBERS)
    first = (root[...] * (1.0 / scale)).astype(BF16)
    ymat[...] = first
    mmat[...] = (1.5 * eye - 0.5 * first.astype(F32)).astype(BF16)
    zmat[...] = mmat[...]
    ymat[...] = jnp.dot(mmat[...], first, preferred_element_type=F32).astype(BF16)

    def newton(step, carry):
        product = jnp.dot(ymat[...], zmat[...], preferred_element_type=F32)
        mmat[...] = (1.5 * eye - 0.5 * product).astype(BF16)
        ynext = jnp.dot(mmat[...], ymat[...], preferred_element_type=F32).astype(BF16)
        znext = jnp.dot(zmat[...], mmat[...], preferred_element_type=F32).astype(BF16)
        ymat[...] = ynext
        zmat[...] = znext
        return carry

    lax.fori_loop(0, ITERS - 2, newton, 0)
    product = jnp.dot(ymat[...], zmat[...], preferred_element_type=F32)
    mmat[...] = (1.5 * eye - 0.5 * product).astype(BF16)
    root[...] = jnp.dot(zmat[...], mmat[...], preferred_element_type=F32) * (
        1.0 / jnp.sqrt(scale)
    )
    across = jnp.sum(root[...] * drive[...], axis=0, keepdims=True)
    wmean = jnp.zeros((1, MEMBERS), F32)
    for block in range(MEMBERS // LANES):
        part = slice(LANES * block, LANES * block + LANES)
        down = jnp.sum(across[:, part] * small, axis=1, keepdims=True)
        wmean += jnp.sum(root[part, :] * down, axis=0, keepdims=True)
    ymat[...] = (root[...] + wmean).astype(BF16)

    for chunk in range(CHUNKS):
        each(lambda offset: cell_copy(chunk, offset).wait())
        total = jnp.zeros((1, WIDE), F32)
        for part in range(PARTS):
            total += jnp.sum(cell_recv[chunk, part].astype(F32), axis=0, keepdims=True)
        xmean = total * (1.0 / MEMBERS)
        for part in range(PARTS):
            zmat[LOCAL * part : LOCAL * part + LOCAL, 0:WIDE] = (
                cell_recv[chunk, part].astype(F32) - xmean
            ).astype(BF16)
        update = jnp.dot(ymat[...], zmat[:, 0:WIDE], preferred_element_type=F32) + xmean
        for part in range(PARTS):
            back_send[chunk, part] = update[LOCAL * part : LOCAL * part + LOCAL].astype(BF16)
        each(lambda offset: back_copy(chunk, offset).start())
        back_recv[chunk, me] = back_send[chunk, me]

    for chunk in range(CHUNKS):
        each(lambda offset: back_copy(chunk, offset).wait())

        def from_cells(part, carry):
            for half in range(2):
                first = pl.multiple_of((part * 8 + 2 * chunk + half) * PITCH, 8)
                turn[pl.ds(first, LOCAL), :] = back_recv[
                    chunk, part, :, half * LANES : (half + 1) * LANES
                ].astype(F32)
            return carry

        lax.fori_loop(0, PARTS, from_cells, 0)

    def to_states(member, carry):
        for part in range(PARTS):
            out_ref[member, part // 4, (part % 4) * 8 : (part % 4) * 8 + 8, :] = turn[
                pl.ds(part * 8 * PITCH + member, 8, stride=PITCH), :
            ]
        return carry

    lax.fori_loop(0, LOCAL, to_states, 0)


def on_device(ensemble, diffusion, obs_cells, obs_values, obs_weights):
    vmem = pl.BlockSpec(memory_space=pltpu.VMEM)
    dma = pltpu.SemaphoreType.DMA
    halo = pltpu.VMEM((LOCAL // 2 + 1, 24, LANES), F32)
    square = pltpu.VMEM((MEMBERS, MEMBERS), BF16)
    return pl.pallas_call(
        kernel,
        name="cycle",
        out_shape=jax.ShapeDtypeStruct(ensemble.shape, F32),
        in_specs=[pl.BlockSpec(memory_space=pl.ANY)] + [vmem] * 4,
        out_specs=vmem,
        scratch_shapes=[
            pltpu.VMEM(ensemble.shape, F32),
            halo, halo, halo, halo,
            pltpu.VMEM((5, LEVELS, ROWS + 16, LANES), F32),
            pltpu.VMEM((LEVELS * ROWS * PITCH, LANES), F32),
            pltpu.VMEM((PARTS, 1, NOBS), jnp.int32),
            pltpu.VMEM((PARTS, CHUNKS, LOCAL, WIDE), BF16),
            pltpu.VMEM((CHUNKS, PARTS, LOCAL, WIDE), BF16),
            pltpu.VMEM((PARTS, LOCAL, NOBS), BF16),
            pltpu.VMEM((PARTS, LOCAL, NOBS), BF16),
            square, square, square,
            pltpu.VMEM((MEMBERS, MEMBERS), F32),
            pltpu.VMEM((MEMBERS, 1), F32),
            pltpu.VMEM((CHUNKS, PARTS, LOCAL, WIDE), BF16),
            pltpu.VMEM((CHUNKS, PARTS, LOCAL, WIDE), BF16),
            dma, dma((2,)), dma((2,)),
            dma((PARTS,)), dma((PARTS,)), dma((PARTS,)), dma((PARTS,)),
            dma((CHUNKS, PARTS)), dma((CHUNKS, PARTS)),
            dma((CHUNKS, PARTS)), dma((CHUNKS, PARTS)),
        ],
        compiler_params=pltpu.CompilerParams(
            collective_id=0, has_side_effects=True, vmem_limit_bytes=56 * 1024 * 1024
        ),
    )(ensemble, diffusion, obs_cells, obs_values, obs_weights)


def solution(mesh):
    return jax.shard_map(
        on_device,
        mesh=mesh,
        in_specs=(
            P("mem", None, "tile", None),
            P(None, "tile", None),
            P("tile", "mem", None),
            P("tile", "mem", None),
            P("tile", "mem", None),
        ),
        out_specs=P("mem", None, "tile", None),
        check_vma=False,
    )
```

```python
import functools

import jax
import jax.numpy as jnp
from jax import lax
from jax.experimental import pallas as pl
from jax.experimental.pallas import tpu as pltpu
from jax.sharding import PartitionSpec as P

ITERS = 6
SUB = 3
ADVECT = 0.3
VERTICAL = 0.1
PARTS = 16
LOCAL = 32
LEVELS = 4
ROWS = 32
LANES = 128
MEMBERS = 512
NOBS = 512
CHUNKS = 4
WIDE = 256
PITCH = 40
MESH = pl.DeviceIdType.MESH
F32 = jnp.float32
BF16 = jnp.bfloat16


def row_ids():
    return lax.broadcasted_iota(jnp.int32, (8, LANES), 0)


def place(tiles, source, target):
    first, last = source // 8, (source + 2) // 8
    shift = (target - source) % 8
    out = pltpu.roll(tiles[first], shift, 0) if shift else tiles[first]
    if last != first:
        other = pltpu.roll(tiles[last], shift, 0) if shift else tiles[last]
        out = jnp.where(row_ids() >= target + 8 * last - source, other, out)
    return out


def pack(pieces, base):
    rows = row_ids()
    out = []
    for block in range(3):
        acc = jnp.zeros((8, LANES), F32)
        for number, piece in enumerate(pieces):
            low, high = 3 * number - 8 * block, 3 * number + 3 - 8 * block
            if high <= 0 or low >= 8:
                continue
            shift = (3 * number - base) % 8
            moved = pltpu.roll(piece, shift, 0) if shift else piece
            acc = jnp.where((rows >= low) & (rows < high), moved, acc)
        out.append(acc)
    return out


def windows(above, upper, lower, below, step):
    rows = row_ids()
    shift = 2 - step
    top = jnp.where(rows < shift, pltpu.roll(above, shift, 0), pltpu.roll(upper, shift, 0))
    shift = 6 - step
    low = jnp.where(rows < shift, pltpu.roll(lower, shift, 0), pltpu.roll(below, shift, 0))
    return jnp.concatenate([top, low], axis=0)


def coefficients(coef, dif_ref, rows):
    lane = lax.broadcasted_iota(jnp.int32, (rows, LANES), 1)
    for level in range(LEVELS):
        dif = dif_ref[level]
        coef[0, level] = 1.0 - ADVECT - 2.0 * VERTICAL - 4.0 * dif
        coef[1, level] = dif + ADVECT
        coef[2, level] = dif
        coef[3, level] = jnp.where(lane == 0, 0.0, dif)
        coef[4, level] = jnp.where(lane == LANES - 1, 0.0, dif)


def column(states, level):
    near = [states[n] for n in (level - 1, level + 1) if 0 <= n < LEVELS]
    return near[0] + near[1] if len(near) == 2 else near[0]


def substep(coef, level, state, west, east, vertical):
    return (
        coef[0, level] * state
        + coef[1, level] * west
        + coef[2, level] * east
        + coef[3, level] * pltpu.roll(state, 1, 1)
        + coef[4, level] * pltpu.roll(state, LANES - 1, 1)
        + VERTICAL * vertical
    )


def kernel(
    ens_hbm, dif_ref, cells_ref, values_ref, weights_ref, out_ref,
    ens, up_send, down_send, top_halo, low_halo, coef, edge_coef, edge_dif, turn,
    oc, cell_send, cell_recv, pred_send, pred_recv,
    ymat, zmat, mmat, root, drive, back_send, back_recv,
    load_sem, halo_ssem, halo_rsem, oc_ssem, oc_rsem, pred_ssem, pred_rsem,
    cell_ssem, cell_rsem, back_ssem, back_rsem,
):
    me = lax.axis_index("mem")
    tile = lax.axis_index("tile")
    tiles = lax.axis_size("tile")
    right, left = lax.rem(tile + 1, tiles), lax.rem(tile + tiles - 1, tiles)

    load = pltpu.make_async_copy(ens_hbm, ens, load_sem)
    load.start()
    barrier = pltpu.get_barrier_semaphore()
    for offset in range(1, PARTS):
        pl.semaphore_signal(
            barrier, inc=1, device_id={"mem": lax.rem(me + offset, PARTS)}, device_id_type=MESH
        )
    for other in (left, right):
        pl.semaphore_signal(barrier, inc=1, device_id={"tile": other}, device_id_type=MESH)
    load.wait()

    def pack_pair(pair, carry):
        tops, lows = [], []
        for half in range(2):
            for level in range(LEVELS):
                tops.append(ens[2 * pair + half, level, 0:8, :])
                lows.append(ens[2 * pair + half, level, ROWS - 8 : ROWS, :])
        for block, value in enumerate(pack(tops, 0)):
            up_send[pair, 8 * block : 8 * block + 8, :] = value
        for block, value in enumerate(pack(lows, 5)):
            down_send[pair, 8 * block : 8 * block + 8, :] = value
        return carry

    lax.fori_loop(0, LOCAL // 2, pack_pair, 0)
    tops = [dif_ref[level, 0:8, :] for level in range(LEVELS)]
    lows = [dif_ref[level, ROWS - 8 : ROWS, :] for level in range(LEVELS)]
    for block, value in enumerate(pack(tops, 0)):
        up_send[LOCAL // 2, 8 * block : 8 * block + 8, :] = value
    for block, value in enumerate(pack(lows, 5)):
        down_send[LOCAL // 2, 8 * block : 8 * block + 8, :] = value

    pl.semaphore_wait(barrier, PARTS + 1)

    def remote(source, target, ssem, rsem, device):
        return pltpu.make_async_remote_copy(
            src_ref=source, dst_ref=target, send_sem=ssem, recv_sem=rsem,
            device_id=device, device_id_type=MESH,
        )

    def oc_copy(offset):
        return remote(
            cells_ref.at[0], oc.at[me], oc_ssem.at[offset], oc_rsem.at[offset],
            {"mem": lax.rem(me + offset, PARTS)},
        )

    def pred_copy(offset):
        other = lax.rem(me + offset, PARTS)
        return remote(
            pred_send.at[other], pred_recv.at[me], pred_ssem.at[offset], pred_rsem.at[offset],
            {"mem": other},
        )

    def cell_copy(chunk, offset):
        other = lax.rem(me + offset, PARTS)
        return remote(
            cell_send.at[other, chunk], cell_recv.at[chunk, me],
            cell_ssem.at[chunk, offset], cell_rsem.at[chunk, offset], {"mem": other},
        )

    def back_copy(chunk, offset):
        other = lax.rem(me + offset, PARTS)
        return remote(
            back_send.at[chunk, other], back_recv.at[chunk, me],
            back_ssem.at[chunk, offset], back_rsem.at[chunk, offset], {"mem": other},
        )

    def each(action):
        def step(offset, carry):
            action(offset)
            return carry

        lax.fori_loop(1, PARTS, step, 0)

    to_right = remote(down_send, top_halo, halo_ssem.at[0], halo_rsem.at[0], {"tile": right})
    to_left = remote(up_send, low_halo, halo_ssem.at[1], halo_rsem.at[1], {"tile": left})
    to_right.start()
    to_left.start()
    each(lambda offset: oc_copy(offset).start())
    oc[me] = cells_ref[0]

    coefficients(coef, dif_ref, ROWS)

    def inner_pair(pair, carry):
        for half in range(2):
            member = 2 * pair + half
            states = [ens[member, level] for level in range(LEVELS)]
            for repeat in range(SUB):
                states = [
                    substep(
                        coef, level, states[level],
                        pltpu.roll(states[level], 1, 0),
                        pltpu.roll(states[level], ROWS - 1, 0),
                        column(states, level),
                    )
                    for level in range(LEVELS)
                ]
            for level in range(LEVELS):
                for block in range(ROWS // 8):
                    first = (level * ROWS + 8 * block) * PITCH
                    turn[pl.ds(first + member, 8, stride=PITCH), :] = states[level][
                        8 * block : 8 * block + 8
                    ]
        return carry

    def to_cells(part, low, count):
        for chunk in range(CHUNKS):
            for half in range(2):
                first = pl.multiple_of((part * 8 + 2 * chunk + half) * PITCH + low, 8)
                cell_send[part, chunk, low : low + count, half * LANES : (half + 1) * LANES] = (
                    turn[pl.ds(first, count), :].astype(BF16)
                )

    half_count = LOCAL // 2
    for low in (0, half_count):
        lax.fori_loop(low // 2, (low + half_count) // 2, inner_pair, 0)

        def inner_cells(number, carry):
            to_cells(4 * (number // 2) + 1 + lax.rem(number, 2), low, half_count)
            return carry

        lax.fori_loop(0, PARTS // 2, inner_cells, 0)

        def inner_send(number, carry):
            turned = lax.rem(number + lax.div(me + 1, 2), PARTS // 2)
            part = 4 * lax.div(turned, 2) + 1 + lax.rem(turned, 2)
            offset = lax.rem(part - me + PARTS, PARTS)

            @pl.when(offset > 0)
            def _():
                for chunk in range(CHUNKS):
                    remote(
                        cell_send.at[part, chunk, pl.ds(low, half_count)],
                        cell_recv.at[chunk, me, pl.ds(low, half_count)],
                        cell_ssem.at[chunk, offset], cell_rsem.at[chunk, offset], {"mem": part},
                    ).start()

            return carry

        lax.fori_loop(0, PARTS // 2, inner_send, 0)

    top_mask = jnp.where(tile > 0, 1.0, 0.0).astype(F32)
    low_mask = jnp.where(tile < tiles - 1, 1.0, 0.0).astype(F32)
    to_right.wait()
    to_left.wait()
    extra = [
        [halo[LOCAL // 2, 8 * block : 8 * block + 8, :] for block in range(3)]
        for halo in (top_halo, low_halo)
    ]
    for level in range(LEVELS):
        edge_dif[level] = windows(
            place(extra[0], 3 * level, 5), dif_ref[level, 0:8],
            dif_ref[level, ROWS - 8 : ROWS], place(extra[1], 3 * level, 0), 0,
        )
    coefficients(edge_coef, edge_dif, 16)
    edge_row = lax.broadcasted_iota(jnp.int32, (16, LANES), 0)
    edge_mask = jnp.where(edge_row < 2, top_mask, jnp.where(edge_row >= 14, low_mask, 1.0))

    def edge_pair(pair, carry):
        above = [top_halo[pair, 8 * block : 8 * block + 8, :] for block in range(3)]
        below = [low_halo[pair, 8 * block : 8 * block + 8, :] for block in range(3)]
        for half in range(2):
            member = 2 * pair + half
            states, wests, easts = [], [], []
            for level in range(LEVELS):
                at = 3 * (LEVELS * half + level)
                parts = (
                    place(above, at, 5) * top_mask, ens[member, level, 0:8],
                    ens[member, level, ROWS - 8 : ROWS], place(below, at, 0) * low_mask,
                )
                states.append(windows(*parts, 0))
                wests.append(windows(*parts, -1))
                easts.append(windows(*parts, 1))
            for repeat in range(SUB):
                updated = []
                for level in range(LEVELS):
                    state = states[level]
                    west = pltpu.roll(state, 1, 0) if repeat else wests[level]
                    east = pltpu.roll(state, 15, 0) if repeat else easts[level]
                    value = substep(
                        edge_coef, level, state, west, east, column(states, level)
                    )
                    updated.append(value * edge_mask if repeat < SUB - 1 else value)
                states = updated
            for level in range(LEVELS):
                first = level * ROWS * PITCH + member
                turn[pl.ds(first, 3, stride=PITCH), :] = states[level][2:5]
                turn[pl.ds(first + (ROWS - 3) * PITCH, 3, stride=PITCH), :] = states[level][11:14]
        return carry

    lax.fori_loop(0, LOCAL // 2, edge_pair, 0)

    def edge_cells(number, carry):
        to_cells(4 * (number // 2) + 3 * lax.rem(number, 2), 0, LOCAL)
        return carry

    lax.fori_loop(0, PARTS // 2, edge_cells, 0)

    each(lambda offset: oc_copy(offset).wait())
    within = lax.broadcasted_iota(jnp.int32, (WIDE, NOBS), 0)

    def gather(offset, carry):
        part = lax.rem(me + offset, PARTS)
        index = oc[part]
        hot = jnp.where(within == jnp.bitwise_and(index, WIDE - 1), 1.0, 0.0).astype(BF16)
        group = jnp.broadcast_to(jnp.right_shift(index, 8), (LOCAL, NOBS))
        pieces = []
        for step in (PARTS - 1, 0, 1):
            other = lax.rem(part + step, PARTS)
            for chunk in range(CHUNKS):
                pieces.append(cell_send[other, chunk])
        found = jnp.dot(jnp.concatenate(pieces, axis=0), hot, preferred_element_type=F32)
        total = jnp.zeros((LOCAL, NOBS), F32)
        for number in range(3 * CHUNKS):
            total += jnp.where(
                group == number, found[LOCAL * number : LOCAL * number + LOCAL], 0.0
            )
        pred_send[part] = total.astype(BF16)
        pl.when(offset > 1)(lambda: pred_copy(offset - 1).start())
        return carry

    lax.fori_loop(1, PARTS + 1, gather, 0)
    for chunk in range(CHUNKS):
        def edge_send(number, carry):
            turned = lax.rem(number + lax.div(me + 1, 2), PARTS // 2)
            part = 4 * lax.div(turned, 2) + 3 * lax.rem(turned, 2)
            offset = lax.rem(part - me + PARTS, PARTS)
            pl.when(offset > 0)(lambda: cell_copy(chunk, offset).start())
            return carry

        lax.fori_loop(0, PARTS // 2, edge_send, 0)
        cell_recv[chunk, me] = cell_send[me, chunk]
    pred_recv[me] = pred_send[me]

    each(lambda offset: pred_copy(offset).wait())
    weights, values = weights_ref[0], values_ref[0]
    total = jnp.zeros((1, NOBS), F32)
    for part in range(PARTS):
        total += jnp.sum(pred_recv[part].astype(F32), axis=0, keepdims=True)
    pmean = total * (1.0 / MEMBERS)
    pull = weights * (values - pmean)
    for part in range(PARTS):
        rows = slice(LOCAL * part, LOCAL * part + LOCAL)
        ppert = pred_recv[part].astype(F32) - pmean
        ymat[rows, :] = (ppert * weights).astype(BF16)
        zmat[rows, :] = ppert.astype(BF16)
        drive[rows, :] = jnp.sum(ppert * pull, axis=1, keepdims=True) * (1.0 / (MEMBERS - 1.0))
    gram = lax.dot_general(
        zmat[...], ymat[...], (((1,), (1,)), ((), ())), preferred_element_type=F32
    )
    eye = jnp.where(
        lax.broadcasted_iota(jnp.int32, (MEMBERS, MEMBERS), 0)
        == lax.broadcasted_iota(jnp.int32, (MEMBERS, MEMBERS), 1),
        1.0,
        0.0,
    )
    root[...] = gram * (1.0 / (MEMBERS - 1.0)) + eye
    small = jnp.where(
        lax.broadcasted_iota(jnp.int32, (LANES, LANES), 0)
        == lax.broadcasted_iota(jnp.int32, (LANES, LANES), 1),
        1.0,
        0.0,
    )
    trace = jnp.zeros((1, 1), F32)
    for block in range(MEMBERS // LANES):
        part = slice(LANES * block, LANES * block + LANES)
        diagonal = jnp.sum(root[part, part] * small, axis=1, keepdims=True)
        trace += jnp.sum(diagonal, axis=0, keepdims=True)
    scale = trace * (3.0 / MEMBERS)
    first = (root[...] * (1.0 / scale)).astype(BF16)
    ymat[...] = first
    mmat[...] = (1.5 * eye - 0.5 * first.astype(F32)).astype(BF16)
    zmat[...] = mmat[...]
    ymat[...] = jnp.dot(mmat[...], first, preferred_element_type=F32).astype(BF16)

    def newton(step, carry):
        product = jnp.dot(ymat[...], zmat[...], preferred_element_type=F32)
        mmat[...] = (1.5 * eye - 0.5 * product).astype(BF16)
        ynext = jnp.dot(mmat[...], ymat[...], preferred_element_type=F32).astype(BF16)
        znext = jnp.dot(zmat[...], mmat[...], preferred_element_type=F32).astype(BF16)
        ymat[...] = ynext
        zmat[...] = znext
        return carry

    lax.fori_loop(0, ITERS - 2, newton, 0)
    product = jnp.dot(ymat[...], zmat[...], preferred_element_type=F32)
    mmat[...] = (1.5 * eye - 0.5 * product).astype(BF16)
    root[...] = jnp.dot(zmat[...], mmat[...], preferred_element_type=F32) * (
        1.0 / jnp.sqrt(scale)
    )
    across = jnp.sum(root[...] * drive[...], axis=0, keepdims=True)
    wmean = jnp.zeros((1, MEMBERS), F32)
    for block in range(MEMBERS // LANES):
        part = slice(LANES * block, LANES * block + LANES)
        down = jnp.sum(across[:, part] * small, axis=1, keepdims=True)
        wmean += jnp.sum(root[part, :] * down, axis=0, keepdims=True)
    ymat[...] = (root[...] + wmean).astype(BF16)

    for chunk in range(CHUNKS):
        each(lambda offset: cell_copy(chunk, offset).wait())
        total = jnp.zeros((1, WIDE), F32)
        for part in range(PARTS):
            total += jnp.sum(cell_recv[chunk, part].astype(F32), axis=0, keepdims=True)
        xmean = total * (1.0 / MEMBERS)
        for part in range(PARTS):
            zmat[LOCAL * part : LOCAL * part + LOCAL, 0:WIDE] = (
                cell_recv[chunk, part].astype(F32) - xmean
            ).astype(BF16)
        update = jnp.dot(ymat[...], zmat[:, 0:WIDE], preferred_element_type=F32) + xmean
        for part in range(PARTS):
            back_send[chunk, part] = update[LOCAL * part : LOCAL * part + LOCAL].astype(BF16)
        each(lambda offset: back_copy(chunk, offset).start())
        back_recv[chunk, me] = back_send[chunk, me]

    for chunk in range(CHUNKS):
        each(lambda offset: back_copy(chunk, offset).wait())

        def from_cells(part, carry):
            for half in range(2):
                first = pl.multiple_of((part * 8 + 2 * chunk + half) * PITCH, 8)
                turn[pl.ds(first, LOCAL), :] = back_recv[
                    chunk, part, :, half * LANES : (half + 1) * LANES
                ].astype(F32)
            return carry

        lax.fori_loop(0, PARTS, from_cells, 0)

    def to_states(member, carry):
        for part in range(PARTS):
            out_ref[member, part // 4, (part % 4) * 8 : (part % 4) * 8 + 8, :] = turn[
                pl.ds(part * 8 * PITCH + member, 8, stride=PITCH), :
            ]
        return carry

    lax.fori_loop(0, LOCAL, to_states, 0)


def on_device(ensemble, diffusion, obs_cells, obs_values, obs_weights):
    vmem = pl.BlockSpec(memory_space=pltpu.VMEM)
    dma = pltpu.SemaphoreType.DMA
    halo = pltpu.VMEM((LOCAL // 2 + 1, 24, LANES), F32)
    square = pltpu.VMEM((MEMBERS, MEMBERS), BF16)
    return pl.pallas_call(
        kernel,
        name="cycle",
        out_shape=pltpu.VMEM(ensemble.shape, F32),
        in_specs=[pl.BlockSpec(memory_space=pl.ANY)] + [vmem] * 4,
        out_specs=vmem,
        scratch_shapes=[
            pltpu.VMEM(ensemble.shape, F32),
            halo, halo, halo, halo,
            pltpu.VMEM((5, LEVELS, ROWS, LANES), F32),
            pltpu.VMEM((5, LEVELS, 16, LANES), F32),
            pltpu.VMEM((LEVELS, 16, LANES), F32),
            pltpu.VMEM((LEVELS * ROWS * PITCH, LANES), F32),
            pltpu.VMEM((PARTS, 1, NOBS), jnp.int32),
            pltpu.VMEM((PARTS, CHUNKS, LOCAL, WIDE), BF16),
            pltpu.VMEM((CHUNKS, PARTS, LOCAL, WIDE), BF16),
            pltpu.VMEM((PARTS, LOCAL, NOBS), BF16),
            pltpu.VMEM((PARTS, LOCAL, NOBS), BF16),
            square, square, square,
            pltpu.VMEM((MEMBERS, MEMBERS), F32),
            pltpu.VMEM((MEMBERS, 1), F32),
            pltpu.VMEM((CHUNKS, PARTS, LOCAL, WIDE), BF16),
            pltpu.VMEM((CHUNKS, PARTS, LOCAL, WIDE), BF16),
            dma, dma((2,)), dma((2,)),
            dma((PARTS,)), dma((PARTS,)), dma((PARTS,)), dma((PARTS,)),
            dma((CHUNKS, PARTS)), dma((CHUNKS, PARTS)),
            dma((CHUNKS, PARTS)), dma((CHUNKS, PARTS)),
        ],
        compiler_params=pltpu.CompilerParams(
            collective_id=0, has_side_effects=True, vmem_limit_bytes=56 * 1024 * 1024
        ),
    )(ensemble, diffusion, obs_cells, obs_values, obs_weights)


def solution(mesh):
    return jax.shard_map(
        on_device,
        mesh=mesh,
        in_specs=(
            P("mem", None, "tile", None),
            P(None, "tile", None),
            P("tile", "mem", None),
            P("tile", "mem", None),
            P("tile", "mem", None),
        ),
        out_specs=P("mem", None, "tile", None),
        check_vma=False,
    )
```

```python
import functools

import jax
import jax.numpy as jnp
from jax import lax
from jax.experimental import pallas as pl
from jax.experimental.pallas import tpu as pltpu
from jax.sharding import PartitionSpec as P

ITERS = 6
SUB = 3
ADVECT = 0.3
VERTICAL = 0.1
PARTS = 16
LOCAL = 32
LEVELS = 4
ROWS = 32
LANES = 128
MEMBERS = 512
NOBS = 512
CHUNKS = 4
WIDE = 256
PITCH = 40
MESH = pl.DeviceIdType.MESH
F32 = jnp.float32
BF16 = jnp.bfloat16


def row_ids():
    return lax.broadcasted_iota(jnp.int32, (8, LANES), 0)


def place(tiles, source, target):
    first, last = source // 8, (source + 2) // 8
    shift = (target - source) % 8
    out = pltpu.roll(tiles[first], shift, 0) if shift else tiles[first]
    if last != first:
        other = pltpu.roll(tiles[last], shift, 0) if shift else tiles[last]
        out = jnp.where(row_ids() >= target + 8 * last - source, other, out)
    return out


def pack(pieces, base):
    rows = row_ids()
    out = []
    for block in range(3):
        acc = jnp.zeros((8, LANES), F32)
        for number, piece in enumerate(pieces):
            low, high = 3 * number - 8 * block, 3 * number + 3 - 8 * block
            if high <= 0 or low >= 8:
                continue
            shift = (3 * number - base) % 8
            moved = pltpu.roll(piece, shift, 0) if shift else piece
            acc = jnp.where((rows >= low) & (rows < high), moved, acc)
        out.append(acc)
    return out


def windows(above, upper, lower, below, step):
    rows = row_ids()
    shift = 2 - step
    top = jnp.where(rows < shift, pltpu.roll(above, shift, 0), pltpu.roll(upper, shift, 0))
    shift = 6 - step
    low = jnp.where(rows < shift, pltpu.roll(lower, shift, 0), pltpu.roll(below, shift, 0))
    return jnp.concatenate([top, low], axis=0)


def coefficients(coef, dif_ref, rows):
    lane = lax.broadcasted_iota(jnp.int32, (rows, LANES), 1)
    for level in range(LEVELS):
        dif = dif_ref[level]
        coef[0, level] = 1.0 - ADVECT - 2.0 * VERTICAL - 4.0 * dif
        coef[1, level] = dif + ADVECT
        coef[2, level] = dif
        coef[3, level] = jnp.where(lane == 0, 0.0, dif)
        coef[4, level] = jnp.where(lane == LANES - 1, 0.0, dif)


def column(states, level):
    near = [states[n] for n in (level - 1, level + 1) if 0 <= n < LEVELS]
    return near[0] + near[1] if len(near) == 2 else near[0]


def substep(coef, level, state, west, east, vertical):
    return (
        coef[0, level] * state
        + coef[1, level] * west
        + coef[2, level] * east
        + coef[3, level] * pltpu.roll(state, 1, 1)
        + coef[4, level] * pltpu.roll(state, LANES - 1, 1)
        + VERTICAL * vertical
    )


def kernel(
    ens_hbm, dif_hbm, cells_hbm, values_hbm, weights_hbm, out_ref,
    ens, dif_ref, cells_ref, values_ref, weights_ref, up_send, down_send, top_halo, low_halo, coef, edge_coef, edge_dif, turn,
    oc, hot, cell_send, cell_recv, pred_send, pred_recv,
    ymat, zmat, mmat, root, drive, back_send, back_recv,
    load_sem, halo_ssem, halo_rsem, oc_ssem, oc_rsem, pred_ssem, pred_rsem,
    cell_ssem, cell_rsem, back_ssem, back_rsem,
):
    me = lax.axis_index("mem")
    tile = lax.axis_index("tile")
    tiles = lax.axis_size("tile")
    right, left = lax.rem(tile + 1, tiles), lax.rem(tile + tiles - 1, tiles)

    half_count = LOCAL // 2
    loads = [
        pltpu.make_async_copy(source, target, load_sem.at[number])
        for number, (source, target) in enumerate(
            [
                (dif_hbm, dif_ref),
                (ens_hbm.at[0:half_count], ens.at[0:half_count]),
                (ens_hbm.at[half_count:LOCAL], ens.at[half_count:LOCAL]),
                (cells_hbm, cells_ref),
                (values_hbm, values_ref),
                (weights_hbm, weights_ref),
            ]
        )
    ]
    for load in loads:
        load.start()
    barrier = pltpu.get_barrier_semaphore()
    for offset in range(1, PARTS):
        pl.semaphore_signal(
            barrier, inc=1, device_id={"mem": lax.rem(me + offset, PARTS)}, device_id_type=MESH
        )
    for other in (left, right):
        pl.semaphore_signal(barrier, inc=1, device_id={"tile": other}, device_id_type=MESH)
    loads[0].wait()
    coefficients(coef, dif_ref, ROWS)

    def inner_pair(pair, carry):
        for half in range(2):
            member = 2 * pair + half
            states = [ens[member, level] for level in range(LEVELS)]
            for repeat in range(SUB):
                states = [
                    substep(
                        coef, level, states[level],
                        pltpu.roll(states[level], 1, 0),
                        pltpu.roll(states[level], ROWS - 1, 0),
                        column(states, level),
                    )
                    for level in range(LEVELS)
                ]
            for level in range(LEVELS):
                for block in range(ROWS // 8):
                    first = (level * ROWS + 8 * block) * PITCH
                    turn[pl.ds(first + member, 8, stride=PITCH), :] = states[level][
                        8 * block : 8 * block + 8
                    ]
        return carry

    def to_cells(part, low, count):
        for chunk in range(CHUNKS):
            for half in range(2):
                first = pl.multiple_of((part * 8 + 2 * chunk + half) * PITCH + low, 8)
                cell_send[part, chunk, low : low + count, half * LANES : (half + 1) * LANES] = (
                    turn[pl.ds(first, count), :].astype(BF16)
                )

    def inner_cells(low, number, carry):
        to_cells(4 * (number // 2) + 1 + lax.rem(number, 2), low, half_count)
        return carry

    loads[1].wait()
    lax.fori_loop(0, half_count // 2, inner_pair, 0)
    lax.fori_loop(0, PARTS // 2, functools.partial(inner_cells, 0), 0)
    loads[2].wait()

    def pack_pair(pair, carry):
        tops, lows = [], []
        for half in range(2):
            for level in range(LEVELS):
                tops.append(ens[2 * pair + half, level, 0:8, :])
                lows.append(ens[2 * pair + half, level, ROWS - 8 : ROWS, :])
        for block, value in enumerate(pack(tops, 0)):
            up_send[pair, 8 * block : 8 * block + 8, :] = value
        for block, value in enumerate(pack(lows, 5)):
            down_send[pair, 8 * block : 8 * block + 8, :] = value
        return carry

    lax.fori_loop(0, LOCAL // 2, pack_pair, 0)
    tops = [dif_ref[level, 0:8, :] for level in range(LEVELS)]
    lows = [dif_ref[level, ROWS - 8 : ROWS, :] for level in range(LEVELS)]
    for block, value in enumerate(pack(tops, 0)):
        up_send[LOCAL // 2, 8 * block : 8 * block + 8, :] = value
    for block, value in enumerate(pack(lows, 5)):
        down_send[LOCAL // 2, 8 * block : 8 * block + 8, :] = value

    pl.semaphore_wait(barrier, PARTS + 1)

    def remote(source, target, ssem, rsem, device):
        return pltpu.make_async_remote_copy(
            src_ref=source, dst_ref=target, send_sem=ssem, recv_sem=rsem,
            device_id=device, device_id_type=MESH,
        )

    def oc_copy(offset):
        return remote(
            cells_ref.at[0], oc.at[me], oc_ssem.at[offset], oc_rsem.at[offset],
            {"mem": lax.rem(me + offset, PARTS)},
        )

    def pred_copy(offset):
        other = lax.rem(me + offset, PARTS)
        return remote(
            pred_send.at[other], pred_recv.at[me], pred_ssem.at[offset], pred_rsem.at[offset],
            {"mem": other},
        )

    def cell_copy(chunk, offset):
        other = lax.rem(me + offset, PARTS)
        return remote(
            cell_send.at[other, chunk], cell_recv.at[chunk, me],
            cell_ssem.at[chunk, offset], cell_rsem.at[chunk, offset], {"mem": other},
        )

    def back_copy(chunk, offset):
        other = lax.rem(me + offset, PARTS)
        return remote(
            back_send.at[chunk, other], back_recv.at[chunk, me],
            back_ssem.at[chunk, offset], back_rsem.at[chunk, offset], {"mem": other},
        )

    def each(action):
        def step(offset, carry):
            action(offset)
            return carry

        lax.fori_loop(1, PARTS, step, 0)

    to_right = remote(down_send, top_halo, halo_ssem.at[0], halo_rsem.at[0], {"tile": right})
    to_left = remote(up_send, low_halo, halo_ssem.at[1], halo_rsem.at[1], {"tile": left})
    to_right.start()
    to_left.start()
    for load in loads[3:]:
        load.wait()
    each(lambda offset: oc_copy(offset).start())
    oc[me] = cells_ref[0]


    def inner_send(low, number, carry):
        turned = lax.rem(number + lax.div(me + 1, 2), PARTS // 2)
        part = 4 * lax.div(turned, 2) + 1 + lax.rem(turned, 2)
        offset = lax.rem(part - me + PARTS, PARTS)

        @pl.when(offset > 0)
        def _():
            for chunk in range(CHUNKS):
                remote(
                    cell_send.at[part, chunk, pl.ds(low, half_count)],
                    cell_recv.at[chunk, me, pl.ds(low, half_count)],
                    cell_ssem.at[chunk, offset], cell_rsem.at[chunk, offset], {"mem": part},
                ).start()

        return carry

    lax.fori_loop(0, PARTS // 2, functools.partial(inner_send, 0), 0)
    lax.fori_loop(half_count // 2, LOCAL // 2, inner_pair, 0)
    lax.fori_loop(0, PARTS // 2, functools.partial(inner_cells, half_count), 0)
    lax.fori_loop(0, PARTS // 2, functools.partial(inner_send, half_count), 0)

    each(lambda offset: oc_copy(offset).wait())
    within = lax.broadcasted_iota(jnp.int32, (WIDE, NOBS), 0)

    def mark(part, carry):
        index = jnp.bitwise_and(oc[part], WIDE - 1)
        hot[part] = jnp.where(within == index, 1.0, 0.0).astype(BF16)
        return carry

    lax.fori_loop(0, PARTS, mark, 0)

    top_mask = jnp.where(tile > 0, 1.0, 0.0).astype(F32)
    low_mask = jnp.where(tile < tiles - 1, 1.0, 0.0).astype(F32)
    to_right.wait()
    to_left.wait()
    extra = [
        [halo[LOCAL // 2, 8 * block : 8 * block + 8, :] for block in range(3)]
        for halo in (top_halo, low_halo)
    ]
    for level in range(LEVELS):
        edge_dif[level] = windows(
            place(extra[0], 3 * level, 5), dif_ref[level, 0:8],
            dif_ref[level, ROWS - 8 : ROWS], place(extra[1], 3 * level, 0), 0,
        )
    coefficients(edge_coef, edge_dif, 16)
    edge_row = lax.broadcasted_iota(jnp.int32, (16, LANES), 0)
    edge_mask = jnp.where(edge_row < 2, top_mask, jnp.where(edge_row >= 14, low_mask, 1.0))

    edge_top = edge_row == 0
    edge_low = edge_row == 15
    rows = row_ids()

    def moved(tiles, source, target, count):
        first, last = source // 8, (source + count - 1) // 8
        shift = (target - source) % 8
        pieces = [
            pltpu.roll(tiles[n], shift, 0) if shift else tiles[n] for n in (first, last)[: 1 + (last > first)]
        ]
        if len(pieces) == 1:
            return pieces[0]
        return jnp.where(rows >= target + 8 * last - source, pieces[1], pieces[0])

    def edge_group(group, carry):
        members = range(4)
        states, wests, easts = {}, {}, {}
        for number in members:
            pair, half = 2 * group + number // 2, number % 2
            above = [top_halo[pair, 8 * n : 8 * n + 8, :] for n in range(3)]
            below = [low_halo[pair, 8 * n : 8 * n + 8, :] for n in range(3)]
            for level in range(LEVELS):
                at = 3 * (LEVELS * half + level)
                block = (2 * pair + half, level)
                upper, lower = ens[(*block, slice(0, 8))], ens[(*block, slice(ROWS - 8, ROWS))]
                top = jnp.where(
                    rows < 2, moved(above, at + 1, 0, 2) * top_mask, pltpu.roll(upper, 2, 0)
                )
                low = jnp.where(
                    rows < 6, pltpu.roll(lower, 6, 0), moved(below, at, 6, 2) * low_mask
                )
                state = jnp.concatenate([top, low], axis=0)
                first = moved(above, at, 0, 1) * top_mask
                last = moved(below, at + 2, 7, 1) * low_mask
                states[number, level] = state
                wests[number, level] = jnp.where(
                    edge_top, jnp.concatenate([first, low], axis=0), pltpu.roll(state, 1, 0)
                )
                easts[number, level] = jnp.where(
                    edge_low, jnp.concatenate([top, last], axis=0), pltpu.roll(state, 15, 0)
                )
        for repeat in range(SUB):
            updated = {}
            for number in members:
                own = [states[number, level] for level in range(LEVELS)]
                for level in range(LEVELS):
                    west = pltpu.roll(own[level], 1, 0) if repeat else wests[number, level]
                    east = pltpu.roll(own[level], 15, 0) if repeat else easts[number, level]
                    value = substep(edge_coef, level, own[level], west, east, column(own, level))
                    updated[number, level] = value * edge_mask if repeat < SUB - 1 else value
            states = updated
        for number in members:
            for level in range(LEVELS):
                first = level * ROWS * PITCH + 4 * group + number
                value = states[number, level]
                turn[pl.ds(first, 3, stride=PITCH), :] = value[2:5]
                turn[pl.ds(first + (ROWS - 3) * PITCH, 3, stride=PITCH), :] = value[11:14]
        return carry

    lax.fori_loop(0, LOCAL // 4, edge_group, 0)

    def edge_cells(number, carry):
        to_cells(4 * (number // 2) + 3 * lax.rem(number, 2), 0, LOCAL)
        return carry

    lax.fori_loop(0, PARTS // 2, edge_cells, 0)

    def order(number):
        half = lax.div(number + 1, 2)
        return jnp.where(lax.rem(number, 2) == 0, PARTS // 2 + half, PARTS // 2 - half)

    def gather(number, carry):
        part = lax.rem(me + order(number), PARTS)
        group = jnp.broadcast_to(jnp.right_shift(oc[part], 8), (LOCAL, NOBS))
        pieces = []
        for step in (PARTS - 1, 0, 1):
            other = lax.rem(part + step, PARTS)
            for chunk in range(CHUNKS):
                pieces.append(cell_send[other, chunk])
        found = jnp.dot(jnp.concatenate(pieces, axis=0), hot[part], preferred_element_type=F32)
        total = jnp.zeros((LOCAL, NOBS), F32)
        for piece in range(3 * CHUNKS):
            total += jnp.where(
                group == piece, found[LOCAL * piece : LOCAL * piece + LOCAL], 0.0
            )
        pred_send[part] = total.astype(BF16)
        pl.when(number > 0)(lambda: pred_copy(order(number - 1)).start())
        return carry

    lax.fori_loop(0, PARTS, gather, 0)
    for chunk in range(CHUNKS):
        def edge_send(number, carry):
            turned = lax.rem(number + lax.div(me + 1, 2), PARTS // 2)
            part = 4 * lax.div(turned, 2) + 3 * lax.rem(turned, 2)
            offset = lax.rem(part - me + PARTS, PARTS)
            pl.when(offset > 0)(lambda: cell_copy(chunk, offset).start())
            return carry

        lax.fori_loop(0, PARTS // 2, edge_send, 0)
        cell_recv[chunk, me] = cell_send[me, chunk]
    pred_recv[me] = pred_send[me]

    each(lambda offset: pred_copy(offset).wait())
    weights, values = weights_ref[0], values_ref[0]
    total = jnp.zeros((1, NOBS), F32)
    for part in range(PARTS):
        total += jnp.sum(pred_recv[part].astype(F32), axis=0, keepdims=True)
    pmean = total * (1.0 / MEMBERS)
    pull = weights * (values - pmean)
    for part in range(PARTS):
        rows = slice(LOCAL * part, LOCAL * part + LOCAL)
        ppert = pred_recv[part].astype(F32) - pmean
        ymat[rows, :] = (ppert * weights).astype(BF16)
        zmat[rows, :] = ppert.astype(BF16)
        drive[rows, :] = jnp.sum(ppert * pull, axis=1, keepdims=True) * (1.0 / (MEMBERS - 1.0))
    gram = lax.dot_general(
        zmat[...], ymat[...], (((1,), (1,)), ((), ())), preferred_element_type=F32
    )
    eye = jnp.where(
        lax.broadcasted_iota(jnp.int32, (MEMBERS, MEMBERS), 0)
        == lax.broadcasted_iota(jnp.int32, (MEMBERS, MEMBERS), 1),
        1.0,
        0.0,
    )
    root[...] = gram * (1.0 / (MEMBERS - 1.0)) + eye
    small = jnp.where(
        lax.broadcasted_iota(jnp.int32, (LANES, LANES), 0)
        == lax.broadcasted_iota(jnp.int32, (LANES, LANES), 1),
        1.0,
        0.0,
    )
    trace = jnp.zeros((1, 1), F32)
    for block in range(MEMBERS // LANES):
        part = slice(LANES * block, LANES * block + LANES)
        diagonal = jnp.sum(root[part, part] * small, axis=1, keepdims=True)
        trace += jnp.sum(diagonal, axis=0, keepdims=True)
    scale = trace * (3.0 / MEMBERS)
    first = (root[...] * (1.0 / scale)).astype(BF16)
    ymat[...] = first
    mmat[...] = (1.5 * eye - 0.5 * first.astype(F32)).astype(BF16)
    zmat[...] = mmat[...]
    ymat[...] = jnp.dot(mmat[...], first, preferred_element_type=F32).astype(BF16)

    def newton(step, carry):
        product = jnp.dot(ymat[...], zmat[...], preferred_element_type=F32)
        mmat[...] = (1.5 * eye - 0.5 * product).astype(BF16)
        ynext = jnp.dot(mmat[...], ymat[...], preferred_element_type=F32).astype(BF16)
        znext = jnp.dot(zmat[...], mmat[...], preferred_element_type=F32).astype(BF16)
        ymat[...] = ynext
        zmat[...] = znext
        return carry

    lax.fori_loop(0, ITERS - 2, newton, 0)
    product = jnp.dot(ymat[...], zmat[...], preferred_element_type=F32)
    mmat[...] = (1.5 * eye - 0.5 * product).astype(BF16)
    root[...] = jnp.dot(zmat[...], mmat[...], preferred_element_type=F32) * (
        1.0 / jnp.sqrt(scale)
    )
    across = jnp.sum(root[...] * drive[...], axis=0, keepdims=True)
    wmean = jnp.zeros((1, MEMBERS), F32)
    for block in range(MEMBERS // LANES):
        part = slice(LANES * block, LANES * block + LANES)
        down = jnp.sum(across[:, part] * small, axis=1, keepdims=True)
        wmean += jnp.sum(root[part, :] * down, axis=0, keepdims=True)
    ymat[...] = (root[...] + wmean).astype(BF16)

    for chunk in range(CHUNKS):
        each(lambda offset: cell_copy(chunk, offset).wait())
        total = jnp.zeros((1, WIDE), F32)
        for part in range(PARTS):
            total += jnp.sum(cell_recv[chunk, part].astype(F32), axis=0, keepdims=True)
        xmean = total * (1.0 / MEMBERS)
        for part in range(PARTS):
            zmat[LOCAL * part : LOCAL * part + LOCAL, 0:WIDE] = (
                cell_recv[chunk, part].astype(F32) - xmean
            ).astype(BF16)
        update = jnp.dot(ymat[...], zmat[:, 0:WIDE], preferred_element_type=F32) + xmean
        for part in range(PARTS):
            back_send[chunk, part] = update[LOCAL * part : LOCAL * part + LOCAL].astype(BF16)
        each(lambda offset: back_copy(chunk, offset).start())
        back_recv[chunk, me] = back_send[chunk, me]

    for chunk in range(CHUNKS):
        each(lambda offset: back_copy(chunk, offset).wait())

        def from_cells(part, carry):
            for half in range(2):
                first = pl.multiple_of((part * 8 + 2 * chunk + half) * PITCH, 8)
                turn[pl.ds(first, LOCAL), :] = back_recv[
                    chunk, part, :, half * LANES : (half + 1) * LANES
                ].astype(F32)
            return carry

        lax.fori_loop(0, PARTS, from_cells, 0)

    def to_states(member, carry):
        for part in range(PARTS):
            out_ref[member, part // 4, (part % 4) * 8 : (part % 4) * 8 + 8, :] = turn[
                pl.ds(part * 8 * PITCH + member, 8, stride=PITCH), :
            ]
        return carry

    lax.fori_loop(0, LOCAL, to_states, 0)


def on_device(ensemble, diffusion, obs_cells, obs_values, obs_weights):
    vmem = pl.BlockSpec(memory_space=pltpu.VMEM)
    dma = pltpu.SemaphoreType.DMA
    halo = pltpu.VMEM((LOCAL // 2 + 1, 24, LANES), F32)
    square = pltpu.VMEM((MEMBERS, MEMBERS), BF16)
    return pl.pallas_call(
        kernel,
        name="cycle",
        out_shape=pltpu.VMEM(ensemble.shape, F32),
        in_specs=[pl.BlockSpec(memory_space=pl.ANY)] * 5,
        out_specs=vmem,
        scratch_shapes=[
            pltpu.VMEM(ensemble.shape, F32),
            pltpu.VMEM(diffusion.shape, F32),
            pltpu.VMEM(obs_cells.shape, jnp.int32),
            pltpu.VMEM(obs_values.shape, F32),
            pltpu.VMEM(obs_weights.shape, F32),
            halo, halo, halo, halo,
            pltpu.VMEM((5, LEVELS, ROWS, LANES), F32),
            pltpu.VMEM((5, LEVELS, 16, LANES), F32),
            pltpu.VMEM((LEVELS, 16, LANES), F32),
            pltpu.VMEM((LEVELS * ROWS * PITCH, LANES), F32),
            pltpu.VMEM((PARTS, 1, NOBS), jnp.int32),
            pltpu.VMEM((PARTS, WIDE, NOBS), BF16),
            pltpu.VMEM((PARTS, CHUNKS, LOCAL, WIDE), BF16),
            pltpu.VMEM((CHUNKS, PARTS, LOCAL, WIDE), BF16),
            pltpu.VMEM((PARTS, LOCAL, NOBS), BF16),
            pltpu.VMEM((PARTS, LOCAL, NOBS), BF16),
            square, square, square,
            pltpu.VMEM((MEMBERS, MEMBERS), F32),
            pltpu.VMEM((MEMBERS, 1), F32),
            pltpu.VMEM((CHUNKS, PARTS, LOCAL, WIDE), BF16),
            pltpu.VMEM((CHUNKS, PARTS, LOCAL, WIDE), BF16),
            dma((6,)), dma((2,)), dma((2,)),
            dma((PARTS,)), dma((PARTS,)), dma((PARTS,)), dma((PARTS,)),
            dma((CHUNKS, PARTS)), dma((CHUNKS, PARTS)),
            dma((CHUNKS, PARTS)), dma((CHUNKS, PARTS)),
        ],
        compiler_params=pltpu.CompilerParams(
            collective_id=0, has_side_effects=True, vmem_limit_bytes=56 * 1024 * 1024
        ),
    )(ensemble, diffusion, obs_cells, obs_values, obs_weights)


def solution(mesh):
    return jax.shard_map(
        on_device,
        mesh=mesh,
        in_specs=(
            P("mem", None, "tile", None),
            P(None, "tile", None),
            P("tile", "mem", None),
            P("tile", "mem", None),
            P("tile", "mem", None),
        ),
        out_specs=P("mem", None, "tile", None),
        check_vma=False,
    )
```

```python
import functools

import jax
import jax.numpy as jnp
from jax import lax
from jax.experimental import pallas as pl
from jax.experimental.pallas import tpu as pltpu
from jax.sharding import PartitionSpec as P

ITERS = 6
SUB = 3
ADVECT = 0.3
VERTICAL = 0.1
PARTS = 16
LOCAL = 32
LEVELS = 4
ROWS = 32
LANES = 128
MEMBERS = 512
NOBS = 512
CHUNKS = 4
WIDE = 256
PITCH = 40
MESH = pl.DeviceIdType.MESH
F32 = jnp.float32
BF16 = jnp.bfloat16


def row_ids():
    return lax.broadcasted_iota(jnp.int32, (8, LANES), 0)


def place(tiles, source, target):
    first, last = source // 8, (source + 2) // 8
    shift = (target - source) % 8
    out = pltpu.roll(tiles[first], shift, 0) if shift else tiles[first]
    if last != first:
        other = pltpu.roll(tiles[last], shift, 0) if shift else tiles[last]
        out = jnp.where(row_ids() >= target + 8 * last - source, other, out)
    return out


def pack(pieces, base):
    rows = row_ids()
    out = []
    for block in range(3):
        acc = jnp.zeros((8, LANES), F32)
        for number, piece in enumerate(pieces):
            low, high = 3 * number - 8 * block, 3 * number + 3 - 8 * block
            if high <= 0 or low >= 8:
                continue
            shift = (3 * number - base) % 8
            moved = pltpu.roll(piece, shift, 0) if shift else piece
            acc = jnp.where((rows >= low) & (rows < high), moved, acc)
        out.append(acc)
    return out


def windows(above, upper, lower, below, step):
    rows = row_ids()
    shift = 2 - step
    top = jnp.where(rows < shift, pltpu.roll(above, shift, 0), pltpu.roll(upper, shift, 0))
    shift = 6 - step
    low = jnp.where(rows < shift, pltpu.roll(lower, shift, 0), pltpu.roll(below, shift, 0))
    return jnp.concatenate([top, low], axis=0)


def coefficients(coef, dif_ref, rows):
    lane = lax.broadcasted_iota(jnp.int32, (rows, LANES), 1)
    for level in range(LEVELS):
        dif = dif_ref[level]
        coef[0, level] = 1.0 - ADVECT - 2.0 * VERTICAL - 4.0 * dif
        coef[1, level] = dif + ADVECT
        coef[2, level] = dif
        coef[3, level] = jnp.where(lane == 0, 0.0, dif)
        coef[4, level] = jnp.where(lane == LANES - 1, 0.0, dif)


def column(states, level):
    near = [states[n] for n in (level - 1, level + 1) if 0 <= n < LEVELS]
    return near[0] + near[1] if len(near) == 2 else near[0]


def substep(coef, level, state, west, east, vertical):
    return (
        coef[0, level] * state
        + coef[1, level] * west
        + coef[2, level] * east
        + coef[3, level] * pltpu.roll(state, 1, 1)
        + coef[4, level] * pltpu.roll(state, LANES - 1, 1)
        + VERTICAL * vertical
    )


def kernel(
    ens_hbm, dif_hbm, cells_hbm, values_hbm, weights_hbm, out_ref,
    ens, dif_ref, cells_ref, values_ref, weights_ref, up_send, down_send, top_halo, low_halo, coef, edge_coef, edge_dif, turn,
    oc, hot, cell_send, cell_recv, pred_send, pred_recv,
    ymat, zmat, mmat, root, drive, back_send, back_recv,
    ready, load_sem, halo_ssem, halo_rsem, oc_ssem, oc_rsem, pred_ssem, pred_rsem,
    cell_ssem, cell_rsem, back_ssem, back_rsem,
):
    me = lax.axis_index("mem")
    tile = lax.axis_index("tile")
    tiles = lax.axis_size("tile")
    right, left = lax.rem(tile + 1, tiles), lax.rem(tile + tiles - 1, tiles)

    half_count = LOCAL // 2
    loads = [
        pltpu.make_async_copy(source, target, load_sem.at[number])
        for number, (source, target) in enumerate(
            [
                (dif_hbm, dif_ref),
                (ens_hbm.at[0:half_count], ens.at[0:half_count]),
                (ens_hbm.at[half_count:LOCAL], ens.at[half_count:LOCAL]),
                (cells_hbm, cells_ref),
                (values_hbm, values_ref),
                (weights_hbm, weights_ref),
            ]
        )
    ]
    for load in loads:
        load.start()
    barrier = pltpu.get_barrier_semaphore()
    plane = lax.div(me, 2)

    def greet(offset, carry):
        other = lax.rem(me + offset, PARTS)

        @pl.when(lax.div(other, 2) >= plane)
        def _():
            pl.semaphore_signal(barrier, inc=1, device_id={"mem": other}, device_id_type=MESH)

        return carry

    lax.fori_loop(1, PARTS, greet, 0)
    for other in (left, right):
        pl.semaphore_signal(barrier, inc=1, device_id={"tile": other}, device_id_type=MESH)
    pl.semaphore_wait(barrier, 2 * plane + 3)

    def announce(other, carry):
        pl.semaphore_signal(
            ready.at[plane], inc=1, device_id={"mem": other}, device_id_type=MESH
        )
        return carry

    lax.fori_loop(0, 2 * plane, announce, 0)

    def remote(source, target, ssem, rsem, device):
        return pltpu.make_async_remote_copy(
            src_ref=source, dst_ref=target, send_sem=ssem, recv_sem=rsem,
            device_id=device, device_id_type=MESH,
        )

    def oc_copy(offset):
        return remote(
            cells_ref.at[0], oc.at[me], oc_ssem.at[offset], oc_rsem.at[offset],
            {"mem": lax.rem(me + offset, PARTS)},
        )

    def pred_copy(offset):
        other = lax.rem(me + offset, PARTS)
        return remote(
            pred_send.at[other], pred_recv.at[me], pred_ssem.at[offset], pred_rsem.at[offset],
            {"mem": other},
        )

    def cell_copy(chunk, offset):
        other = lax.rem(me + offset, PARTS)
        return remote(
            cell_send.at[other, chunk], cell_recv.at[chunk, me],
            cell_ssem.at[chunk, offset], cell_rsem.at[chunk, offset], {"mem": other},
        )

    def back_copy(chunk, offset):
        other = lax.rem(me + offset, PARTS)
        return remote(
            back_send.at[chunk, other], back_recv.at[chunk, me],
            back_ssem.at[chunk, offset], back_rsem.at[chunk, offset], {"mem": other},
        )

    def each(action):
        def step(offset, carry):
            action(offset)
            return carry

        lax.fori_loop(1, PARTS, step, 0)

    to_right = remote(down_send, top_halo, halo_ssem.at[0], halo_rsem.at[0], {"tile": right})
    to_left = remote(up_send, low_halo, halo_ssem.at[1], halo_rsem.at[1], {"tile": left})
    for load in loads[3:]:
        load.wait()
    oc[me] = cells_ref[0]

    def oc_early(offset):
        pl.when(lax.div(lax.rem(me + offset, PARTS), 2) <= plane)(
            lambda: oc_copy(offset).start()
        )

    each(oc_early)
    for load in loads[:3]:
        load.wait()

    def pack_pair(pair, carry):
        tops, lows = [], []
        for half in range(2):
            for level in range(LEVELS):
                tops.append(ens[2 * pair + half, level, 0:8, :])
                lows.append(ens[2 * pair + half, level, ROWS - 8 : ROWS, :])
        for block, value in enumerate(pack(tops, 0)):
            up_send[pair, 8 * block : 8 * block + 8, :] = value
        for block, value in enumerate(pack(lows, 5)):
            down_send[pair, 8 * block : 8 * block + 8, :] = value
        return carry

    lax.fori_loop(0, LOCAL // 2, pack_pair, 0)
    tops = [dif_ref[level, 0:8, :] for level in range(LEVELS)]
    lows = [dif_ref[level, ROWS - 8 : ROWS, :] for level in range(LEVELS)]
    for block, value in enumerate(pack(tops, 0)):
        up_send[LOCAL // 2, 8 * block : 8 * block + 8, :] = value
    for block, value in enumerate(pack(lows, 5)):
        down_send[LOCAL // 2, 8 * block : 8 * block + 8, :] = value
    to_right.start()
    to_left.start()

    coefficients(coef, dif_ref, ROWS)

    def inner_pair(pair, carry):
        for half in range(2):
            member = 2 * pair + half
            states = [ens[member, level] for level in range(LEVELS)]
            for repeat in range(SUB):
                states = [
                    substep(
                        coef, level, states[level],
                        pltpu.roll(states[level], 1, 0),
                        pltpu.roll(states[level], ROWS - 1, 0),
                        column(states, level),
                    )
                    for level in range(LEVELS)
                ]
            for level in range(LEVELS):
                for block in range(ROWS // 8):
                    first = (level * ROWS + 8 * block) * PITCH
                    turn[pl.ds(first + member, 8, stride=PITCH), :] = states[level][
                        8 * block : 8 * block + 8
                    ]
        return carry

    def to_cells(part, low, count):
        for chunk in range(CHUNKS):
            for half in range(2):
                first = pl.multiple_of((part * 8 + 2 * chunk + half) * PITCH + low, 8)
                cell_send[part, chunk, low : low + count, half * LANES : (half + 1) * LANES] = (
                    turn[pl.ds(first, count), :].astype(BF16)
                )

    def inner_cells(low, number, carry):
        to_cells(4 * (number // 2) + 1 + lax.rem(number, 2), low, half_count)
        return carry

    lax.fori_loop(0, half_count // 2, inner_pair, 0)
    lax.fori_loop(0, PARTS // 2, functools.partial(inner_cells, 0), 0)

    def inner_send(low, number, carry):
        turned = lax.rem(number + lax.div(me + 1, 2), PARTS // 2)
        part = 4 * lax.div(turned, 2) + 1 + lax.rem(turned, 2)
        offset = lax.rem(part - me + PARTS, PARTS)

        @pl.when((offset > 0) & (lax.div(part, 2) <= plane))
        def _():
            for chunk in range(CHUNKS):
                remote(
                    cell_send.at[part, chunk, pl.ds(low, half_count)],
                    cell_recv.at[chunk, me, pl.ds(low, half_count)],
                    cell_ssem.at[chunk, offset], cell_rsem.at[chunk, offset], {"mem": part},
                ).start()

        return carry

    lax.fori_loop(0, PARTS // 2, functools.partial(inner_send, 0), 0)
    lax.fori_loop(half_count // 2, LOCAL // 2, inner_pair, 0)
    lax.fori_loop(0, PARTS // 2, functools.partial(inner_cells, half_count), 0)
    lax.fori_loop(0, PARTS // 2, functools.partial(inner_send, half_count), 0)

    def later(number, carry):
        @pl.when(number > plane)
        def _():
            pl.semaphore_wait(ready.at[number], 2)
            for part in (2 * number, 2 * number + 1):
                oc_copy(lax.rem(part - me + PARTS, PARTS)).start()
            part = 2 * number + 1 - lax.rem(number, 2)
            for chunk in range(CHUNKS):
                cell_copy(chunk, lax.rem(part - me + PARTS, PARTS)).start()

        return carry

    lax.fori_loop(1, PARTS // 2, later, 0)

    each(lambda offset: oc_copy(offset).wait())
    within = lax.broadcasted_iota(jnp.int32, (WIDE, NOBS), 0)

    def mark(part, carry):
        index = jnp.bitwise_and(oc[part], WIDE - 1)
        hot[part] = jnp.where(within == index, 1.0, 0.0).astype(BF16)
        return carry

    lax.fori_loop(0, PARTS, mark, 0)

    top_mask = jnp.where(tile > 0, 1.0, 0.0).astype(F32)
    low_mask = jnp.where(tile < tiles - 1, 1.0, 0.0).astype(F32)
    to_right.wait()
    to_left.wait()
    extra = [
        [halo[LOCAL // 2, 8 * block : 8 * block + 8, :] for block in range(3)]
        for halo in (top_halo, low_halo)
    ]
    for level in range(LEVELS):
        edge_dif[level] = windows(
            place(extra[0], 3 * level, 5), dif_ref[level, 0:8],
            dif_ref[level, ROWS - 8 : ROWS], place(extra[1], 3 * level, 0), 0,
        )
    coefficients(edge_coef, edge_dif, 16)
    edge_row = lax.broadcasted_iota(jnp.int32, (16, LANES), 0)
    edge_mask = jnp.where(edge_row < 2, top_mask, jnp.where(edge_row >= 14, low_mask, 1.0))

    edge_top = edge_row == 0
    edge_low = edge_row == 15
    rows = row_ids()

    def moved(tiles, source, target, count):
        first, last = source // 8, (source + count - 1) // 8
        shift = (target - source) % 8
        pieces = [
            pltpu.roll(tiles[n], shift, 0) if shift else tiles[n] for n in (first, last)[: 1 + (last > first)]
        ]
        if len(pieces) == 1:
            return pieces[0]
        return jnp.where(rows >= target + 8 * last - source, pieces[1], pieces[0])

    def edge_group(group, carry):
        members = range(4)
        states, wests, easts = {}, {}, {}
        for number in members:
            pair, half = 2 * group + number // 2, number % 2
            above = [top_halo[pair, 8 * n : 8 * n + 8, :] for n in range(3)]
            below = [low_halo[pair, 8 * n : 8 * n + 8, :] for n in range(3)]
            for level in range(LEVELS):
                at = 3 * (LEVELS * half + level)
                block = (2 * pair + half, level)
                upper, lower = ens[(*block, slice(0, 8))], ens[(*block, slice(ROWS - 8, ROWS))]
                top = jnp.where(
                    rows < 2, moved(above, at + 1, 0, 2) * top_mask, pltpu.roll(upper, 2, 0)
                )
                low = jnp.where(
                    rows < 6, pltpu.roll(lower, 6, 0), moved(below, at, 6, 2) * low_mask
                )
                state = jnp.concatenate([top, low], axis=0)
                first = moved(above, at, 0, 1) * top_mask
                last = moved(below, at + 2, 7, 1) * low_mask
                states[number, level] = state
                wests[number, level] = jnp.where(
                    edge_top, jnp.concatenate([first, low], axis=0), pltpu.roll(state, 1, 0)
                )
                easts[number, level] = jnp.where(
                    edge_low, jnp.concatenate([top, last], axis=0), pltpu.roll(state, 15, 0)
                )
        for repeat in range(SUB):
            updated = {}
            for number in members:
                own = [states[number, level] for level in range(LEVELS)]
                for level in range(LEVELS):
                    west = pltpu.roll(own[level], 1, 0) if repeat else wests[number, level]
                    east = pltpu.roll(own[level], 15, 0) if repeat else easts[number, level]
                    value = substep(edge_coef, level, own[level], west, east, column(own, level))
                    updated[number, level] = value * edge_mask if repeat < SUB - 1 else value
            states = updated
        for number in members:
            for level in range(LEVELS):
                first = level * ROWS * PITCH + 4 * group + number
                value = states[number, level]
                turn[pl.ds(first, 3, stride=PITCH), :] = value[2:5]
                turn[pl.ds(first + (ROWS - 3) * PITCH, 3, stride=PITCH), :] = value[11:14]
        return carry

    lax.fori_loop(0, LOCAL // 4, edge_group, 0)

    def edge_cells(number, carry):
        to_cells(4 * (number // 2) + 3 * lax.rem(number, 2), 0, LOCAL)
        return carry

    lax.fori_loop(0, PARTS // 2, edge_cells, 0)

    def order(number):
        half = lax.div(number + 1, 2)
        return jnp.where(lax.rem(number, 2) == 0, PARTS // 2 + half, PARTS // 2 - half)

    def gather(number, carry):
        part = lax.rem(me + order(number), PARTS)
        group = jnp.broadcast_to(jnp.right_shift(oc[part], 8), (LOCAL, NOBS))
        pieces = []
        for step in (PARTS - 1, 0, 1):
            other = lax.rem(part + step, PARTS)
            for chunk in range(CHUNKS):
                pieces.append(cell_send[other, chunk])
        found = jnp.dot(jnp.concatenate(pieces, axis=0), hot[part], preferred_element_type=F32)
        total = jnp.zeros((LOCAL, NOBS), F32)
        for piece in range(3 * CHUNKS):
            total += jnp.where(
                group == piece, found[LOCAL * piece : LOCAL * piece + LOCAL], 0.0
            )
        pred_send[part] = total.astype(BF16)
        pl.when(number > 0)(lambda: pred_copy(order(number - 1)).start())
        return carry

    lax.fori_loop(0, PARTS, gather, 0)
    for chunk in range(CHUNKS):
        def edge_send(number, carry):
            turned = lax.rem(number + lax.div(me + 1, 2), PARTS // 2)
            part = 4 * lax.div(turned, 2) + 3 * lax.rem(turned, 2)
            offset = lax.rem(part - me + PARTS, PARTS)
            pl.when(offset > 0)(lambda: cell_copy(chunk, offset).start())
            return carry

        lax.fori_loop(0, PARTS // 2, edge_send, 0)
        cell_recv[chunk, me] = cell_send[me, chunk]
    pred_recv[me] = pred_send[me]

    each(lambda offset: pred_copy(offset).wait())
    weights, values = weights_ref[0], values_ref[0]
    total = jnp.zeros((1, NOBS), F32)
    for part in range(PARTS):
        total += jnp.sum(pred_recv[part].astype(F32), axis=0, keepdims=True)
    pmean = total * (1.0 / MEMBERS)
    pull = weights * (values - pmean)
    for part in range(PARTS):
        rows = slice(LOCAL * part, LOCAL * part + LOCAL)
        ppert = pred_recv[part].astype(F32) - pmean
        ymat[rows, :] = (ppert * weights).astype(BF16)
        zmat[rows, :] = ppert.astype(BF16)
        drive[rows, :] = jnp.sum(ppert * pull, axis=1, keepdims=True) * (1.0 / (MEMBERS - 1.0))
    gram = lax.dot_general(
        zmat[...], ymat[...], (((1,), (1,)), ((), ())), preferred_element_type=F32
    )
    eye = jnp.where(
        lax.broadcasted_iota(jnp.int32, (MEMBERS, MEMBERS), 0)
        == lax.broadcasted_iota(jnp.int32, (MEMBERS, MEMBERS), 1),
        1.0,
        0.0,
    )
    root[...] = gram * (1.0 / (MEMBERS - 1.0)) + eye
    small = jnp.where(
        lax.broadcasted_iota(jnp.int32, (LANES, LANES), 0)
        == lax.broadcasted_iota(jnp.int32, (LANES, LANES), 1),
        1.0,
        0.0,
    )
    trace = jnp.zeros((1, 1), F32)
    for block in range(MEMBERS // LANES):
        part = slice(LANES * block, LANES * block + LANES)
        diagonal = jnp.sum(root[part, part] * small, axis=1, keepdims=True)
        trace += jnp.sum(diagonal, axis=0, keepdims=True)
    scale = trace * (3.0 / MEMBERS)
    first = (root[...] * (1.0 / scale)).astype(BF16)
    ymat[...] = first
    mmat[...] = (1.5 * eye - 0.5 * first.astype(F32)).astype(BF16)
    zmat[...] = mmat[...]
    ymat[...] = jnp.dot(mmat[...], first, preferred_element_type=F32).astype(BF16)

    def newton(step, carry):
        product = jnp.dot(ymat[...], zmat[...], preferred_element_type=F32)
        mmat[...] = (1.5 * eye - 0.5 * product).astype(BF16)
        ynext = jnp.dot(mmat[...], ymat[...], preferred_element_type=F32).astype(BF16)
        znext = jnp.dot(zmat[...], mmat[...], preferred_element_type=F32).astype(BF16)
        ymat[...] = ynext
        zmat[...] = znext
        return carry

    lax.fori_loop(0, ITERS - 2, newton, 0)
    product = jnp.dot(ymat[...], zmat[...], preferred_element_type=F32)
    mmat[...] = (1.5 * eye - 0.5 * product).astype(BF16)
    root[...] = jnp.dot(zmat[...], mmat[...], preferred_element_type=F32) * (
        1.0 / jnp.sqrt(scale)
    )
    across = jnp.sum(root[...] * drive[...], axis=0, keepdims=True)
    wmean = jnp.zeros((1, MEMBERS), F32)
    for block in range(MEMBERS // LANES):
        part = slice(LANES * block, LANES * block + LANES)
        down = jnp.sum(across[:, part] * small, axis=1, keepdims=True)
        wmean += jnp.sum(root[part, :] * down, axis=0, keepdims=True)
    ymat[...] = (root[...] + wmean).astype(BF16)

    for chunk in range(CHUNKS):
        each(lambda offset: cell_copy(chunk, offset).wait())
        total = jnp.zeros((1, WIDE), F32)
        for part in range(PARTS):
            total += jnp.sum(cell_recv[chunk, part].astype(F32), axis=0, keepdims=True)
        xmean = total * (1.0 / MEMBERS)
        for part in range(PARTS):
            zmat[LOCAL * part : LOCAL * part + LOCAL, 0:WIDE] = (
                cell_recv[chunk, part].astype(F32) - xmean
            ).astype(BF16)
        update = jnp.dot(ymat[...], zmat[:, 0:WIDE], preferred_element_type=F32) + xmean
        for part in range(PARTS):
            back_send[chunk, part] = update[LOCAL * part : LOCAL * part + LOCAL].astype(BF16)
        each(lambda offset: back_copy(chunk, offset).start())
        back_recv[chunk, me] = back_send[chunk, me]

    for chunk in range(CHUNKS):
        each(lambda offset: back_copy(chunk, offset).wait())

        def from_cells(part, carry):
            for half in range(2):
                first = pl.multiple_of((part * 8 + 2 * chunk + half) * PITCH, 8)
                turn[pl.ds(first, LOCAL), :] = back_recv[
                    chunk, part, :, half * LANES : (half + 1) * LANES
                ].astype(F32)
            return carry

        lax.fori_loop(0, PARTS, from_cells, 0)

    def to_states(member, carry):
        for part in range(PARTS):
            out_ref[member, part // 4, (part % 4) * 8 : (part % 4) * 8 + 8, :] = turn[
                pl.ds(part * 8 * PITCH + member, 8, stride=PITCH), :
            ]
        return carry

    lax.fori_loop(0, LOCAL, to_states, 0)


def on_device(ensemble, diffusion, obs_cells, obs_values, obs_weights):
    vmem = pl.BlockSpec(memory_space=pltpu.VMEM)
    dma = pltpu.SemaphoreType.DMA
    halo = pltpu.VMEM((LOCAL // 2 + 1, 24, LANES), F32)
    square = pltpu.VMEM((MEMBERS, MEMBERS), BF16)
    return pl.pallas_call(
        kernel,
        name="cycle",
        out_shape=pltpu.VMEM(ensemble.shape, F32),
        in_specs=[pl.BlockSpec(memory_space=pl.ANY)] * 5,
        out_specs=vmem,
        scratch_shapes=[
            pltpu.VMEM(ensemble.shape, F32),
            pltpu.VMEM(diffusion.shape, F32),
            pltpu.VMEM(obs_cells.shape, jnp.int32),
            pltpu.VMEM(obs_values.shape, F32),
            pltpu.VMEM(obs_weights.shape, F32),
            halo, halo, halo, halo,
            pltpu.VMEM((5, LEVELS, ROWS, LANES), F32),
            pltpu.VMEM((5, LEVELS, 16, LANES), F32),
            pltpu.VMEM((LEVELS, 16, LANES), F32),
            pltpu.VMEM((LEVELS * ROWS * PITCH, LANES), F32),
            pltpu.VMEM((PARTS, 1, NOBS), jnp.int32),
            pltpu.VMEM((PARTS, WIDE, NOBS), BF16),
            pltpu.VMEM((PARTS, CHUNKS, LOCAL, WIDE), BF16),
            pltpu.VMEM((CHUNKS, PARTS, LOCAL, WIDE), BF16),
            pltpu.VMEM((PARTS, LOCAL, NOBS), BF16),
            pltpu.VMEM((PARTS, LOCAL, NOBS), BF16),
            square, square, square,
            pltpu.VMEM((MEMBERS, MEMBERS), F32),
            pltpu.VMEM((MEMBERS, 1), F32),
            pltpu.VMEM((CHUNKS, PARTS, LOCAL, WIDE), BF16),
            pltpu.VMEM((CHUNKS, PARTS, LOCAL, WIDE), BF16),
            pltpu.SemaphoreType.REGULAR((PARTS // 2,)),
            dma((6,)), dma((2,)), dma((2,)),
            dma((PARTS,)), dma((PARTS,)), dma((PARTS,)), dma((PARTS,)),
            dma((CHUNKS, PARTS)), dma((CHUNKS, PARTS)),
            dma((CHUNKS, PARTS)), dma((CHUNKS, PARTS)),
        ],
        compiler_params=pltpu.CompilerParams(
            collective_id=0, has_side_effects=True, vmem_limit_bytes=56 * 1024 * 1024
        ),
    )(ensemble, diffusion, obs_cells, obs_values, obs_weights)


def solution(mesh):
    return jax.shard_map(
        on_device,
        mesh=mesh,
        in_specs=(
            P("mem", None, "tile", None),
            P(None, "tile", None),
            P("tile", "mem", None),
            P("tile", "mem", None),
            P("tile", "mem", None),
        ),
        out_specs=P("mem", None, "tile", None),
        check_vma=False,
    )
```

```python
import functools

import jax
import jax.numpy as jnp
from jax import lax
from jax.experimental import pallas as pl
from jax.experimental.pallas import tpu as pltpu
from jax.sharding import PartitionSpec as P

ITERS = 6
SUB = 3
ADVECT = 0.3
VERTICAL = 0.1
PARTS = 16
LOCAL = 32
LEVELS = 4
ROWS = 32
LANES = 128
MEMBERS = 512
NOBS = 512
CHUNKS = 4
WIDE = 256
PITCH = 40
MESH = pl.DeviceIdType.MESH
F32 = jnp.float32
BF16 = jnp.bfloat16


def row_ids():
    return lax.broadcasted_iota(jnp.int32, (8, LANES), 0)


def place(tiles, source, target):
    first, last = source // 8, (source + 2) // 8
    shift = (target - source) % 8
    out = pltpu.roll(tiles[first], shift, 0) if shift else tiles[first]
    if last != first:
        other = pltpu.roll(tiles[last], shift, 0) if shift else tiles[last]
        out = jnp.where(row_ids() >= target + 8 * last - source, other, out)
    return out


def pack(pieces, base):
    rows = row_ids()
    out = []
    for block in range(3):
        acc = jnp.zeros((8, LANES), F32)
        for number, piece in enumerate(pieces):
            low, high = 3 * number - 8 * block, 3 * number + 3 - 8 * block
            if high <= 0 or low >= 8:
                continue
            shift = (3 * number - base) % 8
            moved = pltpu.roll(piece, shift, 0) if shift else piece
            acc = jnp.where((rows >= low) & (rows < high), moved, acc)
        out.append(acc)
    return out


def windows(above, upper, lower, below, step):
    rows = row_ids()
    shift = 2 - step
    top = jnp.where(rows < shift, pltpu.roll(above, shift, 0), pltpu.roll(upper, shift, 0))
    shift = 6 - step
    low = jnp.where(rows < shift, pltpu.roll(lower, shift, 0), pltpu.roll(below, shift, 0))
    return jnp.concatenate([top, low], axis=0)


def coefficients(coef, dif_ref, rows):
    lane = lax.broadcasted_iota(jnp.int32, (rows, LANES), 1)
    for level in range(LEVELS):
        dif = dif_ref[level]
        coef[0, level] = 1.0 - ADVECT - 2.0 * VERTICAL - 4.0 * dif
        coef[1, level] = dif + ADVECT
        coef[2, level] = dif
        coef[3, level] = jnp.where(lane == 0, 0.0, dif)
        coef[4, level] = jnp.where(lane == LANES - 1, 0.0, dif)


def column(states, level):
    near = [states[n] for n in (level - 1, level + 1) if 0 <= n < LEVELS]
    return near[0] + near[1] if len(near) == 2 else near[0]


def substep(coef, level, state, west, east, vertical):
    return (
        coef[0, level] * state
        + coef[1, level] * west
        + coef[2, level] * east
        + coef[3, level] * pltpu.roll(state, 1, 1)
        + coef[4, level] * pltpu.roll(state, LANES - 1, 1)
        + VERTICAL * vertical
    )


def kernel(
    ens_hbm, dif_hbm, cells_hbm, values_hbm, weights_hbm, out_ref,
    ens, dif_ref, cells_ref, values_ref, weights_ref, up_send, down_send, top_halo, low_halo, coef, edge_coef, edge_dif, turn,
    oc, hot, cell_send, cell_recv, pred_send, pred_recv,
    ymat, zmat, mmat, root, drive, back_send, back_recv,
    load_sem, halo_ssem, halo_rsem, oc_ssem, oc_rsem, pred_ssem, pred_rsem,
    cell_ssem, cell_rsem, back_ssem, back_rsem,
):
    me = lax.axis_index("mem")
    tile = lax.axis_index("tile")
    tiles = lax.axis_size("tile")
    right, left = lax.rem(tile + 1, tiles), lax.rem(tile + tiles - 1, tiles)

    def order(number):
        half = lax.div(number + 1, 2)
        return jnp.where(lax.rem(number, 2) == 0, PARTS // 2 + half, PARTS // 2 - half)

    def each(action):
        def step(number, carry):
            action(order(number))
            return carry

        lax.fori_loop(0, PARTS - 1, step, 0)

    half_count = LOCAL // 2
    loads = [
        pltpu.make_async_copy(source, target, load_sem.at[number])
        for number, (source, target) in enumerate(
            [
                (dif_hbm, dif_ref),
                (ens_hbm.at[0:half_count], ens.at[0:half_count]),
                (ens_hbm.at[half_count:LOCAL], ens.at[half_count:LOCAL]),
                (cells_hbm, cells_ref),
                (values_hbm, values_ref),
                (weights_hbm, weights_ref),
            ]
        )
    ]
    for load in loads:
        load.start()
    barrier = pltpu.get_barrier_semaphore()
    each(
        lambda offset: pl.semaphore_signal(
            barrier, inc=1, device_id={"mem": lax.rem(me + offset, PARTS)}, device_id_type=MESH
        )
    )
    for other in (left, right):
        pl.semaphore_signal(barrier, inc=1, device_id={"tile": other}, device_id_type=MESH)
    loads[0].wait()
    coefficients(coef, dif_ref, ROWS)

    def inner_pair(pair, carry):
        for half in range(2):
            member = 2 * pair + half
            states = [ens[member, level] for level in range(LEVELS)]
            for repeat in range(SUB):
                states = [
                    substep(
                        coef, level, states[level],
                        pltpu.roll(states[level], 1, 0),
                        pltpu.roll(states[level], ROWS - 1, 0),
                        column(states, level),
                    )
                    for level in range(LEVELS)
                ]
            for level in range(LEVELS):
                for block in range(ROWS // 8):
                    first = (level * ROWS + 8 * block) * PITCH
                    turn[pl.ds(first + member, 8, stride=PITCH), :] = states[level][
                        8 * block : 8 * block + 8
                    ]
        return carry

    def to_cells(part, low, count):
        for chunk in range(CHUNKS):
            for half in range(2):
                first = pl.multiple_of((part * 8 + 2 * chunk + half) * PITCH + low, 8)
                cell_send[part, chunk, low : low + count, half * LANES : (half + 1) * LANES] = (
                    turn[pl.ds(first, count), :].astype(BF16)
                )

    def inner_cells(low, number, carry):
        to_cells(4 * (number // 2) + 1 + lax.rem(number, 2), low, half_count)
        return carry

    loads[1].wait()
    lax.fori_loop(0, half_count // 2, inner_pair, 0)
    lax.fori_loop(0, PARTS // 2, functools.partial(inner_cells, 0), 0)
    loads[2].wait()

    def pack_pair(pair, carry):
        tops, lows = [], []
        for half in range(2):
            for level in range(LEVELS):
                tops.append(ens[2 * pair + half, level, 0:8, :])
                lows.append(ens[2 * pair + half, level, ROWS - 8 : ROWS, :])
        for block, value in enumerate(pack(tops, 0)):
            up_send[pair, 8 * block : 8 * block + 8, :] = value
        for block, value in enumerate(pack(lows, 5)):
            down_send[pair, 8 * block : 8 * block + 8, :] = value
        return carry

    lax.fori_loop(0, LOCAL // 2, pack_pair, 0)
    tops = [dif_ref[level, 0:8, :] for level in range(LEVELS)]
    lows = [dif_ref[level, ROWS - 8 : ROWS, :] for level in range(LEVELS)]
    for block, value in enumerate(pack(tops, 0)):
        up_send[LOCAL // 2, 8 * block : 8 * block + 8, :] = value
    for block, value in enumerate(pack(lows, 5)):
        down_send[LOCAL // 2, 8 * block : 8 * block + 8, :] = value

    pl.semaphore_wait(barrier, PARTS + 1)

    def remote(source, target, ssem, rsem, device):
        return pltpu.make_async_remote_copy(
            src_ref=source, dst_ref=target, send_sem=ssem, recv_sem=rsem,
            device_id=device, device_id_type=MESH,
        )

    def oc_copy(offset):
        return remote(
            cells_ref.at[0], oc.at[me], oc_ssem.at[offset], oc_rsem.at[offset],
            {"mem": lax.rem(me + offset, PARTS)},
        )

    def pred_copy(offset):
        other = lax.rem(me + offset, PARTS)
        return remote(
            pred_send.at[other], pred_recv.at[me], pred_ssem.at[offset], pred_rsem.at[offset],
            {"mem": other},
        )

    def cell_copy(chunk, offset):
        other = lax.rem(me + offset, PARTS)
        return remote(
            cell_send.at[other, chunk], cell_recv.at[chunk, me],
            cell_ssem.at[chunk, offset], cell_rsem.at[chunk, offset], {"mem": other},
        )

    def back_copy(chunk, offset):
        other = lax.rem(me + offset, PARTS)
        return remote(
            back_send.at[chunk, other], back_recv.at[chunk, me],
            back_ssem.at[chunk, offset], back_rsem.at[chunk, offset], {"mem": other},
        )

    to_right = remote(down_send, top_halo, halo_ssem.at[0], halo_rsem.at[0], {"tile": right})
    to_left = remote(up_send, low_halo, halo_ssem.at[1], halo_rsem.at[1], {"tile": left})
    to_right.start()
    to_left.start()
    for load in loads[3:]:
        load.wait()
    each(lambda offset: oc_copy(offset).start())
    oc[me] = cells_ref[0]


    def inner(part):
        return lax.rem(lax.rem(part, 4) + 1, 4) >= 2

    def inner_send(low, offset):
        part = lax.rem(me + offset, PARTS)

        @pl.when(inner(part))
        def _():
            for chunk in range(CHUNKS):
                remote(
                    cell_send.at[part, chunk, pl.ds(low, half_count)],
                    cell_recv.at[chunk, me, pl.ds(low, half_count)],
                    cell_ssem.at[chunk, offset], cell_rsem.at[chunk, offset], {"mem": part},
                ).start()

    each(functools.partial(inner_send, 0))
    lax.fori_loop(half_count // 2, LOCAL // 2, inner_pair, 0)
    lax.fori_loop(0, PARTS // 2, functools.partial(inner_cells, half_count), 0)
    each(functools.partial(inner_send, half_count))

    each(lambda offset: oc_copy(offset).wait())
    within = lax.broadcasted_iota(jnp.int32, (WIDE, NOBS), 0)

    def mark(part, carry):
        index = jnp.bitwise_and(oc[part], WIDE - 1)
        hot[part] = jnp.where(within == index, 1.0, 0.0).astype(BF16)
        return carry

    lax.fori_loop(0, PARTS, mark, 0)

    top_mask = jnp.where(tile > 0, 1.0, 0.0).astype(F32)
    low_mask = jnp.where(tile < tiles - 1, 1.0, 0.0).astype(F32)
    to_right.wait()
    to_left.wait()
    extra = [
        [halo[LOCAL // 2, 8 * block : 8 * block + 8, :] for block in range(3)]
        for halo in (top_halo, low_halo)
    ]
    for level in range(LEVELS):
        edge_dif[level] = windows(
            place(extra[0], 3 * level, 5), dif_ref[level, 0:8],
            dif_ref[level, ROWS - 8 : ROWS], place(extra[1], 3 * level, 0), 0,
        )
    coefficients(edge_coef, edge_dif, 16)
    edge_row = lax.broadcasted_iota(jnp.int32, (16, LANES), 0)
    edge_mask = jnp.where(edge_row < 2, top_mask, jnp.where(edge_row >= 14, low_mask, 1.0))

    edge_top = edge_row == 0
    edge_low = edge_row == 15
    rows = row_ids()

    def moved(tiles, source, target, count):
        first, last = source // 8, (source + count - 1) // 8
        shift = (target - source) % 8
        pieces = [
            pltpu.roll(tiles[n], shift, 0) if shift else tiles[n] for n in (first, last)[: 1 + (last > first)]
        ]
        if len(pieces) == 1:
            return pieces[0]
        return jnp.where(rows >= target + 8 * last - source, pieces[1], pieces[0])

    def edge_group(group, carry):
        members = range(4)
        states, wests, easts = {}, {}, {}
        for number in members:
            pair, half = 2 * group + number // 2, number % 2
            above = [top_halo[pair, 8 * n : 8 * n + 8, :] for n in range(3)]
            below = [low_halo[pair, 8 * n : 8 * n + 8, :] for n in range(3)]
            for level in range(LEVELS):
                at = 3 * (LEVELS * half + level)
                block = (2 * pair + half, level)
                upper, lower = ens[(*block, slice(0, 8))], ens[(*block, slice(ROWS - 8, ROWS))]
                top = jnp.where(
                    rows < 2, moved(above, at + 1, 0, 2) * top_mask, pltpu.roll(upper, 2, 0)
                )
                low = jnp.where(
                    rows < 6, pltpu.roll(lower, 6, 0), moved(below, at, 6, 2) * low_mask
                )
                state = jnp.concatenate([top, low], axis=0)
                first = moved(above, at, 0, 1) * top_mask
                last = moved(below, at + 2, 7, 1) * low_mask
                states[number, level] = state
                wests[number, level] = jnp.where(
                    edge_top, jnp.concatenate([first, low], axis=0), pltpu.roll(state, 1, 0)
                )
                easts[number, level] = jnp.where(
                    edge_low, jnp.concatenate([top, last], axis=0), pltpu.roll(state, 15, 0)
                )
        for repeat in range(SUB):
            updated = {}
            for number in members:
                own = [states[number, level] for level in range(LEVELS)]
                for level in range(LEVELS):
                    west = pltpu.roll(own[level], 1, 0) if repeat else wests[number, level]
                    east = pltpu.roll(own[level], 15, 0) if repeat else easts[number, level]
                    value = substep(edge_coef, level, own[level], west, east, column(own, level))
                    updated[number, level] = value * edge_mask if repeat < SUB - 1 else value
            states = updated
        for number in members:
            for level in range(LEVELS):
                first = level * ROWS * PITCH + 4 * group + number
                value = states[number, level]
                turn[pl.ds(first, 3, stride=PITCH), :] = value[2:5]
                turn[pl.ds(first + (ROWS - 3) * PITCH, 3, stride=PITCH), :] = value[11:14]
        return carry

    lax.fori_loop(0, LOCAL // 4, edge_group, 0)

    def edge_cells(number, carry):
        to_cells(4 * (number // 2) + 3 * lax.rem(number, 2), 0, LOCAL)
        return carry

    lax.fori_loop(0, PARTS // 2, edge_cells, 0)

    def gather(number, carry):
        part = lax.rem(me + order(number), PARTS)
        group = jnp.broadcast_to(jnp.right_shift(oc[part], 8), (LOCAL, NOBS))
        pieces = []
        for step in (PARTS - 1, 0, 1):
            other = lax.rem(part + step, PARTS)
            for chunk in range(CHUNKS):
                pieces.append(cell_send[other, chunk])
        found = jnp.dot(jnp.concatenate(pieces, axis=0), hot[part], preferred_element_type=F32)
        total = jnp.zeros((LOCAL, NOBS), F32)
        for piece in range(3 * CHUNKS):
            total += jnp.where(
                group == piece, found[LOCAL * piece : LOCAL * piece + LOCAL], 0.0
            )
        pred_send[part] = total.astype(BF16)
        pl.when(number > 0)(lambda: pred_copy(order(number - 1)).start())
        return carry

    lax.fori_loop(0, PARTS, gather, 0)
    for chunk in range(CHUNKS):
        def edge_send(offset):
            part = lax.rem(me + offset, PARTS)
            pl.when(jnp.logical_not(inner(part)))(lambda: cell_copy(chunk, offset).start())

        each(edge_send)
        cell_recv[chunk, me] = cell_send[me, chunk]
    pred_recv[me] = pred_send[me]

    each(lambda offset: pred_copy(offset).wait())
    weights, values = weights_ref[0], values_ref[0]
    total = jnp.zeros((1, NOBS), F32)
    for part in range(PARTS):
        total += jnp.sum(pred_recv[part].astype(F32), axis=0, keepdims=True)
    pmean = total * (1.0 / MEMBERS)
    pull = weights * (values - pmean)
    for part in range(PARTS):
        rows = slice(LOCAL * part, LOCAL * part + LOCAL)
        ppert = pred_recv[part].astype(F32) - pmean
        ymat[rows, :] = (ppert * weights).astype(BF16)
        zmat[rows, :] = ppert.astype(BF16)
        drive[rows, :] = jnp.sum(ppert * pull, axis=1, keepdims=True) * (1.0 / (MEMBERS - 1.0))
    gram = lax.dot_general(
        zmat[...], ymat[...], (((1,), (1,)), ((), ())), preferred_element_type=F32
    )
    eye = jnp.where(
        lax.broadcasted_iota(jnp.int32, (MEMBERS, MEMBERS), 0)
        == lax.broadcasted_iota(jnp.int32, (MEMBERS, MEMBERS), 1),
        1.0,
        0.0,
    )
    root[...] = gram * (1.0 / (MEMBERS - 1.0)) + eye
    small = jnp.where(
        lax.broadcasted_iota(jnp.int32, (LANES, LANES), 0)
        == lax.broadcasted_iota(jnp.int32, (LANES, LANES), 1),
        1.0,
        0.0,
    )
    trace = jnp.zeros((1, 1), F32)
    for block in range(MEMBERS // LANES):
        part = slice(LANES * block, LANES * block + LANES)
        diagonal = jnp.sum(root[part, part] * small, axis=1, keepdims=True)
        trace += jnp.sum(diagonal, axis=0, keepdims=True)
    scale = trace * (3.0 / MEMBERS)
    first = (root[...] * (1.0 / scale)).astype(BF16)
    ymat[...] = first
    mmat[...] = (1.5 * eye - 0.5 * first.astype(F32)).astype(BF16)
    zmat[...] = mmat[...]
    ymat[...] = jnp.dot(mmat[...], first, preferred_element_type=F32).astype(BF16)

    def newton(step, carry):
        product = jnp.dot(ymat[...], zmat[...], preferred_element_type=F32)
        mmat[...] = (1.5 * eye - 0.5 * product).astype(BF16)
        ynext = jnp.dot(mmat[...], ymat[...], preferred_element_type=F32).astype(BF16)
        znext = jnp.dot(zmat[...], mmat[...], preferred_element_type=F32).astype(BF16)
        ymat[...] = ynext
        zmat[...] = znext
        return carry

    lax.fori_loop(0, ITERS - 2, newton, 0)
    product = jnp.dot(ymat[...], zmat[...], preferred_element_type=F32)
    mmat[...] = (1.5 * eye - 0.5 * product).astype(BF16)
    root[...] = jnp.dot(zmat[...], mmat[...], preferred_element_type=F32) * (
        1.0 / jnp.sqrt(scale)
    )
    across = jnp.sum(root[...] * drive[...], axis=0, keepdims=True)
    wmean = jnp.zeros((1, MEMBERS), F32)
    for block in range(MEMBERS // LANES):
        part = slice(LANES * block, LANES * block + LANES)
        down = jnp.sum(across[:, part] * small, axis=1, keepdims=True)
        wmean += jnp.sum(root[part, :] * down, axis=0, keepdims=True)
    ymat[...] = (root[...] + wmean).astype(BF16)

    for chunk in range(CHUNKS):
        each(lambda offset: cell_copy(chunk, offset).wait())
        total = jnp.zeros((1, WIDE), F32)
        for part in range(PARTS):
            total += jnp.sum(cell_recv[chunk, part].astype(F32), axis=0, keepdims=True)
        xmean = total * (1.0 / MEMBERS)
        for part in range(PARTS):
            zmat[LOCAL * part : LOCAL * part + LOCAL, 0:WIDE] = (
                cell_recv[chunk, part].astype(F32) - xmean
            ).astype(BF16)
        update = jnp.dot(ymat[...], zmat[:, 0:WIDE], preferred_element_type=F32) + xmean
        for part in range(PARTS):
            back_send[chunk, part] = update[LOCAL * part : LOCAL * part + LOCAL].astype(BF16)
        each(lambda offset: back_copy(chunk, offset).start())
        back_recv[chunk, me] = back_send[chunk, me]

    for chunk in range(CHUNKS):
        each(lambda offset: back_copy(chunk, offset).wait())

        def from_cells(part, carry):
            for half in range(2):
                first = pl.multiple_of((part * 8 + 2 * chunk + half) * PITCH, 8)
                turn[pl.ds(first, LOCAL), :] = back_recv[
                    chunk, part, :, half * LANES : (half + 1) * LANES
                ].astype(F32)
            return carry

        lax.fori_loop(0, PARTS, from_cells, 0)

    def to_states(member, carry):
        for part in range(PARTS):
            out_ref[member, part // 4, (part % 4) * 8 : (part % 4) * 8 + 8, :] = turn[
                pl.ds(part * 8 * PITCH + member, 8, stride=PITCH), :
            ]
        return carry

    lax.fori_loop(0, LOCAL, to_states, 0)


def on_device(ensemble, diffusion, obs_cells, obs_values, obs_weights):
    vmem = pl.BlockSpec(memory_space=pltpu.VMEM)
    dma = pltpu.SemaphoreType.DMA
    halo = pltpu.VMEM((LOCAL // 2 + 1, 24, LANES), F32)
    square = pltpu.VMEM((MEMBERS, MEMBERS), BF16)
    return pl.pallas_call(
        kernel,
        name="cycle",
        out_shape=pltpu.VMEM(ensemble.shape, F32),
        in_specs=[pl.BlockSpec(memory_space=pl.ANY)] * 5,
        out_specs=vmem,
        scratch_shapes=[
            pltpu.VMEM(ensemble.shape, F32),
            pltpu.VMEM(diffusion.shape, F32),
            pltpu.VMEM(obs_cells.shape, jnp.int32),
            pltpu.VMEM(obs_values.shape, F32),
            pltpu.VMEM(obs_weights.shape, F32),
            halo, halo, halo, halo,
            pltpu.VMEM((5, LEVELS, ROWS, LANES), F32),
            pltpu.VMEM((5, LEVELS, 16, LANES), F32),
            pltpu.VMEM((LEVELS, 16, LANES), F32),
            pltpu.VMEM((LEVELS * ROWS * PITCH, LANES), F32),
            pltpu.VMEM((PARTS, 1, NOBS), jnp.int32),
            pltpu.VMEM((PARTS, WIDE, NOBS), BF16),
            pltpu.VMEM((PARTS, CHUNKS, LOCAL, WIDE), BF16),
            pltpu.VMEM((CHUNKS, PARTS, LOCAL, WIDE), BF16),
            pltpu.VMEM((PARTS, LOCAL, NOBS), BF16),
            pltpu.VMEM((PARTS, LOCAL, NOBS), BF16),
            square, square, square,
            pltpu.VMEM((MEMBERS, MEMBERS), F32),
            pltpu.VMEM((MEMBERS, 1), F32),
            pltpu.VMEM((CHUNKS, PARTS, LOCAL, WIDE), BF16),
            pltpu.VMEM((CHUNKS, PARTS, LOCAL, WIDE), BF16),
            dma((6,)), dma((2,)), dma((2,)),
            dma((PARTS,)), dma((PARTS,)), dma((PARTS,)), dma((PARTS,)),
            dma((CHUNKS, PARTS)), dma((CHUNKS, PARTS)),
            dma((CHUNKS, PARTS)), dma((CHUNKS, PARTS)),
        ],
        compiler_params=pltpu.CompilerParams(
            collective_id=0, has_side_effects=True, vmem_limit_bytes=56 * 1024 * 1024
        ),
    )(ensemble, diffusion, obs_cells, obs_values, obs_weights)


def solution(mesh):
    return jax.shard_map(
        on_device,
        mesh=mesh,
        in_specs=(
            P("mem", None, "tile", None),
            P(None, "tile", None),
            P("tile", "mem", None),
            P("tile", "mem", None),
            P("tile", "mem", None),
        ),
        out_specs=P("mem", None, "tile", None),
        check_vma=False,
    )
```

```python
import functools

import jax
import jax.numpy as jnp
from jax import lax
from jax.experimental import pallas as pl
from jax.experimental.pallas import tpu as pltpu
from jax.sharding import PartitionSpec as P

ITERS = 6
SUB = 3
ADVECT = 0.3
VERTICAL = 0.1
PARTS = 16
LOCAL = 32
LEVELS = 4
ROWS = 32
LANES = 128
MEMBERS = 512
NOBS = 512
CHUNKS = 2
WIDE = 512
SPAN = WIDE // LANES
HOT = 256
PITCH = 40
MESH = pl.DeviceIdType.MESH
F32 = jnp.float32
BF16 = jnp.bfloat16


def row_ids():
    return lax.broadcasted_iota(jnp.int32, (8, LANES), 0)


def place(tiles, source, target):
    first, last = source // 8, (source + 2) // 8
    shift = (target - source) % 8
    out = pltpu.roll(tiles[first], shift, 0) if shift else tiles[first]
    if last != first:
        other = pltpu.roll(tiles[last], shift, 0) if shift else tiles[last]
        out = jnp.where(row_ids() >= target + 8 * last - source, other, out)
    return out


def pack(pieces, base):
    rows = row_ids()
    out = []
    for block in range(3):
        acc = jnp.zeros((8, LANES), F32)
        for number, piece in enumerate(pieces):
            low, high = 3 * number - 8 * block, 3 * number + 3 - 8 * block
            if high <= 0 or low >= 8:
                continue
            shift = (3 * number - base) % 8
            moved = pltpu.roll(piece, shift, 0) if shift else piece
            acc = jnp.where((rows >= low) & (rows < high), moved, acc)
        out.append(acc)
    return out


def windows(above, upper, lower, below, step):
    rows = row_ids()
    shift = 2 - step
    top = jnp.where(rows < shift, pltpu.roll(above, shift, 0), pltpu.roll(upper, shift, 0))
    shift = 6 - step
    low = jnp.where(rows < shift, pltpu.roll(lower, shift, 0), pltpu.roll(below, shift, 0))
    return jnp.concatenate([top, low], axis=0)


def coefficients(coef, dif_ref, rows):
    lane = lax.broadcasted_iota(jnp.int32, (rows, LANES), 1)
    for level in range(LEVELS):
        dif = dif_ref[level]
        coef[0, level] = 1.0 - ADVECT - 2.0 * VERTICAL - 4.0 * dif
        coef[1, level] = dif + ADVECT
        coef[2, level] = dif
        coef[3, level] = jnp.where(lane == 0, 0.0, dif)
        coef[4, level] = jnp.where(lane == LANES - 1, 0.0, dif)


def column(states, level):
    near = [states[n] for n in (level - 1, level + 1) if 0 <= n < LEVELS]
    return near[0] + near[1] if len(near) == 2 else near[0]


def substep(coef, level, state, west, east, vertical):
    return (
        coef[0, level] * state
        + coef[1, level] * west
        + coef[2, level] * east
        + coef[3, level] * pltpu.roll(state, 1, 1)
        + coef[4, level] * pltpu.roll(state, LANES - 1, 1)
        + VERTICAL * vertical
    )


def kernel(
    ens_hbm, dif_hbm, cells_hbm, values_hbm, weights_hbm, out_ref,
    ens, dif_ref, cells_ref, values_ref, weights_ref, up_send, down_send, top_halo, low_halo, coef, edge_coef, edge_dif, turn,
    oc, hot, cell_send, cell_recv, pred_send, pred_recv,
    ymat, zmat, mmat, root, drive, back_send, back_recv,
    load_sem, halo_ssem, halo_rsem, oc_ssem, oc_rsem, pred_ssem, pred_rsem,
    cell_ssem, cell_rsem, back_ssem, back_rsem,
):
    me = lax.axis_index("mem")
    tile = lax.axis_index("tile")
    tiles = lax.axis_size("tile")
    right, left = lax.rem(tile + 1, tiles), lax.rem(tile + tiles - 1, tiles)

    def order(number):
        half = lax.div(number + 1, 2)
        return jnp.where(lax.rem(number, 2) == 0, PARTS // 2 + half, PARTS // 2 - half)

    def each(action):
        def step(number, carry):
            action(order(number))
            return carry

        lax.fori_loop(0, PARTS - 1, step, 0)

    half_count = LOCAL // 2
    loads = [
        pltpu.make_async_copy(source, target, load_sem.at[number])
        for number, (source, target) in enumerate(
            [
                (dif_hbm, dif_ref),
                (ens_hbm.at[0:half_count], ens.at[0:half_count]),
                (ens_hbm.at[half_count:LOCAL], ens.at[half_count:LOCAL]),
                (cells_hbm, cells_ref),
                (values_hbm, values_ref),
                (weights_hbm, weights_ref),
            ]
        )
    ]
    for load in loads:
        load.start()
    barrier = pltpu.get_barrier_semaphore()
    each(
        lambda offset: pl.semaphore_signal(
            barrier, inc=1, device_id={"mem": lax.rem(me + offset, PARTS)}, device_id_type=MESH
        )
    )
    for other in (left, right):
        pl.semaphore_signal(barrier, inc=1, device_id={"tile": other}, device_id_type=MESH)
    loads[0].wait()
    coefficients(coef, dif_ref, ROWS)

    def inner_pair(pair, carry):
        for half in range(2):
            member = 2 * pair + half
            states = [ens[member, level] for level in range(LEVELS)]
            for repeat in range(SUB):
                states = [
                    substep(
                        coef, level, states[level],
                        pltpu.roll(states[level], 1, 0),
                        pltpu.roll(states[level], ROWS - 1, 0),
                        column(states, level),
                    )
                    for level in range(LEVELS)
                ]
            for level in range(LEVELS):
                for block in range(ROWS // 8):
                    first = (level * ROWS + 8 * block) * PITCH
                    turn[pl.ds(first + member, 8, stride=PITCH), :] = states[level][
                        8 * block : 8 * block + 8
                    ]
        return carry

    def to_cells(part, low, count):
        for chunk in range(CHUNKS):
            for half in range(SPAN):
                first = pl.multiple_of((part * 8 + SPAN * chunk + half) * PITCH + low, 8)
                cell_send[part, chunk, low : low + count, half * LANES : (half + 1) * LANES] = (
                    turn[pl.ds(first, count), :].astype(BF16)
                )

    def inner_cells(low, number, carry):
        to_cells(4 * (number // 2) + 1 + lax.rem(number, 2), low, half_count)
        return carry

    loads[1].wait()
    lax.fori_loop(0, half_count // 2, inner_pair, 0)
    lax.fori_loop(0, PARTS // 2, functools.partial(inner_cells, 0), 0)
    loads[2].wait()

    def pack_pair(pair, carry):
        tops, lows = [], []
        for half in range(2):
            for level in range(LEVELS):
                tops.append(ens[2 * pair + half, level, 0:8, :])
                lows.append(ens[2 * pair + half, level, ROWS - 8 : ROWS, :])
        for block, value in enumerate(pack(tops, 0)):
            up_send[pair, 8 * block : 8 * block + 8, :] = value
        for block, value in enumerate(pack(lows, 5)):
            down_send[pair, 8 * block : 8 * block + 8, :] = value
        return carry

    lax.fori_loop(0, LOCAL // 2, pack_pair, 0)
    tops = [dif_ref[level, 0:8, :] for level in range(LEVELS)]
    lows = [dif_ref[level, ROWS - 8 : ROWS, :] for level in range(LEVELS)]
    for block, value in enumerate(pack(tops, 0)):
        up_send[LOCAL // 2, 8 * block : 8 * block + 8, :] = value
    for block, value in enumerate(pack(lows, 5)):
        down_send[LOCAL // 2, 8 * block : 8 * block + 8, :] = value

    pl.semaphore_wait(barrier, PARTS + 1)

    def remote(source, target, ssem, rsem, device):
        return pltpu.make_async_remote_copy(
            src_ref=source, dst_ref=target, send_sem=ssem, recv_sem=rsem,
            device_id=device, device_id_type=MESH,
        )

    def oc_copy(offset):
        return remote(
            cells_ref.at[0], oc.at[me], oc_ssem.at[offset], oc_rsem.at[offset],
            {"mem": lax.rem(me + offset, PARTS)},
        )

    def pred_copy(offset):
        other = lax.rem(me + offset, PARTS)
        return remote(
            pred_send.at[other], pred_recv.at[me], pred_ssem.at[offset], pred_rsem.at[offset],
            {"mem": other},
        )

    def cell_copy(chunk, offset):
        other = lax.rem(me + offset, PARTS)
        return remote(
            cell_send.at[other, chunk], cell_recv.at[chunk, me],
            cell_ssem.at[chunk, offset], cell_rsem.at[chunk, offset], {"mem": other},
        )

    def back_copy(chunk, offset):
        other = lax.rem(me + offset, PARTS)
        return remote(
            back_send.at[chunk, other], back_recv.at[chunk, me],
            back_ssem.at[chunk, offset], back_rsem.at[chunk, offset], {"mem": other},
        )

    to_right = remote(down_send, top_halo, halo_ssem.at[0], halo_rsem.at[0], {"tile": right})
    to_left = remote(up_send, low_halo, halo_ssem.at[1], halo_rsem.at[1], {"tile": left})
    to_right.start()
    to_left.start()
    for load in loads[3:]:
        load.wait()
    each(lambda offset: oc_copy(offset).start())
    oc[me] = cells_ref[0]


    def inner(part):
        return lax.rem(lax.rem(part, 4) + 1, 4) >= 2

    def inner_send(low, offset):
        part = lax.rem(me + offset, PARTS)

        @pl.when(inner(part))
        def _():
            for chunk in range(CHUNKS):
                remote(
                    cell_send.at[part, chunk, pl.ds(low, half_count)],
                    cell_recv.at[chunk, me, pl.ds(low, half_count)],
                    cell_ssem.at[chunk, offset], cell_rsem.at[chunk, offset], {"mem": part},
                ).start()

    each(functools.partial(inner_send, 0))
    lax.fori_loop(half_count // 2, LOCAL // 2, inner_pair, 0)
    lax.fori_loop(0, PARTS // 2, functools.partial(inner_cells, half_count), 0)
    each(functools.partial(inner_send, half_count))

    each(lambda offset: oc_copy(offset).wait())
    within = lax.broadcasted_iota(jnp.int32, (HOT, NOBS), 0)

    def mark(part, carry):
        index = jnp.bitwise_and(oc[part], HOT - 1)
        hot[part] = jnp.where(within == index, 1.0, 0.0).astype(BF16)
        return carry

    lax.fori_loop(0, PARTS, mark, 0)

    top_mask = jnp.where(tile > 0, 1.0, 0.0).astype(F32)
    low_mask = jnp.where(tile < tiles - 1, 1.0, 0.0).astype(F32)
    to_right.wait()
    to_left.wait()
    extra = [
        [halo[LOCAL // 2, 8 * block : 8 * block + 8, :] for block in range(3)]
        for halo in (top_halo, low_halo)
    ]
    for level in range(LEVELS):
        edge_dif[level] = windows(
            place(extra[0], 3 * level, 5), dif_ref[level, 0:8],
            dif_ref[level, ROWS - 8 : ROWS], place(extra[1], 3 * level, 0), 0,
        )
    coefficients(edge_coef, edge_dif, 16)
    edge_row = lax.broadcasted_iota(jnp.int32, (16, LANES), 0)
    edge_mask = jnp.where(edge_row < 2, top_mask, jnp.where(edge_row >= 14, low_mask, 1.0))

    edge_top = edge_row == 0
    edge_low = edge_row == 15
    rows = row_ids()

    def moved(tiles, source, target, count):
        first, last = source // 8, (source + count - 1) // 8
        shift = (target - source) % 8
        pieces = [
            pltpu.roll(tiles[n], shift, 0) if shift else tiles[n] for n in (first, last)[: 1 + (last > first)]
        ]
        if len(pieces) == 1:
            return pieces[0]
        return jnp.where(rows >= target + 8 * last - source, pieces[1], pieces[0])

    def edge_group(group, carry):
        members = range(4)
        states, wests, easts = {}, {}, {}
        for number in members:
            pair, half = 2 * group + number // 2, number % 2
            above = [top_halo[pair, 8 * n : 8 * n + 8, :] for n in range(3)]
            below = [low_halo[pair, 8 * n : 8 * n + 8, :] for n in range(3)]
            for level in range(LEVELS):
                at = 3 * (LEVELS * half + level)
                block = (2 * pair + half, level)
                upper, lower = ens[(*block, slice(0, 8))], ens[(*block, slice(ROWS - 8, ROWS))]
                top = jnp.where(
                    rows < 2, moved(above, at + 1, 0, 2) * top_mask, pltpu.roll(upper, 2, 0)
                )
                low = jnp.where(
                    rows < 6, pltpu.roll(lower, 6, 0), moved(below, at, 6, 2) * low_mask
                )
                state = jnp.concatenate([top, low], axis=0)
                first = moved(above, at, 0, 1) * top_mask
                last = moved(below, at + 2, 7, 1) * low_mask
                states[number, level] = state
                wests[number, level] = jnp.where(
                    edge_top, jnp.concatenate([first, low], axis=0), pltpu.roll(state, 1, 0)
                )
                easts[number, level] = jnp.where(
                    edge_low, jnp.concatenate([top, last], axis=0), pltpu.roll(state, 15, 0)
                )
        for repeat in range(SUB):
            updated = {}
            for number in members:
                own = [states[number, level] for level in range(LEVELS)]
                for level in range(LEVELS):
                    west = pltpu.roll(own[level], 1, 0) if repeat else wests[number, level]
                    east = pltpu.roll(own[level], 15, 0) if repeat else easts[number, level]
                    value = substep(edge_coef, level, own[level], west, east, column(own, level))
                    updated[number, level] = value * edge_mask if repeat < SUB - 1 else value
            states = updated
        for number in members:
            for level in range(LEVELS):
                first = level * ROWS * PITCH + 4 * group + number
                value = states[number, level]
                turn[pl.ds(first, 3, stride=PITCH), :] = value[2:5]
                turn[pl.ds(first + (ROWS - 3) * PITCH, 3, stride=PITCH), :] = value[11:14]
        return carry

    lax.fori_loop(0, LOCAL // 4, edge_group, 0)

    def edge_cells(number, carry):
        to_cells(4 * (number // 2) + 3 * lax.rem(number, 2), 0, LOCAL)
        return carry

    lax.fori_loop(0, PARTS // 2, edge_cells, 0)

    def gather(number, carry):
        part = lax.rem(me + order(number), PARTS)
        group = jnp.broadcast_to(jnp.right_shift(oc[part], 8), (LOCAL, NOBS))
        pieces = []
        for step in (PARTS - 1, 0, 1):
            other = lax.rem(part + step, PARTS)
            for chunk in range(CHUNKS):
                for first in range(0, WIDE, HOT):
                    pieces.append(cell_send[other, chunk, :, first : first + HOT])
        found = jnp.dot(jnp.concatenate(pieces, axis=0), hot[part], preferred_element_type=F32)
        total = jnp.zeros((LOCAL, NOBS), F32)
        for piece in range(3 * CHUNKS * (WIDE // HOT)):
            total += jnp.where(
                group == piece, found[LOCAL * piece : LOCAL * piece + LOCAL], 0.0
            )
        pred_send[part] = total.astype(BF16)
        pl.when(number > 0)(lambda: pred_copy(order(number - 1)).start())
        return carry

    lax.fori_loop(0, PARTS, gather, 0)
    for chunk in range(CHUNKS):
        def edge_send(offset):
            part = lax.rem(me + offset, PARTS)
            pl.when(jnp.logical_not(inner(part)))(lambda: cell_copy(chunk, offset).start())

        each(edge_send)
        cell_recv[chunk, me] = cell_send[me, chunk]
    pred_recv[me] = pred_send[me]

    each(lambda offset: pred_copy(offset).wait())
    weights, values = weights_ref[0], values_ref[0]
    total = jnp.zeros((1, NOBS), F32)
    for part in range(PARTS):
        total += jnp.sum(pred_recv[part].astype(F32), axis=0, keepdims=True)
    pmean = total * (1.0 / MEMBERS)
    pull = weights * (values - pmean)
    for part in range(PARTS):
        rows = slice(LOCAL * part, LOCAL * part + LOCAL)
        ppert = pred_recv[part].astype(F32) - pmean
        ymat[rows, :] = (ppert * weights).astype(BF16)
        zmat[rows, :] = ppert.astype(BF16)
        drive[rows, :] = jnp.sum(ppert * pull, axis=1, keepdims=True) * (1.0 / (MEMBERS - 1.0))
    gram = lax.dot_general(
        zmat[...], ymat[...], (((1,), (1,)), ((), ())), preferred_element_type=F32
    )
    eye = jnp.where(
        lax.broadcasted_iota(jnp.int32, (MEMBERS, MEMBERS), 0)
        == lax.broadcasted_iota(jnp.int32, (MEMBERS, MEMBERS), 1),
        1.0,
        0.0,
    )
    root[...] = gram * (1.0 / (MEMBERS - 1.0)) + eye
    small = jnp.where(
        lax.broadcasted_iota(jnp.int32, (LANES, LANES), 0)
        == lax.broadcasted_iota(jnp.int32, (LANES, LANES), 1),
        1.0,
        0.0,
    )
    trace = jnp.zeros((1, 1), F32)
    for block in range(MEMBERS // LANES):
        part = slice(LANES * block, LANES * block + LANES)
        diagonal = jnp.sum(root[part, part] * small, axis=1, keepdims=True)
        trace += jnp.sum(diagonal, axis=0, keepdims=True)
    scale = trace * (3.0 / MEMBERS)
    first = (root[...] * (1.0 / scale)).astype(BF16)
    ymat[...] = first
    mmat[...] = (1.5 * eye - 0.5 * first.astype(F32)).astype(BF16)
    zmat[...] = mmat[...]
    ymat[...] = jnp.dot(mmat[...], first, preferred_element_type=F32).astype(BF16)

    def newton(step, carry):
        product = jnp.dot(ymat[...], zmat[...], preferred_element_type=F32)
        mmat[...] = (1.5 * eye - 0.5 * product).astype(BF16)
        ynext = jnp.dot(mmat[...], ymat[...], preferred_element_type=F32).astype(BF16)
        znext = jnp.dot(zmat[...], mmat[...], preferred_element_type=F32).astype(BF16)
        ymat[...] = ynext
        zmat[...] = znext
        return carry

    lax.fori_loop(0, ITERS - 2, newton, 0)
    product = jnp.dot(ymat[...], zmat[...], preferred_element_type=F32)
    mmat[...] = (1.5 * eye - 0.5 * product).astype(BF16)
    root[...] = jnp.dot(zmat[...], mmat[...], preferred_element_type=F32) * (
        1.0 / jnp.sqrt(scale)
    )
    across = jnp.sum(root[...] * drive[...], axis=0, keepdims=True)
    wmean = jnp.zeros((1, MEMBERS), F32)
    for block in range(MEMBERS // LANES):
        part = slice(LANES * block, LANES * block + LANES)
        down = jnp.sum(across[:, part] * small, axis=1, keepdims=True)
        wmean += jnp.sum(root[part, :] * down, axis=0, keepdims=True)
    ymat[...] = (root[...] + wmean).astype(BF16)

    for chunk in range(CHUNKS):
        each(lambda offset: cell_copy(chunk, offset).wait())
        total = jnp.zeros((1, WIDE), F32)
        for part in range(PARTS):
            total += jnp.sum(cell_recv[chunk, part].astype(F32), axis=0, keepdims=True)
        xmean = total * (1.0 / MEMBERS)
        for part in range(PARTS):
            zmat[LOCAL * part : LOCAL * part + LOCAL, 0:WIDE] = (
                cell_recv[chunk, part].astype(F32) - xmean
            ).astype(BF16)
        update = jnp.dot(ymat[...], zmat[:, 0:WIDE], preferred_element_type=F32) + xmean
        for part in range(PARTS):
            back_send[chunk, part] = update[LOCAL * part : LOCAL * part + LOCAL].astype(BF16)
        each(lambda offset: back_copy(chunk, offset).start())
        back_recv[chunk, me] = back_send[chunk, me]

    for chunk in range(CHUNKS):
        each(lambda offset: back_copy(chunk, offset).wait())

        def from_cells(part, carry):
            for half in range(SPAN):
                first = pl.multiple_of((part * 8 + SPAN * chunk + half) * PITCH, 8)
                turn[pl.ds(first, LOCAL), :] = back_recv[
                    chunk, part, :, half * LANES : (half + 1) * LANES
                ].astype(F32)
            return carry

        lax.fori_loop(0, PARTS, from_cells, 0)

    def to_states(member, carry):
        for part in range(PARTS):
            out_ref[member, part // 4, (part % 4) * 8 : (part % 4) * 8 + 8, :] = turn[
                pl.ds(part * 8 * PITCH + member, 8, stride=PITCH), :
            ]
        return carry

    lax.fori_loop(0, LOCAL, to_states, 0)


def on_device(ensemble, diffusion, obs_cells, obs_values, obs_weights):
    vmem = pl.BlockSpec(memory_space=pltpu.VMEM)
    dma = pltpu.SemaphoreType.DMA
    halo = pltpu.VMEM((LOCAL // 2 + 1, 24, LANES), F32)
    square = pltpu.VMEM((MEMBERS, MEMBERS), BF16)
    return pl.pallas_call(
        kernel,
        name="cycle",
        out_shape=pltpu.VMEM(ensemble.shape, F32),
        in_specs=[pl.BlockSpec(memory_space=pl.ANY)] * 5,
        out_specs=vmem,
        scratch_shapes=[
            pltpu.VMEM(ensemble.shape, F32),
            pltpu.VMEM(diffusion.shape, F32),
            pltpu.VMEM(obs_cells.shape, jnp.int32),
            pltpu.VMEM(obs_values.shape, F32),
            pltpu.VMEM(obs_weights.shape, F32),
            halo, halo, halo, halo,
            pltpu.VMEM((5, LEVELS, ROWS, LANES), F32),
            pltpu.VMEM((5, LEVELS, 16, LANES), F32),
            pltpu.VMEM((LEVELS, 16, LANES), F32),
            pltpu.VMEM((LEVELS * ROWS * PITCH, LANES), F32),
            pltpu.VMEM((PARTS, 1, NOBS), jnp.int32),
            pltpu.VMEM((PARTS, HOT, NOBS), BF16),
            pltpu.VMEM((PARTS, CHUNKS, LOCAL, WIDE), BF16),
            pltpu.VMEM((CHUNKS, PARTS, LOCAL, WIDE), BF16),
            pltpu.VMEM((PARTS, LOCAL, NOBS), BF16),
            pltpu.VMEM((PARTS, LOCAL, NOBS), BF16),
            square, square, square,
            pltpu.VMEM((MEMBERS, MEMBERS), F32),
            pltpu.VMEM((MEMBERS, 1), F32),
            pltpu.VMEM((CHUNKS, PARTS, LOCAL, WIDE), BF16),
            pltpu.VMEM((CHUNKS, PARTS, LOCAL, WIDE), BF16),
            dma((6,)), dma((2,)), dma((2,)),
            dma((PARTS,)), dma((PARTS,)), dma((PARTS,)), dma((PARTS,)),
            dma((CHUNKS, PARTS)), dma((CHUNKS, PARTS)),
            dma((CHUNKS, PARTS)), dma((CHUNKS, PARTS)),
        ],
        compiler_params=pltpu.CompilerParams(
            collective_id=0, has_side_effects=True, vmem_limit_bytes=56 * 1024 * 1024
        ),
    )(ensemble, diffusion, obs_cells, obs_values, obs_weights)


def solution(mesh):
    return jax.shard_map(
        on_device,
        mesh=mesh,
        in_specs=(
            P("mem", None, "tile", None),
            P(None, "tile", None),
            P("tile", "mem", None),
            P("tile", "mem", None),
            P("tile", "mem", None),
        ),
        out_specs=P("mem", None, "tile", None),
        check_vma=False,
    )
```

```python
import functools

import jax
import jax.numpy as jnp
from jax import lax
from jax.experimental import pallas as pl
from jax.experimental.pallas import tpu as pltpu
from jax.sharding import PartitionSpec as P

ITERS = 6
SUB = 3
ADVECT = 0.3
VERTICAL = 0.1
PARTS = 16
LOCAL = 32
LEVELS = 4
ROWS = 32
LANES = 128
MEMBERS = 512
NOBS = 512
PATCH = 1024
CHUNKS = 2
WIDE = 512
SPAN = WIDE // LANES
HOT = 256
PITCH = 40
MESH = pl.DeviceIdType.MESH
F32 = jnp.float32
BF16 = jnp.bfloat16


def row_ids():
    return lax.broadcasted_iota(jnp.int32, (8, LANES), 0)


def place(tiles, source, target):
    first, last = source // 8, (source + 2) // 8
    shift = (target - source) % 8
    out = pltpu.roll(tiles[first], shift, 0) if shift else tiles[first]
    if last != first:
        other = pltpu.roll(tiles[last], shift, 0) if shift else tiles[last]
        out = jnp.where(row_ids() >= target + 8 * last - source, other, out)
    return out


def pack(pieces, base):
    rows = row_ids()
    out = []
    for block in range(3):
        acc = jnp.zeros((8, LANES), F32)
        for number, piece in enumerate(pieces):
            low, high = 3 * number - 8 * block, 3 * number + 3 - 8 * block
            if high <= 0 or low >= 8:
                continue
            shift = (3 * number - base) % 8
            moved = pltpu.roll(piece, shift, 0) if shift else piece
            acc = jnp.where((rows >= low) & (rows < high), moved, acc)
        out.append(acc)
    return out


def windows(above, upper, lower, below, step):
    rows = row_ids()
    shift = 2 - step
    top = jnp.where(rows < shift, pltpu.roll(above, shift, 0), pltpu.roll(upper, shift, 0))
    shift = 6 - step
    low = jnp.where(rows < shift, pltpu.roll(lower, shift, 0), pltpu.roll(below, shift, 0))
    return jnp.concatenate([top, low], axis=0)


def coefficients(coef, dif_ref, rows):
    lane = lax.broadcasted_iota(jnp.int32, (rows, LANES), 1)
    for level in range(LEVELS):
        dif = dif_ref[level]
        coef[0, level] = 1.0 - ADVECT - 2.0 * VERTICAL - 4.0 * dif
        coef[1, level] = dif + ADVECT
        coef[2, level] = dif
        coef[3, level] = jnp.where(lane == 0, 0.0, dif)
        coef[4, level] = jnp.where(lane == LANES - 1, 0.0, dif)


def column(states, level):
    near = [states[n] for n in (level - 1, level + 1) if 0 <= n < LEVELS]
    return near[0] + near[1] if len(near) == 2 else near[0]


def substep(coef, level, state, west, east, vertical):
    return (
        coef[0, level] * state
        + coef[1, level] * west
        + coef[2, level] * east
        + coef[3, level] * pltpu.roll(state, 1, 1)
        + coef[4, level] * pltpu.roll(state, LANES - 1, 1)
        + VERTICAL * vertical
    )


def kernel(
    ens_hbm, dif_hbm, cells_hbm, values_hbm, weights_hbm, out_ref,
    ens, dif_ref, cells_ref, values_ref, weights_ref, up_send, down_send, top_halo, low_halo, coef, edge_coef, edge_dif, turn,
    oc, hot, hot_own, near, near_recv, cell_send, cell_recv, pred_send, pred_recv,
    ymat, zmat, mmat, root, drive, back_send, back_recv,
    load_sem, halo_ssem, halo_rsem, oc_ssem, oc_rsem, pred_ssem, pred_rsem, near_ssem, near_rsem,
    cell_ssem, cell_rsem, back_ssem, back_rsem,
):
    me = lax.axis_index("mem")
    tile = lax.axis_index("tile")
    tiles = lax.axis_size("tile")
    right, left = lax.rem(tile + 1, tiles), lax.rem(tile + tiles - 1, tiles)

    def order(number):
        half = lax.div(number + 1, 2)
        return jnp.where(lax.rem(number, 2) == 0, PARTS // 2 + half, PARTS // 2 - half)

    def each(action):
        def step(number, carry):
            action(order(number))
            return carry

        lax.fori_loop(0, PARTS - 1, step, 0)

    half_count = LOCAL // 2
    loads = [
        pltpu.make_async_copy(source, target, load_sem.at[number])
        for number, (source, target) in enumerate(
            [
                (dif_hbm, dif_ref),
                (ens_hbm.at[0:half_count], ens.at[0:half_count]),
                (ens_hbm.at[half_count:LOCAL], ens.at[half_count:LOCAL]),
                (cells_hbm, cells_ref),
                (values_hbm, values_ref),
                (weights_hbm, weights_ref),
            ]
        )
    ]
    for load in loads:
        load.start()
    barrier = pltpu.get_barrier_semaphore()
    each(
        lambda offset: pl.semaphore_signal(
            barrier, inc=1, device_id={"mem": lax.rem(me + offset, PARTS)}, device_id_type=MESH
        )
    )
    for other in (left, right):
        pl.semaphore_signal(barrier, inc=1, device_id={"tile": other}, device_id_type=MESH)
    loads[0].wait()
    coefficients(coef, dif_ref, ROWS)

    def inner_pair(pair, carry):
        for half in range(2):
            member = 2 * pair + half
            states = [ens[member, level] for level in range(LEVELS)]
            for repeat in range(SUB):
                states = [
                    substep(
                        coef, level, states[level],
                        pltpu.roll(states[level], 1, 0),
                        pltpu.roll(states[level], ROWS - 1, 0),
                        column(states, level),
                    )
                    for level in range(LEVELS)
                ]
            for level in range(LEVELS):
                for block in range(ROWS // 8):
                    first = (level * ROWS + 8 * block) * PITCH
                    turn[pl.ds(first + member, 8, stride=PITCH), :] = states[level][
                        8 * block : 8 * block + 8
                    ]
        return carry

    def to_cells(part, low, count):
        for chunk in range(CHUNKS):
            for half in range(SPAN):
                first = pl.multiple_of((part * 8 + SPAN * chunk + half) * PITCH + low, 8)
                cell_send[part, chunk, low : low + count, half * LANES : (half + 1) * LANES] = (
                    turn[pl.ds(first, count), :].astype(BF16)
                )

    def inner_cells(low, number, carry):
        to_cells(4 * (number // 2) + 1 + lax.rem(number, 2), low, half_count)
        return carry

    loads[1].wait()
    lax.fori_loop(0, half_count // 2, inner_pair, 0)
    lax.fori_loop(0, PARTS // 2, functools.partial(inner_cells, 0), 0)
    loads[2].wait()

    def pack_pair(pair, carry):
        tops, lows = [], []
        for half in range(2):
            for level in range(LEVELS):
                tops.append(ens[2 * pair + half, level, 0:8, :])
                lows.append(ens[2 * pair + half, level, ROWS - 8 : ROWS, :])
        for block, value in enumerate(pack(tops, 0)):
            up_send[pair, 8 * block : 8 * block + 8, :] = value
        for block, value in enumerate(pack(lows, 5)):
            down_send[pair, 8 * block : 8 * block + 8, :] = value
        return carry

    lax.fori_loop(0, LOCAL // 2, pack_pair, 0)
    tops = [dif_ref[level, 0:8, :] for level in range(LEVELS)]
    lows = [dif_ref[level, ROWS - 8 : ROWS, :] for level in range(LEVELS)]
    for block, value in enumerate(pack(tops, 0)):
        up_send[LOCAL // 2, 8 * block : 8 * block + 8, :] = value
    for block, value in enumerate(pack(lows, 5)):
        down_send[LOCAL // 2, 8 * block : 8 * block + 8, :] = value

    pl.semaphore_wait(barrier, PARTS + 1)

    def remote(source, target, ssem, rsem, device):
        return pltpu.make_async_remote_copy(
            src_ref=source, dst_ref=target, send_sem=ssem, recv_sem=rsem,
            device_id=device, device_id_type=MESH,
        )

    def oc_copy(offset):
        return remote(
            cells_ref.at[0], oc.at[me], oc_ssem.at[offset], oc_rsem.at[offset],
            {"mem": lax.rem(me + offset, PARTS)},
        )

    def pred_copy(offset):
        other = lax.rem(me + offset, PARTS)
        return remote(
            pred_send.at[other], pred_recv.at[me, pl.ds(half_count, half_count)], pred_ssem.at[offset], pred_rsem.at[offset],
            {"mem": other},
        )

    def cell_copy(side, chunk, offset):
        other = lax.rem(me + offset, PARTS)
        rows = pl.ds(side * half_count, half_count)
        return remote(
            cell_send.at[other, chunk, rows], cell_recv.at[chunk, me, rows],
            cell_ssem.at[side, chunk, offset], cell_rsem.at[side, chunk, offset],
            {"mem": other},
        )

    def back_copy(chunk, offset):
        other = lax.rem(me + offset, PARTS)
        return remote(
            back_send.at[chunk, other], back_recv.at[chunk, me],
            back_ssem.at[chunk, offset], back_rsem.at[chunk, offset], {"mem": other},
        )

    to_right = remote(down_send, top_halo, halo_ssem.at[0], halo_rsem.at[0], {"tile": right})
    to_left = remote(up_send, low_halo, halo_ssem.at[1], halo_rsem.at[1], {"tile": left})
    to_right.start()
    to_left.start()
    for load in loads[3:]:
        load.wait()
    each(lambda offset: oc_copy(offset).start())
    oc[me] = cells_ref[0]


    def inner(part):
        return lax.rem(lax.rem(part, 4) + 1, 4) >= 2

    def send(wanted, side, offset):
        @pl.when(inner(lax.rem(me + offset, PARTS)) == wanted)
        def _():
            for chunk in range(CHUNKS):
                cell_copy(side, chunk, offset).start()

    each(functools.partial(send, True, 0))
    lax.fori_loop(half_count // 2, LOCAL // 2, inner_pair, 0)
    lax.fori_loop(0, PARTS // 2, functools.partial(inner_cells, half_count), 0)
    each(functools.partial(send, True, 1))

    each(lambda offset: oc_copy(offset).wait())
    within = lax.broadcasted_iota(jnp.int32, (HOT, NOBS), 0)

    def mark(part, carry):
        index = jnp.bitwise_and(oc[part], HOT - 1)
        hot[part] = jnp.where(within == index, 1.0, 0.0).astype(BF16)
        return carry

    lax.fori_loop(0, PARTS, mark, 0)

    top_mask = jnp.where(tile > 0, 1.0, 0.0).astype(F32)
    low_mask = jnp.where(tile < tiles - 1, 1.0, 0.0).astype(F32)
    to_right.wait()
    to_left.wait()
    extra = [
        [halo[LOCAL // 2, 8 * block : 8 * block + 8, :] for block in range(3)]
        for halo in (top_halo, low_halo)
    ]
    for level in range(LEVELS):
        edge_dif[level] = windows(
            place(extra[0], 3 * level, 5), dif_ref[level, 0:8],
            dif_ref[level, ROWS - 8 : ROWS], place(extra[1], 3 * level, 0), 0,
        )
    coefficients(edge_coef, edge_dif, 16)
    edge_row = lax.broadcasted_iota(jnp.int32, (16, LANES), 0)
    edge_mask = jnp.where(edge_row < 2, top_mask, jnp.where(edge_row >= 14, low_mask, 1.0))

    edge_top = edge_row == 0
    edge_low = edge_row == 15
    rows = row_ids()

    def moved(tiles, source, target, count):
        first, last = source // 8, (source + count - 1) // 8
        shift = (target - source) % 8
        pieces = [
            pltpu.roll(tiles[n], shift, 0) if shift else tiles[n] for n in (first, last)[: 1 + (last > first)]
        ]
        if len(pieces) == 1:
            return pieces[0]
        return jnp.where(rows >= target + 8 * last - source, pieces[1], pieces[0])

    def edge_group(group, carry):
        members = range(4)
        states, wests, easts = {}, {}, {}
        for number in members:
            pair, half = 2 * group + number // 2, number % 2
            above = [top_halo[pair, 8 * n : 8 * n + 8, :] for n in range(3)]
            below = [low_halo[pair, 8 * n : 8 * n + 8, :] for n in range(3)]
            for level in range(LEVELS):
                at = 3 * (LEVELS * half + level)
                block = (2 * pair + half, level)
                upper, lower = ens[(*block, slice(0, 8))], ens[(*block, slice(ROWS - 8, ROWS))]
                top = jnp.where(
                    rows < 2, moved(above, at + 1, 0, 2) * top_mask, pltpu.roll(upper, 2, 0)
                )
                low = jnp.where(
                    rows < 6, pltpu.roll(lower, 6, 0), moved(below, at, 6, 2) * low_mask
                )
                state = jnp.concatenate([top, low], axis=0)
                first = moved(above, at, 0, 1) * top_mask
                last = moved(below, at + 2, 7, 1) * low_mask
                states[number, level] = state
                wests[number, level] = jnp.where(
                    edge_top, jnp.concatenate([first, low], axis=0), pltpu.roll(state, 1, 0)
                )
                easts[number, level] = jnp.where(
                    edge_low, jnp.concatenate([top, last], axis=0), pltpu.roll(state, 15, 0)
                )
        for repeat in range(SUB):
            updated = {}
            for number in members:
                own = [states[number, level] for level in range(LEVELS)]
                for level in range(LEVELS):
                    west = pltpu.roll(own[level], 1, 0) if repeat else wests[number, level]
                    east = pltpu.roll(own[level], 15, 0) if repeat else easts[number, level]
                    value = substep(edge_coef, level, own[level], west, east, column(own, level))
                    updated[number, level] = value * edge_mask if repeat < SUB - 1 else value
            states = updated
        for number in members:
            for level in range(LEVELS):
                first = level * ROWS * PITCH + 4 * group + number
                value = states[number, level]
                turn[pl.ds(first, 3, stride=PITCH), :] = value[2:5]
                turn[pl.ds(first + (ROWS - 3) * PITCH, 3, stride=PITCH), :] = value[11:14]
        return carry

    lax.fori_loop(0, LOCAL // 4, edge_group, 0)

    def edge_cells(number, carry):
        to_cells(4 * (number // 2) + 3 * lax.rem(number, 2), 0, LOCAL)
        return carry

    lax.fori_loop(0, PARTS // 2, edge_cells, 0)

    each(functools.partial(send, False, 0))

    def gather(number, carry):
        part = lax.rem(me + order(number), PARTS)
        group = jnp.broadcast_to(jnp.right_shift(oc[part], 8), (half_count, NOBS))
        pieces = []
        for step in (PARTS - 1, 0, 1):
            other = lax.rem(part + step, PARTS)
            for chunk in range(CHUNKS):
                for first in range(0, WIDE, HOT):
                    pieces.append(cell_send[other, chunk, half_count:, first : first + HOT])
        found = jnp.dot(jnp.concatenate(pieces, axis=0), hot[part], preferred_element_type=F32)
        total = jnp.zeros((half_count, NOBS), F32)
        for piece in range(3 * CHUNKS * (WIDE // HOT)):
            total += jnp.where(
                group == piece, found[half_count * piece : half_count * piece + half_count], 0.0
            )
        pred_send[part] = total.astype(BF16)
        pl.when(number > 0)(lambda: pred_copy(order(number - 1)).start())
        return carry

    lax.fori_loop(0, PARTS, gather, 0)
    pred_recv[me, half_count:] = pred_send[me]
    for chunk in range(CHUNKS):
        cell_recv[chunk, me] = cell_send[me, chunk]
        each(lambda offset: cell_copy(0, chunk, offset).wait())

    def find(step, carry):
        index = oc[lax.rem(me + step + PARTS - 1, PARTS)] - PATCH * (2 - step)
        for block in range(PATCH // HOT):
            hot_own[HOT * block : HOT * block + HOT, :] = jnp.where(
                within == index - HOT * block, 1.0, 0.0
            ).astype(BF16)
        found = jnp.zeros((half_count * PARTS, NOBS), F32)
        for chunk in range(CHUNKS):
            rows = [cell_recv[chunk, part, 0:half_count] for part in range(PARTS)]
            found += jnp.dot(
                jnp.concatenate(rows, axis=0),
                hot_own[WIDE * chunk : WIDE * chunk + WIDE, :],
                preferred_element_type=F32,
            )
        near[step] = found.astype(BF16)
        return carry

    lax.fori_loop(0, 3, find, 0)
    to_last = remote(
        near.at[0], near_recv.at[1], near_ssem.at[0], near_rsem.at[0],
        {"mem": lax.rem(me + PARTS - 1, PARTS)},
    )
    to_next = remote(
        near.at[2], near_recv.at[0], near_ssem.at[1], near_rsem.at[1],
        {"mem": lax.rem(me + 1, PARTS)},
    )
    to_last.start()
    to_next.start()
    each(functools.partial(send, False, 1))
    to_last.wait()
    to_next.wait()
    for part in range(PARTS):
        rows = slice(half_count * part, half_count * part + half_count)
        pred_recv[part, 0:half_count] = (
            near[1, rows, :].astype(F32)
            + near_recv[0, rows, :].astype(F32)
            + near_recv[1, rows, :].astype(F32)
        ).astype(BF16)

    each(lambda offset: pred_copy(offset).wait())
    weights, values = weights_ref[0], values_ref[0]
    total = jnp.zeros((1, NOBS), F32)
    for part in range(PARTS):
        total += jnp.sum(pred_recv[part].astype(F32), axis=0, keepdims=True)
    pmean = total * (1.0 / MEMBERS)
    pull = weights * (values - pmean)
    for part in range(PARTS):
        rows = slice(LOCAL * part, LOCAL * part + LOCAL)
        ppert = pred_recv[part].astype(F32) - pmean
        ymat[rows, :] = (ppert * weights).astype(BF16)
        zmat[rows, :] = ppert.astype(BF16)
        drive[rows, :] = jnp.sum(ppert * pull, axis=1, keepdims=True) * (1.0 / (MEMBERS - 1.0))
    gram = lax.dot_general(
        zmat[...], ymat[...], (((1,), (1,)), ((), ())), preferred_element_type=F32
    )
    eye = jnp.where(
        lax.broadcasted_iota(jnp.int32, (MEMBERS, MEMBERS), 0)
        == lax.broadcasted_iota(jnp.int32, (MEMBERS, MEMBERS), 1),
        1.0,
        0.0,
    )
    root[...] = gram * (1.0 / (MEMBERS - 1.0)) + eye
    small = jnp.where(
        lax.broadcasted_iota(jnp.int32, (LANES, LANES), 0)
        == lax.broadcasted_iota(jnp.int32, (LANES, LANES), 1),
        1.0,
        0.0,
    )
    trace = jnp.zeros((1, 1), F32)
    for block in range(MEMBERS // LANES):
        part = slice(LANES * block, LANES * block + LANES)
        diagonal = jnp.sum(root[part, part] * small, axis=1, keepdims=True)
        trace += jnp.sum(diagonal, axis=0, keepdims=True)
    scale = trace * (3.0 / MEMBERS)
    first = (root[...] * (1.0 / scale)).astype(BF16)
    ymat[...] = first
    mmat[...] = (1.5 * eye - 0.5 * first.astype(F32)).astype(BF16)
    zmat[...] = mmat[...]
    ymat[...] = jnp.dot(mmat[...], first, preferred_element_type=F32).astype(BF16)

    def newton(step, carry):
        product = jnp.dot(ymat[...], zmat[...], preferred_element_type=F32)
        mmat[...] = (1.5 * eye - 0.5 * product).astype(BF16)
        ynext = jnp.dot(mmat[...], ymat[...], preferred_element_type=F32).astype(BF16)
        znext = jnp.dot(zmat[...], mmat[...], preferred_element_type=F32).astype(BF16)
        ymat[...] = ynext
        zmat[...] = znext
        return carry

    lax.fori_loop(0, ITERS - 2, newton, 0)
    product = jnp.dot(ymat[...], zmat[...], preferred_element_type=F32)
    mmat[...] = (1.5 * eye - 0.5 * product).astype(BF16)
    root[...] = jnp.dot(zmat[...], mmat[...], preferred_element_type=F32) * (
        1.0 / jnp.sqrt(scale)
    )
    across = jnp.sum(root[...] * drive[...], axis=0, keepdims=True)
    wmean = jnp.zeros((1, MEMBERS), F32)
    for block in range(MEMBERS // LANES):
        part = slice(LANES * block, LANES * block + LANES)
        down = jnp.sum(across[:, part] * small, axis=1, keepdims=True)
        wmean += jnp.sum(root[part, :] * down, axis=0, keepdims=True)
    ymat[...] = (root[...] + wmean).astype(BF16)

    for chunk in range(CHUNKS):
        each(lambda offset: cell_copy(1, chunk, offset).wait())
        total = jnp.zeros((1, WIDE), F32)
        for part in range(PARTS):
            total += jnp.sum(cell_recv[chunk, part].astype(F32), axis=0, keepdims=True)
        xmean = total * (1.0 / MEMBERS)
        for part in range(PARTS):
            zmat[LOCAL * part : LOCAL * part + LOCAL, 0:WIDE] = (
                cell_recv[chunk, part].astype(F32) - xmean
            ).astype(BF16)
        update = jnp.dot(ymat[...], zmat[:, 0:WIDE], preferred_element_type=F32) + xmean
        for part in range(PARTS):
            back_send[chunk, part] = update[LOCAL * part : LOCAL * part + LOCAL].astype(BF16)
        each(lambda offset: back_copy(chunk, offset).start())
        back_recv[chunk, me] = back_send[chunk, me]

    for chunk in range(CHUNKS):
        each(lambda offset: back_copy(chunk, offset).wait())

        def from_cells(part, carry):
            for half in range(SPAN):
                first = pl.multiple_of((part * 8 + SPAN * chunk + half) * PITCH, 8)
                turn[pl.ds(first, LOCAL), :] = back_recv[
                    chunk, part, :, half * LANES : (half + 1) * LANES
                ].astype(F32)
            return carry

        lax.fori_loop(0, PARTS, from_cells, 0)

    def to_states(member, carry):
        for part in range(PARTS):
            out_ref[member, part // 4, (part % 4) * 8 : (part % 4) * 8 + 8, :] = turn[
                pl.ds(part * 8 * PITCH + member, 8, stride=PITCH), :
            ]
        return carry

    lax.fori_loop(0, LOCAL, to_states, 0)


def on_device(ensemble, diffusion, obs_cells, obs_values, obs_weights):
    vmem = pl.BlockSpec(memory_space=pltpu.VMEM)
    dma = pltpu.SemaphoreType.DMA
    halo = pltpu.VMEM((LOCAL // 2 + 1, 24, LANES), F32)
    square = pltpu.VMEM((MEMBERS, MEMBERS), BF16)
    return pl.pallas_call(
        kernel,
        name="cycle",
        out_shape=pltpu.VMEM(ensemble.shape, F32),
        in_specs=[pl.BlockSpec(memory_space=pl.ANY)] * 5,
        out_specs=vmem,
        scratch_shapes=[
            pltpu.VMEM(ensemble.shape, F32),
            pltpu.VMEM(diffusion.shape, F32),
            pltpu.VMEM(obs_cells.shape, jnp.int32),
            pltpu.VMEM(obs_values.shape, F32),
            pltpu.VMEM(obs_weights.shape, F32),
            halo, halo, halo, halo,
            pltpu.VMEM((5, LEVELS, ROWS, LANES), F32),
            pltpu.VMEM((5, LEVELS, 16, LANES), F32),
            pltpu.VMEM((LEVELS, 16, LANES), F32),
            pltpu.VMEM((LEVELS * ROWS * PITCH, LANES), F32),
            pltpu.VMEM((PARTS, 1, NOBS), jnp.int32),
            pltpu.VMEM((PARTS, HOT, NOBS), BF16),
            pltpu.VMEM((PATCH, NOBS), BF16),
            pltpu.VMEM((3, MEMBERS // 2, NOBS), BF16),
            pltpu.VMEM((2, MEMBERS // 2, NOBS), BF16),
            pltpu.VMEM((PARTS, CHUNKS, LOCAL, WIDE), BF16),
            pltpu.VMEM((CHUNKS, PARTS, LOCAL, WIDE), BF16),
            pltpu.VMEM((PARTS, LOCAL // 2, NOBS), BF16),
            pltpu.VMEM((PARTS, LOCAL, NOBS), BF16),
            square, square, square,
            pltpu.VMEM((MEMBERS, MEMBERS), F32),
            pltpu.VMEM((MEMBERS, 1), F32),
            pltpu.VMEM((CHUNKS, PARTS, LOCAL, WIDE), BF16),
            pltpu.VMEM((CHUNKS, PARTS, LOCAL, WIDE), BF16),
            dma((6,)), dma((2,)), dma((2,)),
            dma((PARTS,)), dma((PARTS,)), dma((PARTS,)), dma((PARTS,)),
            dma((2,)), dma((2,)),
            dma((2, CHUNKS, PARTS)), dma((2, CHUNKS, PARTS)),
            dma((CHUNKS, PARTS)), dma((CHUNKS, PARTS)),
        ],
        compiler_params=pltpu.CompilerParams(
            collective_id=0, has_side_effects=True, vmem_limit_bytes=56 * 1024 * 1024
        ),
    )(ensemble, diffusion, obs_cells, obs_values, obs_weights)


def solution(mesh):
    return jax.shard_map(
        on_device,
        mesh=mesh,
        in_specs=(
            P("mem", None, "tile", None),
            P(None, "tile", None),
            P("tile", "mem", None),
            P("tile", "mem", None),
            P("tile", "mem", None),
        ),
        out_specs=P("mem", None, "tile", None),
        check_vma=False,
    )
```

```python
import functools

import jax
import jax.numpy as jnp
from jax import lax
from jax.experimental import pallas as pl
from jax.experimental.pallas import tpu as pltpu
from jax.sharding import PartitionSpec as P

ITERS = 6
SUB = 3
ADVECT = 0.3
VERTICAL = 0.1
PARTS = 16
LOCAL = 32
LEVELS = 4
ROWS = 32
LANES = 128
MEMBERS = 512
NOBS = 512
CHUNKS = 2
WIDE = 512
SPAN = WIDE // LANES
HOT = 256
PITCH = 40
MESH = pl.DeviceIdType.MESH
F32 = jnp.float32
BF16 = jnp.bfloat16


def row_ids():
    return lax.broadcasted_iota(jnp.int32, (8, LANES), 0)


def place(tiles, source, target):
    first, last = source // 8, (source + 2) // 8
    shift = (target - source) % 8
    out = pltpu.roll(tiles[first], shift, 0) if shift else tiles[first]
    if last != first:
        other = pltpu.roll(tiles[last], shift, 0) if shift else tiles[last]
        out = jnp.where(row_ids() >= target + 8 * last - source, other, out)
    return out


def pack(pieces, base):
    rows = row_ids()
    out = []
    for block in range(3):
        acc = jnp.zeros((8, LANES), F32)
        for number, piece in enumerate(pieces):
            low, high = 3 * number - 8 * block, 3 * number + 3 - 8 * block
            if high <= 0 or low >= 8:
                continue
            shift = (3 * number - base) % 8
            moved = pltpu.roll(piece, shift, 0) if shift else piece
            acc = jnp.where((rows >= low) & (rows < high), moved, acc)
        out.append(acc)
    return out


def windows(above, upper, lower, below, step):
    rows = row_ids()
    shift = 2 - step
    top = jnp.where(rows < shift, pltpu.roll(above, shift, 0), pltpu.roll(upper, shift, 0))
    shift = 6 - step
    low = jnp.where(rows < shift, pltpu.roll(lower, shift, 0), pltpu.roll(below, shift, 0))
    return jnp.concatenate([top, low], axis=0)


def coefficients(coef, dif_ref, rows):
    lane = lax.broadcasted_iota(jnp.int32, (rows, LANES), 1)
    for level in range(LEVELS):
        dif = dif_ref[level]
        coef[0, level] = 1.0 - ADVECT - 2.0 * VERTICAL - 4.0 * dif
        coef[1, level] = dif + ADVECT
        coef[2, level] = dif
        coef[3, level] = jnp.where(lane == 0, 0.0, dif)
        coef[4, level] = jnp.where(lane == LANES - 1, 0.0, dif)


def column(states, level):
    near = [states[n] for n in (level - 1, level + 1) if 0 <= n < LEVELS]
    return near[0] + near[1] if len(near) == 2 else near[0]


def substep(coef, level, state, west, east, vertical):
    return (
        coef[0, level] * state
        + coef[1, level] * west
        + coef[2, level] * east
        + coef[3, level] * pltpu.roll(state, 1, 1)
        + coef[4, level] * pltpu.roll(state, LANES - 1, 1)
        + VERTICAL * vertical
    )


def kernel(
    ens_hbm, dif_hbm, cells_hbm, values_hbm, weights_hbm, out_ref,
    ens, dif_ref, cells_ref, values_ref, weights_ref, up_send, down_send, top_halo, low_halo, coef, edge_coef, edge_dif, turn,
    oc, hot, cell_send, cell_recv, pred_send, pred_recv,
    ymat, zmat, mmat, root, drive, back_send, back_recv,
    load_sem, halo_ssem, halo_rsem, oc_ssem, oc_rsem, pred_ssem, pred_rsem,
    cell_ssem, cell_rsem, back_ssem, back_rsem,
):
    me = lax.axis_index("mem")
    tile = lax.axis_index("tile")
    tiles = lax.axis_size("tile")
    right, left = lax.rem(tile + 1, tiles), lax.rem(tile + tiles - 1, tiles)

    def order(number):
        half = lax.div(number + 1, 2)
        return jnp.where(lax.rem(number, 2) == 0, PARTS // 2 + half, PARTS // 2 - half)

    def each(action):
        def step(number, carry):
            action(order(number))
            return carry

        lax.fori_loop(0, PARTS - 1, step, 0)

    half_count = LOCAL // 2
    loads = [
        pltpu.make_async_copy(source, target, load_sem.at[number])
        for number, (source, target) in enumerate(
            [
                (dif_hbm, dif_ref),
                (ens_hbm.at[0:half_count], ens.at[0:half_count]),
                (ens_hbm.at[half_count:LOCAL], ens.at[half_count:LOCAL]),
                (cells_hbm, cells_ref),
                (values_hbm, values_ref),
                (weights_hbm, weights_ref),
            ]
        )
    ]
    for load in loads:
        load.start()
    barrier = pltpu.get_barrier_semaphore()
    each(
        lambda offset: pl.semaphore_signal(
            barrier, inc=1, device_id={"mem": lax.rem(me + offset, PARTS)}, device_id_type=MESH
        )
    )
    for other in (left, right):
        pl.semaphore_signal(barrier, inc=1, device_id={"tile": other}, device_id_type=MESH)
    loads[0].wait()
    coefficients(coef, dif_ref, ROWS)

    def inner_pair(pair, carry):
        for half in range(2):
            member = 2 * pair + half
            states = [ens[member, level] for level in range(LEVELS)]
            for repeat in range(SUB):
                states = [
                    substep(
                        coef, level, states[level],
                        pltpu.roll(states[level], 1, 0),
                        pltpu.roll(states[level], ROWS - 1, 0),
                        column(states, level),
                    )
                    for level in range(LEVELS)
                ]
            for level in range(LEVELS):
                for block in range(ROWS // 8):
                    first = (level * ROWS + 8 * block) * PITCH
                    turn[pl.ds(first + member, 8, stride=PITCH), :] = states[level][
                        8 * block : 8 * block + 8
                    ]
        return carry

    def to_cells(part, low, count, chunks=range(CHUNKS)):
        for chunk in chunks:
            for half in range(SPAN):
                first = pl.multiple_of((part * 8 + SPAN * chunk + half) * PITCH + low, 8)
                cell_send[part, chunk, low : low + count, half * LANES : (half + 1) * LANES] = (
                    turn[pl.ds(first, count), :].astype(BF16)
                )

    def inner_cells(low, number, carry):
        to_cells(4 * (number // 2) + 1 + lax.rem(number, 2), low, half_count)
        return carry

    loads[1].wait()
    lax.fori_loop(0, half_count // 2, inner_pair, 0)
    lax.fori_loop(0, PARTS // 2, functools.partial(inner_cells, 0), 0)
    loads[2].wait()

    def pack_pair(pair, carry):
        tops, lows = [], []
        for half in range(2):
            for level in range(LEVELS):
                tops.append(ens[2 * pair + half, level, 0:8, :])
                lows.append(ens[2 * pair + half, level, ROWS - 8 : ROWS, :])
        for block, value in enumerate(pack(tops, 0)):
            up_send[pair + 1, 8 * block : 8 * block + 8, :] = value
        for block, value in enumerate(pack(lows, 5)):
            down_send[pair + 1, 8 * block : 8 * block + 8, :] = value
        return carry

    lax.fori_loop(0, LOCAL // 2, pack_pair, 0)
    tops = [dif_ref[level, 0:8, :] for level in range(LEVELS)]
    lows = [dif_ref[level, ROWS - 8 : ROWS, :] for level in range(LEVELS)]
    for block, value in enumerate(pack(tops, 0)):
        up_send[0, 8 * block : 8 * block + 8, :] = value
    for block, value in enumerate(pack(lows, 5)):
        down_send[0, 8 * block : 8 * block + 8, :] = value

    pl.semaphore_wait(barrier, PARTS + 1)

    def remote(source, target, ssem, rsem, device):
        return pltpu.make_async_remote_copy(
            src_ref=source, dst_ref=target, send_sem=ssem, recv_sem=rsem,
            device_id=device, device_id_type=MESH,
        )

    def oc_copy(offset):
        return remote(
            cells_ref.at[0], oc.at[me], oc_ssem.at[offset], oc_rsem.at[offset],
            {"mem": lax.rem(me + offset, PARTS)},
        )

    def pred_copy(offset):
        other = lax.rem(me + offset, PARTS)
        return remote(
            pred_send.at[other], pred_recv.at[me], pred_ssem.at[offset], pred_rsem.at[offset],
            {"mem": other},
        )

    def cell_copy(chunk, offset):
        other = lax.rem(me + offset, PARTS)
        return remote(
            cell_send.at[other, chunk], cell_recv.at[chunk, me],
            cell_ssem.at[chunk, offset], cell_rsem.at[chunk, offset], {"mem": other},
        )

    def back_copy(chunk, offset):
        other = lax.rem(me + offset, PARTS)
        return remote(
            back_send.at[chunk, other], back_recv.at[chunk, me],
            back_ssem.at[chunk, offset], back_rsem.at[chunk, offset], {"mem": other},
        )

    halos = []
    for number, rows in enumerate((pl.ds(0, LOCAL // 4 + 1), pl.ds(LOCAL // 4 + 1, LOCAL // 4))):
        halos.append(
            [
                remote(
                    down_send.at[rows], top_halo.at[rows],
                    halo_ssem.at[number, 0], halo_rsem.at[number, 0], {"tile": right},
                ),
                remote(
                    up_send.at[rows], low_halo.at[rows],
                    halo_ssem.at[number, 1], halo_rsem.at[number, 1], {"tile": left},
                ),
            ]
        )
        for copy in halos[number]:
            copy.start()
    for load in loads[3:]:
        load.wait()
    each(lambda offset: oc_copy(offset).start())
    oc[me] = cells_ref[0]


    def inner(part):
        return lax.rem(lax.rem(part, 4) + 1, 4) >= 2

    def inner_send(low, offset):
        part = lax.rem(me + offset, PARTS)

        @pl.when(inner(part))
        def _():
            for chunk in range(CHUNKS):
                remote(
                    cell_send.at[part, chunk, pl.ds(low, half_count)],
                    cell_recv.at[chunk, me, pl.ds(low, half_count)],
                    cell_ssem.at[chunk, offset], cell_rsem.at[chunk, offset], {"mem": part},
                ).start()

    each(functools.partial(inner_send, 0))
    lax.fori_loop(half_count // 2, LOCAL // 2, inner_pair, 0)
    lax.fori_loop(0, PARTS // 2, functools.partial(inner_cells, half_count), 0)
    each(functools.partial(inner_send, half_count))

    def upper_cells(level, carry):
        to_cells(4 * level, 0, LOCAL, range(1, CHUNKS))
        return carry

    lax.fori_loop(0, LEVELS, upper_cells, 0)

    def upper_send(offset):
        first = lax.rem(lax.rem(me + offset, PARTS), 4) == 0
        pl.when(first)(lambda: cell_copy(1, offset).start())

    each(upper_send)

    each(lambda offset: oc_copy(offset).wait())
    within = lax.broadcasted_iota(jnp.int32, (HOT, NOBS), 0)

    def mark(part, carry):
        index = jnp.bitwise_and(oc[part], HOT - 1)
        hot[part] = jnp.where(within == index, 1.0, 0.0).astype(BF16)
        return carry

    lax.fori_loop(0, PARTS, mark, 0)

    top_mask = jnp.where(tile > 0, 1.0, 0.0).astype(F32)
    low_mask = jnp.where(tile < tiles - 1, 1.0, 0.0).astype(F32)
    for copy in halos[0]:
        copy.wait()
    extra = [
        [halo[0, 8 * block : 8 * block + 8, :] for block in range(3)]
        for halo in (top_halo, low_halo)
    ]
    for level in range(LEVELS):
        edge_dif[level] = windows(
            place(extra[0], 3 * level, 5), dif_ref[level, 0:8],
            dif_ref[level, ROWS - 8 : ROWS], place(extra[1], 3 * level, 0), 0,
        )
    coefficients(edge_coef, edge_dif, 16)
    edge_row = lax.broadcasted_iota(jnp.int32, (16, LANES), 0)
    edge_mask = jnp.where(edge_row < 2, top_mask, jnp.where(edge_row >= 14, low_mask, 1.0))

    edge_top = edge_row == 0
    edge_low = edge_row == 15
    rows = row_ids()

    def moved(tiles, source, target, count):
        first, last = source // 8, (source + count - 1) // 8
        shift = (target - source) % 8
        pieces = [
            pltpu.roll(tiles[n], shift, 0) if shift else tiles[n] for n in (first, last)[: 1 + (last > first)]
        ]
        if len(pieces) == 1:
            return pieces[0]
        return jnp.where(rows >= target + 8 * last - source, pieces[1], pieces[0])

    def edge_group(group, carry):
        members = range(4)
        states, wests, easts = {}, {}, {}
        for number in members:
            pair, half = 2 * group + number // 2, number % 2
            above = [top_halo[pair + 1, 8 * n : 8 * n + 8, :] for n in range(3)]
            below = [low_halo[pair + 1, 8 * n : 8 * n + 8, :] for n in range(3)]
            for level in range(LEVELS):
                at = 3 * (LEVELS * half + level)
                block = (2 * pair + half, level)
                upper, lower = ens[(*block, slice(0, 8))], ens[(*block, slice(ROWS - 8, ROWS))]
                top = jnp.where(
                    rows < 2, moved(above, at + 1, 0, 2) * top_mask, pltpu.roll(upper, 2, 0)
                )
                low = jnp.where(
                    rows < 6, pltpu.roll(lower, 6, 0), moved(below, at, 6, 2) * low_mask
                )
                state = jnp.concatenate([top, low], axis=0)
                first = moved(above, at, 0, 1) * top_mask
                last = moved(below, at + 2, 7, 1) * low_mask
                states[number, level] = state
                wests[number, level] = jnp.where(
                    edge_top, jnp.concatenate([first, low], axis=0), pltpu.roll(state, 1, 0)
                )
                easts[number, level] = jnp.where(
                    edge_low, jnp.concatenate([top, last], axis=0), pltpu.roll(state, 15, 0)
                )
        for repeat in range(SUB):
            updated = {}
            for number in members:
                own = [states[number, level] for level in range(LEVELS)]
                for level in range(LEVELS):
                    west = pltpu.roll(own[level], 1, 0) if repeat else wests[number, level]
                    east = pltpu.roll(own[level], 15, 0) if repeat else easts[number, level]
                    value = substep(edge_coef, level, own[level], west, east, column(own, level))
                    updated[number, level] = value * edge_mask if repeat < SUB - 1 else value
            states = updated
        for number in members:
            for level in range(LEVELS):
                first = level * ROWS * PITCH + 4 * group + number
                value = states[number, level]
                turn[pl.ds(first, 3, stride=PITCH), :] = value[2:5]
                turn[pl.ds(first + (ROWS - 3) * PITCH, 3, stride=PITCH), :] = value[11:14]
        return carry

    lax.fori_loop(0, LOCAL // 8, edge_group, 0)
    for copy in halos[1]:
        copy.wait()
    lax.fori_loop(LOCAL // 8, LOCAL // 4, edge_group, 0)

    def edge_cells(level, carry):
        to_cells(4 * level, 0, LOCAL, range(1))
        to_cells(4 * level + 3, 0, LOCAL)
        return carry

    lax.fori_loop(0, LEVELS, edge_cells, 0)

    def gather(number, carry):
        part = lax.rem(me + order(number), PARTS)
        group = jnp.broadcast_to(jnp.right_shift(oc[part], 8), (LOCAL, NOBS))
        pieces = []
        for step in (PARTS - 1, 0, 1):
            other = lax.rem(part + step, PARTS)
            for chunk in range(CHUNKS):
                for first in range(0, WIDE, HOT):
                    pieces.append(cell_send[other, chunk, :, first : first + HOT])
        found = jnp.dot(jnp.concatenate(pieces, axis=0), hot[part], preferred_element_type=F32)
        total = jnp.zeros((LOCAL, NOBS), F32)
        for piece in range(3 * CHUNKS * (WIDE // HOT)):
            total += jnp.where(
                group == piece, found[LOCAL * piece : LOCAL * piece + LOCAL], 0.0
            )
        pred_send[part] = total.astype(BF16)
        pl.when(number > 0)(lambda: pred_copy(order(number - 1)).start())
        return carry

    lax.fori_loop(0, PARTS, gather, 0)
    for chunk in range(CHUNKS):
        def edge_send(offset):
            part = lax.rem(me + offset, PARTS)
            wanted = lax.rem(part, 4) == 3 if chunk else jnp.logical_not(inner(part))
            pl.when(wanted)(lambda: cell_copy(chunk, offset).start())

        each(edge_send)
        cell_recv[chunk, me] = cell_send[me, chunk]
    pred_recv[me] = pred_send[me]

    each(lambda offset: pred_copy(offset).wait())
    weights, values = weights_ref[0], values_ref[0]
    total = jnp.zeros((1, NOBS), F32)
    for part in range(PARTS):
        total += jnp.sum(pred_recv[part].astype(F32), axis=0, keepdims=True)
    pmean = total * (1.0 / MEMBERS)
    pull = weights * (values - pmean)
    for part in range(PARTS):
        rows = slice(LOCAL * part, LOCAL * part + LOCAL)
        ppert = pred_recv[part].astype(F32) - pmean
        ymat[rows, :] = (ppert * weights).astype(BF16)
        zmat[rows, :] = ppert.astype(BF16)
        drive[rows, :] = jnp.sum(ppert * pull, axis=1, keepdims=True) * (1.0 / (MEMBERS - 1.0))
    gram = lax.dot_general(
        zmat[...], ymat[...], (((1,), (1,)), ((), ())), preferred_element_type=F32
    )
    eye = jnp.where(
        lax.broadcasted_iota(jnp.int32, (MEMBERS, MEMBERS), 0)
        == lax.broadcasted_iota(jnp.int32, (MEMBERS, MEMBERS), 1),
        1.0,
        0.0,
    )
    root[...] = gram * (1.0 / (MEMBERS - 1.0)) + eye
    small = jnp.where(
        lax.broadcasted_iota(jnp.int32, (LANES, LANES), 0)
        == lax.broadcasted_iota(jnp.int32, (LANES, LANES), 1),
        1.0,
        0.0,
    )
    trace = jnp.zeros((1, 1), F32)
    for block in range(MEMBERS // LANES):
        part = slice(LANES * block, LANES * block + LANES)
        diagonal = jnp.sum(root[part, part] * small, axis=1, keepdims=True)
        trace += jnp.sum(diagonal, axis=0, keepdims=True)
    scale = trace * (3.0 / MEMBERS)
    first = (root[...] * (1.0 / scale)).astype(BF16)
    ymat[...] = first
    mmat[...] = (1.5 * eye - 0.5 * first.astype(F32)).astype(BF16)
    zmat[...] = mmat[...]
    ymat[...] = jnp.dot(mmat[...], first, preferred_element_type=F32).astype(BF16)

    def newton(step, carry):
        product = jnp.dot(ymat[...], zmat[...], preferred_element_type=F32)
        mmat[...] = (1.5 * eye - 0.5 * product).astype(BF16)
        ynext = jnp.dot(mmat[...], ymat[...], preferred_element_type=F32).astype(BF16)
        znext = jnp.dot(zmat[...], mmat[...], preferred_element_type=F32).astype(BF16)
        ymat[...] = ynext
        zmat[...] = znext
        return carry

    lax.fori_loop(0, ITERS - 2, newton, 0)
    product = jnp.dot(ymat[...], zmat[...], preferred_element_type=F32)
    mmat[...] = (1.5 * eye - 0.5 * product).astype(BF16)
    root[...] = jnp.dot(zmat[...], mmat[...], preferred_element_type=F32) * (
        1.0 / jnp.sqrt(scale)
    )
    across = jnp.sum(root[...] * drive[...], axis=0, keepdims=True)
    wmean = jnp.zeros((1, MEMBERS), F32)
    for block in range(MEMBERS // LANES):
        part = slice(LANES * block, LANES * block + LANES)
        down = jnp.sum(across[:, part] * small, axis=1, keepdims=True)
        wmean += jnp.sum(root[part, :] * down, axis=0, keepdims=True)
    ymat[...] = (root[...] + wmean).astype(BF16)

    for chunk in range(CHUNKS):
        each(lambda offset: cell_copy(chunk, offset).wait())
        total = jnp.zeros((1, WIDE), F32)
        for part in range(PARTS):
            total += jnp.sum(cell_recv[chunk, part].astype(F32), axis=0, keepdims=True)
        xmean = total * (1.0 / MEMBERS)
        for part in range(PARTS):
            zmat[LOCAL * part : LOCAL * part + LOCAL, 0:WIDE] = (
                cell_recv[chunk, part].astype(F32) - xmean
            ).astype(BF16)
        update = jnp.dot(ymat[...], zmat[:, 0:WIDE], preferred_element_type=F32) + xmean
        for part in range(PARTS):
            back_send[chunk, part] = update[LOCAL * part : LOCAL * part + LOCAL].astype(BF16)
        each(lambda offset: back_copy(chunk, offset).start())
        back_recv[chunk, me] = back_send[chunk, me]

    for chunk in range(CHUNKS):
        each(lambda offset: back_copy(chunk, offset).wait())

        def from_cells(part, carry):
            for half in range(SPAN):
                first = pl.multiple_of((part * 8 + SPAN * chunk + half) * PITCH, 8)
                turn[pl.ds(first, LOCAL), :] = back_recv[
                    chunk, part, :, half * LANES : (half + 1) * LANES
                ].astype(F32)
            return carry

        lax.fori_loop(0, PARTS, from_cells, 0)

    def to_states(member, carry):
        for part in range(PARTS):
            out_ref[member, part // 4, (part % 4) * 8 : (part % 4) * 8 + 8, :] = turn[
                pl.ds(part * 8 * PITCH + member, 8, stride=PITCH), :
            ]
        return carry

    lax.fori_loop(0, LOCAL, to_states, 0)


def on_device(ensemble, diffusion, obs_cells, obs_values, obs_weights):
    vmem = pl.BlockSpec(memory_space=pltpu.VMEM)
    dma = pltpu.SemaphoreType.DMA
    halo = pltpu.VMEM((LOCAL // 2 + 1, 24, LANES), F32)
    square = pltpu.VMEM((MEMBERS, MEMBERS), BF16)
    return pl.pallas_call(
        kernel,
        name="cycle",
        out_shape=pltpu.VMEM(ensemble.shape, F32),
        in_specs=[pl.BlockSpec(memory_space=pl.ANY)] * 5,
        out_specs=vmem,
        scratch_shapes=[
            pltpu.VMEM(ensemble.shape, F32),
            pltpu.VMEM(diffusion.shape, F32),
            pltpu.VMEM(obs_cells.shape, jnp.int32),
            pltpu.VMEM(obs_values.shape, F32),
            pltpu.VMEM(obs_weights.shape, F32),
            halo, halo, halo, halo,
            pltpu.VMEM((5, LEVELS, ROWS, LANES), F32),
            pltpu.VMEM((5, LEVELS, 16, LANES), F32),
            pltpu.VMEM((LEVELS, 16, LANES), F32),
            pltpu.VMEM((LEVELS * ROWS * PITCH, LANES), F32),
            pltpu.VMEM((PARTS, 1, NOBS), jnp.int32),
            pltpu.VMEM((PARTS, HOT, NOBS), BF16),
            pltpu.VMEM((PARTS, CHUNKS, LOCAL, WIDE), BF16),
            pltpu.VMEM((CHUNKS, PARTS, LOCAL, WIDE), BF16),
            pltpu.VMEM((PARTS, LOCAL, NOBS), BF16),
            pltpu.VMEM((PARTS, LOCAL, NOBS), BF16),
            square, square, square,
            pltpu.VMEM((MEMBERS, MEMBERS), F32),
            pltpu.VMEM((MEMBERS, 1), F32),
            pltpu.VMEM((CHUNKS, PARTS, LOCAL, WIDE), BF16),
            pltpu.VMEM((CHUNKS, PARTS, LOCAL, WIDE), BF16),
            dma((6,)), dma((2, 2)), dma((2, 2)),
            dma((PARTS,)), dma((PARTS,)), dma((PARTS,)), dma((PARTS,)),
            dma((CHUNKS, PARTS)), dma((CHUNKS, PARTS)),
            dma((CHUNKS, PARTS)), dma((CHUNKS, PARTS)),
        ],
        compiler_params=pltpu.CompilerParams(
            collective_id=0, has_side_effects=True, vmem_limit_bytes=56 * 1024 * 1024
        ),
    )(ensemble, diffusion, obs_cells, obs_values, obs_weights)


def solution(mesh):
    return jax.shard_map(
        on_device,
        mesh=mesh,
        in_specs=(
            P("mem", None, "tile", None),
            P(None, "tile", None),
            P("tile", "mem", None),
            P("tile", "mem", None),
            P("tile", "mem", None),
        ),
        out_specs=P("mem", None, "tile", None),
        check_vma=False,
    )
```

```python
import functools

import jax
import jax.numpy as jnp
from jax import lax
from jax.experimental import pallas as pl
from jax.experimental.pallas import tpu as pltpu
from jax.sharding import PartitionSpec as P

ITERS = 6
SUB = 3
ADVECT = 0.3
VERTICAL = 0.1
PARTS = 16
LOCAL = 32
LEVELS = 4
ROWS = 32
LANES = 128
MEMBERS = 512
NOBS = 512
CHUNKS = 2
WIDE = 512
SPAN = WIDE // LANES
HOT = 256
PITCH = 40
MESH = pl.DeviceIdType.MESH
F32 = jnp.float32
BF16 = jnp.bfloat16


def row_ids():
    return lax.broadcasted_iota(jnp.int32, (8, LANES), 0)


def place(tiles, source, target):
    first, last = source // 8, (source + 2) // 8
    shift = (target - source) % 8
    out = pltpu.roll(tiles[first], shift, 0) if shift else tiles[first]
    if last != first:
        other = pltpu.roll(tiles[last], shift, 0) if shift else tiles[last]
        out = jnp.where(row_ids() >= target + 8 * last - source, other, out)
    return out


def pack(pieces, base):
    rows = row_ids()
    out = []
    for block in range(3):
        acc = jnp.zeros((8, LANES), F32)
        for number, piece in enumerate(pieces):
            low, high = 3 * number - 8 * block, 3 * number + 3 - 8 * block
            if high <= 0 or low >= 8:
                continue
            shift = (3 * number - base) % 8
            moved = pltpu.roll(piece, shift, 0) if shift else piece
            acc = jnp.where((rows >= low) & (rows < high), moved, acc)
        out.append(acc)
    return out


def windows(above, upper, lower, below, step):
    rows = row_ids()
    shift = 2 - step
    top = jnp.where(rows < shift, pltpu.roll(above, shift, 0), pltpu.roll(upper, shift, 0))
    shift = 6 - step
    low = jnp.where(rows < shift, pltpu.roll(lower, shift, 0), pltpu.roll(below, shift, 0))
    return jnp.concatenate([top, low], axis=0)


def coefficients(coef, dif_ref, rows):
    lane = lax.broadcasted_iota(jnp.int32, (rows, LANES), 1)
    for level in range(LEVELS):
        dif = dif_ref[level]
        coef[0, level] = 1.0 - ADVECT - 2.0 * VERTICAL - 4.0 * dif
        coef[1, level] = dif + ADVECT
        coef[2, level] = dif
        coef[3, level] = jnp.where(lane == 0, 0.0, dif)
        coef[4, level] = jnp.where(lane == LANES - 1, 0.0, dif)


def column(states, level):
    near = [states[n] for n in (level - 1, level + 1) if 0 <= n < LEVELS]
    return near[0] + near[1] if len(near) == 2 else near[0]


def substep(coef, level, state, west, east, vertical):
    return (
        coef[0, level] * state
        + coef[1, level] * west
        + coef[2, level] * east
        + coef[3, level] * pltpu.roll(state, 1, 1)
        + coef[4, level] * pltpu.roll(state, LANES - 1, 1)
        + VERTICAL * vertical
    )


def kernel(
    ens_hbm, dif_hbm, cells_hbm, values_hbm, weights_hbm, out_ref,
    ens, dif_ref, cells_ref, values_ref, weights_ref, up_send, down_send, top_halo, low_halo, coef, edge_coef, edge_dif, turn,
    oc, hot, cell_send, cell_recv, pred_send, pred_recv,
    ymat, zmat, mmat, root, drive, back_send, back_recv,
    load_sem, halo_ssem, halo_rsem, oc_ssem, oc_rsem, pred_ssem, pred_rsem,
    cell_ssem, cell_rsem, back_ssem, back_rsem,
):
    me = lax.axis_index("mem")
    tile = lax.axis_index("tile")
    tiles = lax.axis_size("tile")
    right, left = lax.rem(tile + 1, tiles), lax.rem(tile + tiles - 1, tiles)

    def order(number):
        half = lax.div(number + 1, 2)
        return jnp.where(lax.rem(number, 2) == 0, PARTS // 2 + half, PARTS // 2 - half)

    def each(action):
        def step(number, carry):
            action(order(number))
            return carry

        lax.fori_loop(0, PARTS - 1, step, 0)

    half_count = LOCAL // 2
    loads = [
        pltpu.make_async_copy(source, target, load_sem.at[number])
        for number, (source, target) in enumerate(
            [
                (dif_hbm, dif_ref),
                (ens_hbm.at[0:half_count], ens.at[0:half_count]),
                (ens_hbm.at[half_count:LOCAL], ens.at[half_count:LOCAL]),
                (cells_hbm, cells_ref),
                (values_hbm, values_ref),
                (weights_hbm, weights_ref),
            ]
        )
    ]
    for load in loads:
        load.start()
    barrier = pltpu.get_barrier_semaphore()
    each(
        lambda offset: pl.semaphore_signal(
            barrier, inc=1, device_id={"mem": lax.rem(me + offset, PARTS)}, device_id_type=MESH
        )
    )
    for other in (left, right):
        pl.semaphore_signal(barrier, inc=1, device_id={"tile": other}, device_id_type=MESH)
    loads[0].wait()
    coefficients(coef, dif_ref, ROWS)

    def inner_pair(pair, carry):
        for half in range(2):
            member = 2 * pair + half
            states = [ens[member, level] for level in range(LEVELS)]
            for repeat in range(SUB):
                states = [
                    substep(
                        coef, level, states[level],
                        pltpu.roll(states[level], 1, 0),
                        pltpu.roll(states[level], ROWS - 1, 0),
                        column(states, level),
                    )
                    for level in range(LEVELS)
                ]
            for level in range(LEVELS):
                for block in range(ROWS // 8):
                    first = (level * ROWS + 8 * block) * PITCH
                    turn[pl.ds(first + member, 8, stride=PITCH), :] = states[level][
                        8 * block : 8 * block + 8
                    ]
        return carry

    def to_cells(part, low, count):
        for chunk in range(CHUNKS):
            for half in range(SPAN):
                first = pl.multiple_of((part * 8 + SPAN * chunk + half) * PITCH + low, 8)
                cell_send[part, chunk, low : low + count, half * LANES : (half + 1) * LANES] = (
                    turn[pl.ds(first, count), :].astype(BF16)
                )

    def inner_cells(low, number, carry):
        to_cells(4 * (number // 2) + 1 + lax.rem(number, 2), low, half_count)
        return carry

    loads[1].wait()
    lax.fori_loop(0, half_count // 2, inner_pair, 0)
    lax.fori_loop(0, PARTS // 2, functools.partial(inner_cells, 0), 0)
    loads[2].wait()

    def pack_pair(pair, carry):
        tops, lows = [], []
        for half in range(2):
            for level in range(LEVELS):
                tops.append(ens[2 * pair + half, level, 0:8, :])
                lows.append(ens[2 * pair + half, level, ROWS - 8 : ROWS, :])
        for block, value in enumerate(pack(tops, 0)):
            up_send[pair + 1, 8 * block : 8 * block + 8, :] = value
        for block, value in enumerate(pack(lows, 5)):
            down_send[pair + 1, 8 * block : 8 * block + 8, :] = value
        return carry

    lax.fori_loop(0, LOCAL // 2, pack_pair, 0)
    tops = [dif_ref[level, 0:8, :] for level in range(LEVELS)]
    lows = [dif_ref[level, ROWS - 8 : ROWS, :] for level in range(LEVELS)]
    for block, value in enumerate(pack(tops, 0)):
        up_send[0, 8 * block : 8 * block + 8, :] = value
    for block, value in enumerate(pack(lows, 5)):
        down_send[0, 8 * block : 8 * block + 8, :] = value

    pl.semaphore_wait(barrier, PARTS + 1)

    def remote(source, target, ssem, rsem, device):
        return pltpu.make_async_remote_copy(
            src_ref=source, dst_ref=target, send_sem=ssem, recv_sem=rsem,
            device_id=device, device_id_type=MESH,
        )

    def oc_copy(offset):
        return remote(
            cells_ref.at[0], oc.at[me], oc_ssem.at[offset], oc_rsem.at[offset],
            {"mem": lax.rem(me + offset, PARTS)},
        )

    def pred_copy(offset):
        other = lax.rem(me + offset, PARTS)
        return remote(
            pred_send.at[other], pred_recv.at[me], pred_ssem.at[offset], pred_rsem.at[offset],
            {"mem": other},
        )

    def cell_copy(chunk, offset):
        other = lax.rem(me + offset, PARTS)
        return remote(
            cell_send.at[other, chunk], cell_recv.at[chunk, me],
            cell_ssem.at[chunk, offset], cell_rsem.at[chunk, offset], {"mem": other},
        )

    def back_copy(chunk, offset):
        other = lax.rem(me + offset, PARTS)
        return remote(
            back_send.at[chunk, other], back_recv.at[chunk, me],
            back_ssem.at[chunk, offset], back_rsem.at[chunk, offset], {"mem": other},
        )

    halos = []
    for number, rows in enumerate((pl.ds(0, LOCAL // 4 + 1), pl.ds(LOCAL // 4 + 1, LOCAL // 4))):
        halos.append(
            [
                remote(
                    down_send.at[rows], top_halo.at[rows],
                    halo_ssem.at[number, 0], halo_rsem.at[number, 0], {"tile": right},
                ),
                remote(
                    up_send.at[rows], low_halo.at[rows],
                    halo_ssem.at[number, 1], halo_rsem.at[number, 1], {"tile": left},
                ),
            ]
        )
        for copy in halos[number]:
            copy.start()
    for load in loads[3:]:
        load.wait()
    each(lambda offset: oc_copy(offset).start())
    oc[me] = cells_ref[0]


    def inner(part):
        return lax.rem(lax.rem(part, 4) + 1, 4) >= 2

    def inner_send(low, offset):
        part = lax.rem(me + offset, PARTS)

        @pl.when(inner(part))
        def _():
            for chunk in range(CHUNKS):
                remote(
                    cell_send.at[part, chunk, pl.ds(low, half_count)],
                    cell_recv.at[chunk, me, pl.ds(low, half_count)],
                    cell_ssem.at[chunk, offset], cell_rsem.at[chunk, offset], {"mem": part},
                ).start()

    each(functools.partial(inner_send, 0))
    lax.fori_loop(half_count // 2, LOCAL // 2, inner_pair, 0)
    lax.fori_loop(0, PARTS // 2, functools.partial(inner_cells, half_count), 0)
    each(functools.partial(inner_send, half_count))

    each(lambda offset: oc_copy(offset).wait())
    within = lax.broadcasted_iota(jnp.int32, (HOT, NOBS), 0)

    def mark(part, carry):
        index = jnp.bitwise_and(oc[part], HOT - 1)
        hot[part] = jnp.where(within == index, 1.0, 0.0).astype(BF16)
        return carry

    lax.fori_loop(0, PARTS, mark, 0)

    top_mask = jnp.where(tile > 0, 1.0, 0.0).astype(F32)
    low_mask = jnp.where(tile < tiles - 1, 1.0, 0.0).astype(F32)
    for copy in halos[0]:
        copy.wait()
    extra = [
        [halo[0, 8 * block : 8 * block + 8, :] for block in range(3)]
        for halo in (top_halo, low_halo)
    ]
    for level in range(LEVELS):
        edge_dif[level] = windows(
            place(extra[0], 3 * level, 5), dif_ref[level, 0:8],
            dif_ref[level, ROWS - 8 : ROWS], place(extra[1], 3 * level, 0), 0,
        )
    coefficients(edge_coef, edge_dif, 16)
    edge_row = lax.broadcasted_iota(jnp.int32, (16, LANES), 0)
    edge_mask = jnp.where(edge_row < 2, top_mask, jnp.where(edge_row >= 14, low_mask, 1.0))

    edge_top = edge_row == 0
    edge_low = edge_row == 15
    rows = row_ids()

    def moved(tiles, source, target, count):
        first, last = source // 8, (source + count - 1) // 8
        shift = (target - source) % 8
        pieces = [
            pltpu.roll(tiles[n], shift, 0) if shift else tiles[n] for n in (first, last)[: 1 + (last > first)]
        ]
        if len(pieces) == 1:
            return pieces[0]
        return jnp.where(rows >= target + 8 * last - source, pieces[1], pieces[0])

    def edge_group(group, carry):
        members = range(4)
        states, wests, easts = {}, {}, {}
        for number in members:
            pair, half = 2 * group + number // 2, number % 2
            above = [top_halo[pair + 1, 8 * n : 8 * n + 8, :] for n in range(3)]
            below = [low_halo[pair + 1, 8 * n : 8 * n + 8, :] for n in range(3)]
            for level in range(LEVELS):
                at = 3 * (LEVELS * half + level)
                block = (2 * pair + half, level)
                upper, lower = ens[(*block, slice(0, 8))], ens[(*block, slice(ROWS - 8, ROWS))]
                top = jnp.where(
                    rows < 2, moved(above, at + 1, 0, 2) * top_mask, pltpu.roll(upper, 2, 0)
                )
                low = jnp.where(
                    rows < 6, pltpu.roll(lower, 6, 0), moved(below, at, 6, 2) * low_mask
                )
                state = jnp.concatenate([top, low], axis=0)
                first = moved(above, at, 0, 1) * top_mask
                last = moved(below, at + 2, 7, 1) * low_mask
                states[number, level] = state
                wests[number, level] = jnp.where(
                    edge_top, jnp.concatenate([first, low], axis=0), pltpu.roll(state, 1, 0)
                )
                easts[number, level] = jnp.where(
                    edge_low, jnp.concatenate([top, last], axis=0), pltpu.roll(state, 15, 0)
                )
        for repeat in range(SUB):
            updated = {}
            for number in members:
                own = [states[number, level] for level in range(LEVELS)]
                for level in range(LEVELS):
                    west = pltpu.roll(own[level], 1, 0) if repeat else wests[number, level]
                    east = pltpu.roll(own[level], 15, 0) if repeat else easts[number, level]
                    value = substep(edge_coef, level, own[level], west, east, column(own, level))
                    updated[number, level] = value * edge_mask if repeat < SUB - 1 else value
            states = updated
        for number in members:
            for level in range(LEVELS):
                first = level * ROWS * PITCH + 4 * group + number
                value = states[number, level]
                turn[pl.ds(first, 3, stride=PITCH), :] = value[2:5]
                turn[pl.ds(first + (ROWS - 3) * PITCH, 3, stride=PITCH), :] = value[11:14]
        return carry

    lax.fori_loop(0, LOCAL // 8, edge_group, 0)
    for copy in halos[1]:
        copy.wait()
    lax.fori_loop(LOCAL // 8, LOCAL // 4, edge_group, 0)

    def edge_cells(number, carry):
        to_cells(4 * (number // 2) + 3 * lax.rem(number, 2), 0, LOCAL)
        return carry

    lax.fori_loop(0, PARTS // 2, edge_cells, 0)

    def gather(number, carry):
        part = lax.rem(me + order(number), PARTS)
        group = jnp.broadcast_to(jnp.right_shift(oc[part], 8), (LOCAL, NOBS))
        pieces = []
        for step in (PARTS - 1, 0, 1):
            other = lax.rem(part + step, PARTS)
            for chunk in range(CHUNKS):
                for first in range(0, WIDE, HOT):
                    pieces.append(cell_send[other, chunk, :, first : first + HOT])
        found = jnp.dot(jnp.concatenate(pieces, axis=0), hot[part], preferred_element_type=F32)
        total = jnp.zeros((LOCAL, NOBS), F32)
        for piece in range(3 * CHUNKS * (WIDE // HOT)):
            total += jnp.where(
                group == piece, found[LOCAL * piece : LOCAL * piece + LOCAL], 0.0
            )
        pred_send[part] = total.astype(BF16)
        pl.when(number > 0)(lambda: pred_copy(order(number - 1)).start())
        return carry

    lax.fori_loop(0, PARTS, gather, 0)
    for chunk in range(CHUNKS):
        def edge_send(offset):
            part = lax.rem(me + offset, PARTS)
            pl.when(jnp.logical_not(inner(part)))(lambda: cell_copy(chunk, offset).start())

        each(edge_send)
        cell_recv[chunk, me] = cell_send[me, chunk]
    pred_recv[me] = pred_send[me]

    each(lambda offset: pred_copy(offset).wait())
    weights, values = weights_ref[0], values_ref[0]
    total = jnp.zeros((1, NOBS), F32)
    for part in range(PARTS):
        total += jnp.sum(pred_recv[part].astype(F32), axis=0, keepdims=True)
    pmean = total * (1.0 / MEMBERS)
    pull = weights * (values - pmean)
    for part in range(PARTS):
        rows = slice(LOCAL * part, LOCAL * part + LOCAL)
        ppert = pred_recv[part].astype(F32) - pmean
        ymat[rows, :] = (ppert * weights).astype(BF16)
        zmat[rows, :] = ppert.astype(BF16)
        drive[rows, :] = jnp.sum(ppert * pull, axis=1, keepdims=True) * (1.0 / (MEMBERS - 1.0))
    gram = lax.dot_general(
        zmat[...], ymat[...], (((1,), (1,)), ((), ())), preferred_element_type=F32
    )
    eye = jnp.where(
        lax.broadcasted_iota(jnp.int32, (MEMBERS, MEMBERS), 0)
        == lax.broadcasted_iota(jnp.int32, (MEMBERS, MEMBERS), 1),
        1.0,
        0.0,
    )
    root[...] = gram * (1.0 / (MEMBERS - 1.0)) + eye
    small = jnp.where(
        lax.broadcasted_iota(jnp.int32, (LANES, LANES), 0)
        == lax.broadcasted_iota(jnp.int32, (LANES, LANES), 1),
        1.0,
        0.0,
    )
    trace = jnp.zeros((1, 1), F32)
    for block in range(MEMBERS // LANES):
        part = slice(LANES * block, LANES * block + LANES)
        diagonal = jnp.sum(root[part, part] * small, axis=1, keepdims=True)
        trace += jnp.sum(diagonal, axis=0, keepdims=True)
    scale = trace * (3.0 / MEMBERS)
    first = (root[...] * (1.0 / scale)).astype(BF16)
    ymat[...] = first
    mmat[...] = (1.5 * eye - 0.5 * first.astype(F32)).astype(BF16)
    zmat[...] = mmat[...]
    ymat[...] = jnp.dot(mmat[...], first, preferred_element_type=F32).astype(BF16)

    def newton(step, carry):
        product = jnp.dot(ymat[...], zmat[...], preferred_element_type=F32)
        mmat[...] = (1.5 * eye - 0.5 * product).astype(BF16)
        ynext = jnp.dot(mmat[...], ymat[...], preferred_element_type=F32).astype(BF16)
        znext = jnp.dot(zmat[...], mmat[...], preferred_element_type=F32).astype(BF16)
        ymat[...] = ynext
        zmat[...] = znext
        return carry

    lax.fori_loop(0, ITERS - 2, newton, 0)
    product = jnp.dot(ymat[...], zmat[...], preferred_element_type=F32)
    mmat[...] = (1.5 * eye - 0.5 * product).astype(BF16)
    root[...] = jnp.dot(zmat[...], mmat[...], preferred_element_type=F32) * (
        1.0 / jnp.sqrt(scale)
    )
    across = jnp.sum(root[...] * drive[...], axis=0, keepdims=True)
    wmean = jnp.zeros((1, MEMBERS), F32)
    for block in range(MEMBERS // LANES):
        part = slice(LANES * block, LANES * block + LANES)
        down = jnp.sum(across[:, part] * small, axis=1, keepdims=True)
        wmean += jnp.sum(root[part, :] * down, axis=0, keepdims=True)
    ymat[...] = (root[...] + wmean).astype(BF16)

    for chunk in range(CHUNKS):
        each(lambda offset: cell_copy(chunk, offset).wait())
        total = jnp.zeros((1, WIDE), F32)
        for part in range(PARTS):
            total += jnp.sum(cell_recv[chunk, part].astype(F32), axis=0, keepdims=True)
        xmean = total * (1.0 / MEMBERS)
        for part in range(PARTS):
            zmat[LOCAL * part : LOCAL * part + LOCAL, 0:WIDE] = (
                cell_recv[chunk, part].astype(F32) - xmean
            ).astype(BF16)
        update = jnp.dot(ymat[...], zmat[:, 0:WIDE], preferred_element_type=F32) + xmean
        for part in range(PARTS):
            back_send[chunk, part] = update[LOCAL * part : LOCAL * part + LOCAL].astype(BF16)
        each(lambda offset: back_copy(chunk, offset).start())
        back_recv[chunk, me] = back_send[chunk, me]

    for chunk in range(CHUNKS):
        each(lambda offset: back_copy(chunk, offset).wait())

        def from_cells(part, carry):
            for half in range(SPAN):
                first = pl.multiple_of((part * 8 + SPAN * chunk + half) * PITCH, 8)
                turn[pl.ds(first, LOCAL), :] = back_recv[
                    chunk, part, :, half * LANES : (half + 1) * LANES
                ].astype(F32)
            return carry

        lax.fori_loop(0, PARTS, from_cells, 0)

    def to_states(member, carry):
        for part in range(PARTS):
            out_ref[member, part // 4, (part % 4) * 8 : (part % 4) * 8 + 8, :] = turn[
                pl.ds(part * 8 * PITCH + member, 8, stride=PITCH), :
            ]
        return carry

    lax.fori_loop(0, LOCAL, to_states, 0)


def on_device(ensemble, diffusion, obs_cells, obs_values, obs_weights):
    vmem = pl.BlockSpec(memory_space=pltpu.VMEM)
    dma = pltpu.SemaphoreType.DMA
    halo = pltpu.VMEM((LOCAL // 2 + 1, 24, LANES), F32)
    square = pltpu.VMEM((MEMBERS, MEMBERS), BF16)
    return pl.pallas_call(
        kernel,
        name="cycle",
        out_shape=pltpu.VMEM(ensemble.shape, F32),
        in_specs=[pl.BlockSpec(memory_space=pl.ANY)] * 5,
        out_specs=vmem,
        scratch_shapes=[
            pltpu.VMEM(ensemble.shape, F32),
            pltpu.VMEM(diffusion.shape, F32),
            pltpu.VMEM(obs_cells.shape, jnp.int32),
            pltpu.VMEM(obs_values.shape, F32),
            pltpu.VMEM(obs_weights.shape, F32),
            halo, halo, halo, halo,
            pltpu.VMEM((5, LEVELS, ROWS, LANES), F32),
            pltpu.VMEM((5, LEVELS, 16, LANES), F32),
            pltpu.VMEM((LEVELS, 16, LANES), F32),
            pltpu.VMEM((LEVELS * ROWS * PITCH, LANES), F32),
            pltpu.VMEM((PARTS, 1, NOBS), jnp.int32),
            pltpu.VMEM((PARTS, HOT, NOBS), BF16),
            pltpu.VMEM((PARTS, CHUNKS, LOCAL, WIDE), BF16),
            pltpu.VMEM((CHUNKS, PARTS, LOCAL, WIDE), BF16),
            pltpu.VMEM((PARTS, LOCAL, NOBS), BF16),
            pltpu.VMEM((PARTS, LOCAL, NOBS), BF16),
            square, square, square,
            pltpu.VMEM((MEMBERS, MEMBERS), F32),
            pltpu.VMEM((MEMBERS, 1), F32),
            pltpu.VMEM((CHUNKS, PARTS, LOCAL, WIDE), BF16),
            pltpu.VMEM((CHUNKS, PARTS, LOCAL, WIDE), BF16),
            dma((6,)), dma((2, 2)), dma((2, 2)),
            dma((PARTS,)), dma((PARTS,)), dma((PARTS,)), dma((PARTS,)),
            dma((CHUNKS, PARTS)), dma((CHUNKS, PARTS)),
            dma((CHUNKS, PARTS)), dma((CHUNKS, PARTS)),
        ],
        compiler_params=pltpu.CompilerParams(
            collective_id=0, has_side_effects=True, vmem_limit_bytes=56 * 1024 * 1024
        ),
    )(ensemble, diffusion, obs_cells, obs_values, obs_weights)


def solution(mesh):
    return jax.shard_map(
        on_device,
        mesh=mesh,
        in_specs=(
            P("mem", None, "tile", None),
            P(None, "tile", None),
            P("tile", "mem", None),
            P("tile", "mem", None),
            P("tile", "mem", None),
        ),
        out_specs=P("mem", None, "tile", None),
        check_vma=False,
    )
```

```python
import functools

import jax
import jax.numpy as jnp
from jax import lax
from jax.experimental import pallas as pl
from jax.experimental.pallas import tpu as pltpu
from jax.sharding import PartitionSpec as P

ITERS = 6
SUB = 3
ADVECT = 0.3
VERTICAL = 0.1
PARTS = 16
LOCAL = 32
LEVELS = 4
ROWS = 32
LANES = 128
MEMBERS = 512
NOBS = 512
CHUNKS = 2
WIDE = 512
SPAN = WIDE // LANES
HOT = 256
PITCH = 40
MESH = pl.DeviceIdType.MESH
F32 = jnp.float32
BF16 = jnp.bfloat16


def row_ids():
    return lax.broadcasted_iota(jnp.int32, (8, LANES), 0)


def place(tiles, source, target):
    first, last = source // 8, (source + 2) // 8
    shift = (target - source) % 8
    out = pltpu.roll(tiles[first], shift, 0) if shift else tiles[first]
    if last != first:
        other = pltpu.roll(tiles[last], shift, 0) if shift else tiles[last]
        out = jnp.where(row_ids() >= target + 8 * last - source, other, out)
    return out


def pack(pieces, base):
    rows = row_ids()
    out = []
    for block in range(3):
        acc = jnp.zeros((8, LANES), F32)
        for number, piece in enumerate(pieces):
            low, high = 3 * number - 8 * block, 3 * number + 3 - 8 * block
            if high <= 0 or low >= 8:
                continue
            shift = (3 * number - base) % 8
            moved = pltpu.roll(piece, shift, 0) if shift else piece
            acc = jnp.where((rows >= low) & (rows < high), moved, acc)
        out.append(acc)
    return out


def windows(above, upper, lower, below, step):
    rows = row_ids()
    shift = 2 - step
    top = jnp.where(rows < shift, pltpu.roll(above, shift, 0), pltpu.roll(upper, shift, 0))
    shift = 6 - step
    low = jnp.where(rows < shift, pltpu.roll(lower, shift, 0), pltpu.roll(below, shift, 0))
    return jnp.concatenate([top, low], axis=0)


def coefficients(coef, dif_ref, rows):
    lane = lax.broadcasted_iota(jnp.int32, (rows, LANES), 1)
    for level in range(LEVELS):
        dif = dif_ref[level]
        coef[0, level] = 1.0 - ADVECT - 2.0 * VERTICAL - 4.0 * dif
        coef[1, level] = dif + ADVECT
        coef[2, level] = dif
        coef[3, level] = jnp.where(lane == 0, 0.0, dif)
        coef[4, level] = jnp.where(lane == LANES - 1, 0.0, dif)


def column(states, level):
    near = [states[n] for n in (level - 1, level + 1) if 0 <= n < LEVELS]
    return near[0] + near[1] if len(near) == 2 else near[0]


def substep(coef, level, state, west, east, vertical):
    return (
        coef[0, level] * state
        + coef[1, level] * west
        + coef[2, level] * east
        + coef[3, level] * pltpu.roll(state, 1, 1)
        + coef[4, level] * pltpu.roll(state, LANES - 1, 1)
        + VERTICAL * vertical
    )


def kernel(
    ens_hbm, dif_hbm, cells_hbm, values_hbm, weights_hbm, out_ref,
    ens, dif_ref, cells_ref, values_ref, weights_ref, up_send, down_send, top_halo, low_halo, coef, edge_coef, edge_dif, turn,
    oc, hot, cell_send, cell_recv, pred_send, pred_recv,
    ymat, zmat, mmat, root, drive, back_send, back_recv,
    load_sem, halo_ssem, halo_rsem, oc_ssem, oc_rsem, pred_ssem, pred_rsem,
    cell_ssem, cell_rsem, back_ssem, back_rsem,
):
    me = lax.axis_index("mem")
    tile = lax.axis_index("tile")
    tiles = lax.axis_size("tile")
    right, left = lax.rem(tile + 1, tiles), lax.rem(tile + tiles - 1, tiles)

    def order(number):
        half = lax.div(number + 1, 2)
        return jnp.where(lax.rem(number, 2) == 0, PARTS // 2 + half, PARTS // 2 - half)

    def each(action):
        def step(number, carry):
            action(order(number))
            return carry

        lax.fori_loop(0, PARTS - 1, step, 0)

    half_count = LOCAL // 2
    loads = [
        pltpu.make_async_copy(source, target, load_sem.at[number])
        for number, (source, target) in enumerate(
            [
                (dif_hbm, dif_ref),
                (ens_hbm.at[0:half_count], ens.at[0:half_count]),
                (ens_hbm.at[half_count:LOCAL], ens.at[half_count:LOCAL]),
                (cells_hbm, cells_ref),
                (values_hbm, values_ref),
                (weights_hbm, weights_ref),
            ]
        )
    ]
    for load in loads:
        load.start()
    barrier = pltpu.get_barrier_semaphore()
    each(
        lambda offset: pl.semaphore_signal(
            barrier, inc=1, device_id={"mem": lax.rem(me + offset, PARTS)}, device_id_type=MESH
        )
    )
    for other in (left, right):
        pl.semaphore_signal(barrier, inc=1, device_id={"tile": other}, device_id_type=MESH)
    loads[0].wait()
    coefficients(coef, dif_ref, ROWS)

    def inner_pair(pair, carry):
        for half in range(2):
            member = 2 * pair + half
            states = [ens[member, level] for level in range(LEVELS)]
            for repeat in range(SUB):
                states = [
                    substep(
                        coef, level, states[level],
                        pltpu.roll(states[level], 1, 0),
                        pltpu.roll(states[level], ROWS - 1, 0),
                        column(states, level),
                    )
                    for level in range(LEVELS)
                ]
            for level in range(LEVELS):
                for block in range(ROWS // 8):
                    first = (level * ROWS + 8 * block) * PITCH
                    turn[pl.ds(first + member, 8, stride=PITCH), :] = states[level][
                        8 * block : 8 * block + 8
                    ]
        return carry

    def to_cells(part, low, count):
        for chunk in range(CHUNKS):
            for half in range(SPAN):
                first = pl.multiple_of((part * 8 + SPAN * chunk + half) * PITCH + low, 8)
                cell_send[part, chunk, low : low + count, half * LANES : (half + 1) * LANES] = (
                    turn[pl.ds(first, count), :].astype(BF16)
                )

    def inner_cells(low, number, carry):
        to_cells(4 * (number // 2) + 1 + lax.rem(number, 2), low, half_count)
        return carry

    loads[1].wait()
    lax.fori_loop(0, half_count // 4, inner_pair, 0)
    loads[2].wait()

    def pack_pair(pair, carry):
        tops, lows = [], []
        for half in range(2):
            for level in range(LEVELS):
                tops.append(ens[2 * pair + half, level, 0:8, :])
                lows.append(ens[2 * pair + half, level, ROWS - 8 : ROWS, :])
        for block, value in enumerate(pack(tops, 0)):
            up_send[pair + 1, 8 * block : 8 * block + 8, :] = value
        for block, value in enumerate(pack(lows, 5)):
            down_send[pair + 1, 8 * block : 8 * block + 8, :] = value
        return carry

    lax.fori_loop(0, LOCAL // 2, pack_pair, 0)
    tops = [dif_ref[level, 0:8, :] for level in range(LEVELS)]
    lows = [dif_ref[level, ROWS - 8 : ROWS, :] for level in range(LEVELS)]
    for block, value in enumerate(pack(tops, 0)):
        up_send[0, 8 * block : 8 * block + 8, :] = value
    for block, value in enumerate(pack(lows, 5)):
        down_send[0, 8 * block : 8 * block + 8, :] = value

    pl.semaphore_wait(barrier, PARTS + 1)

    def remote(source, target, ssem, rsem, device):
        return pltpu.make_async_remote_copy(
            src_ref=source, dst_ref=target, send_sem=ssem, recv_sem=rsem,
            device_id=device, device_id_type=MESH,
        )

    def oc_copy(offset):
        return remote(
            cells_ref.at[0], oc.at[me], oc_ssem.at[offset], oc_rsem.at[offset],
            {"mem": lax.rem(me + offset, PARTS)},
        )

    def pred_copy(offset):
        other = lax.rem(me + offset, PARTS)
        return remote(
            pred_send.at[other], pred_recv.at[me], pred_ssem.at[offset], pred_rsem.at[offset],
            {"mem": other},
        )

    def cell_copy(chunk, offset):
        other = lax.rem(me + offset, PARTS)
        return remote(
            cell_send.at[other, chunk], cell_recv.at[chunk, me],
            cell_ssem.at[chunk, offset], cell_rsem.at[chunk, offset], {"mem": other},
        )

    def back_copy(chunk, offset):
        other = lax.rem(me + offset, PARTS)
        return remote(
            back_send.at[chunk, other], back_recv.at[chunk, me],
            back_ssem.at[chunk, offset], back_rsem.at[chunk, offset], {"mem": other},
        )

    halos = []
    for number in range(4):
        rows = pl.ds(4 * number + 1, 4) if number else pl.ds(0, 5)
        halos.append(
            [
                remote(
                    down_send.at[rows], top_halo.at[rows],
                    halo_ssem.at[number, 0], halo_rsem.at[number, 0], {"tile": right},
                ),
                remote(
                    up_send.at[rows], low_halo.at[rows],
                    halo_ssem.at[number, 1], halo_rsem.at[number, 1], {"tile": left},
                ),
            ]
        )
        for copy in halos[number]:
            copy.start()
    for load in loads[3:]:
        load.wait()
    each(lambda offset: oc_copy(offset).start())
    oc[me] = cells_ref[0]


    def inner(part):
        return lax.rem(lax.rem(part, 4) + 1, 4) >= 2

    def inner_send(low, offset):
        part = lax.rem(me + offset, PARTS)

        @pl.when(inner(part))
        def _():
            for chunk in range(CHUNKS):
                remote(
                    cell_send.at[part, chunk, pl.ds(low, half_count)],
                    cell_recv.at[chunk, me, pl.ds(low, half_count)],
                    cell_ssem.at[chunk, offset], cell_rsem.at[chunk, offset], {"mem": part},
                ).start()

    lax.fori_loop(half_count // 4, half_count // 2, inner_pair, 0)
    lax.fori_loop(0, PARTS // 2, functools.partial(inner_cells, 0), 0)
    each(functools.partial(inner_send, 0))
    lax.fori_loop(half_count // 2, LOCAL // 2, inner_pair, 0)
    lax.fori_loop(0, PARTS // 2, functools.partial(inner_cells, half_count), 0)
    each(functools.partial(inner_send, half_count))

    each(lambda offset: oc_copy(offset).wait())
    within = lax.broadcasted_iota(jnp.int32, (HOT, NOBS), 0)

    def mark(part, carry):
        index = jnp.bitwise_and(oc[part], HOT - 1)
        hot[part] = jnp.where(within == index, 1.0, 0.0).astype(BF16)
        return carry

    lax.fori_loop(0, PARTS, mark, 0)

    top_mask = jnp.where(tile > 0, 1.0, 0.0).astype(F32)
    low_mask = jnp.where(tile < tiles - 1, 1.0, 0.0).astype(F32)
    for copy in halos[0]:
        copy.wait()
    extra = [
        [halo[0, 8 * block : 8 * block + 8, :] for block in range(3)]
        for halo in (top_halo, low_halo)
    ]
    for level in range(LEVELS):
        edge_dif[level] = windows(
            place(extra[0], 3 * level, 5), dif_ref[level, 0:8],
            dif_ref[level, ROWS - 8 : ROWS], place(extra[1], 3 * level, 0), 0,
        )
    coefficients(edge_coef, edge_dif, 16)
    edge_row = lax.broadcasted_iota(jnp.int32, (16, LANES), 0)
    edge_mask = jnp.where(edge_row < 2, top_mask, jnp.where(edge_row >= 14, low_mask, 1.0))

    edge_top = edge_row == 0
    edge_low = edge_row == 15
    rows = row_ids()

    def moved(tiles, source, target, count):
        first, last = source // 8, (source + count - 1) // 8
        shift = (target - source) % 8
        pieces = [
            pltpu.roll(tiles[n], shift, 0) if shift else tiles[n] for n in (first, last)[: 1 + (last > first)]
        ]
        if len(pieces) == 1:
            return pieces[0]
        return jnp.where(rows >= target + 8 * last - source, pieces[1], pieces[0])

    def edge_group(group, carry):
        members = range(4)
        states, wests, easts = {}, {}, {}
        for number in members:
            pair, half = 2 * group + number // 2, number % 2
            above = [top_halo[pair + 1, 8 * n : 8 * n + 8, :] for n in range(3)]
            below = [low_halo[pair + 1, 8 * n : 8 * n + 8, :] for n in range(3)]
            for level in range(LEVELS):
                at = 3 * (LEVELS * half + level)
                block = (2 * pair + half, level)
                upper, lower = ens[(*block, slice(0, 8))], ens[(*block, slice(ROWS - 8, ROWS))]
                top = jnp.where(
                    rows < 2, moved(above, at + 1, 0, 2) * top_mask, pltpu.roll(upper, 2, 0)
                )
                low = jnp.where(
                    rows < 6, pltpu.roll(lower, 6, 0), moved(below, at, 6, 2) * low_mask
                )
                state = jnp.concatenate([top, low], axis=0)
                first = moved(above, at, 0, 1) * top_mask
                last = moved(below, at + 2, 7, 1) * low_mask
                states[number, level] = state
                wests[number, level] = jnp.where(
                    edge_top, jnp.concatenate([first, low], axis=0), pltpu.roll(state, 1, 0)
                )
                easts[number, level] = jnp.where(
                    edge_low, jnp.concatenate([top, last], axis=0), pltpu.roll(state, 15, 0)
                )
        for repeat in range(SUB):
            updated = {}
            for number in members:
                own = [states[number, level] for level in range(LEVELS)]
                for level in range(LEVELS):
                    west = pltpu.roll(own[level], 1, 0) if repeat else wests[number, level]
                    east = pltpu.roll(own[level], 15, 0) if repeat else easts[number, level]
                    value = substep(edge_coef, level, own[level], west, east, column(own, level))
                    updated[number, level] = value * edge_mask if repeat < SUB - 1 else value
            states = updated
        for number in members:
            for level in range(LEVELS):
                first = level * ROWS * PITCH + 4 * group + number
                value = states[number, level]
                turn[pl.ds(first, 3, stride=PITCH), :] = value[2:5]
                turn[pl.ds(first + (ROWS - 3) * PITCH, 3, stride=PITCH), :] = value[11:14]
        return carry

    for number in range(4):
        if number:
            for copy in halos[number]:
                copy.wait()
        lax.fori_loop(2 * number, 2 * number + 2, edge_group, 0)

    def edge_cells(number, carry):
        to_cells(4 * (number // 2) + 3 * lax.rem(number, 2), 0, LOCAL)
        return carry

    lax.fori_loop(0, PARTS // 2, edge_cells, 0)

    def gather(number, carry):
        part = lax.rem(me + order(number), PARTS)
        group = jnp.broadcast_to(jnp.right_shift(oc[part], 8), (LOCAL, NOBS))
        pieces = []
        for step in (PARTS - 1, 0, 1):
            other = lax.rem(part + step, PARTS)
            for chunk in range(CHUNKS):
                for first in range(0, WIDE, HOT):
                    pieces.append(cell_send[other, chunk, :, first : first + HOT])
        found = jnp.dot(jnp.concatenate(pieces, axis=0), hot[part], preferred_element_type=F32)
        total = jnp.zeros((LOCAL, NOBS), F32)
        for piece in range(3 * CHUNKS * (WIDE // HOT)):
            total += jnp.where(
                group == piece, found[LOCAL * piece : LOCAL * piece + LOCAL], 0.0
            )
        pred_send[part] = total.astype(BF16)
        pl.when(number > 0)(lambda: pred_copy(order(number - 1)).start())
        return carry

    lax.fori_loop(0, PARTS, gather, 0)
    for chunk in range(CHUNKS):
        def edge_send(offset):
            part = lax.rem(me + offset, PARTS)
            pl.when(jnp.logical_not(inner(part)))(lambda: cell_copy(chunk, offset).start())

        each(edge_send)
        cell_recv[chunk, me] = cell_send[me, chunk]
    pred_recv[me] = pred_send[me]

    each(lambda offset: pred_copy(offset).wait())
    weights, values = weights_ref[0], values_ref[0]
    total = jnp.zeros((1, NOBS), F32)
    for part in range(PARTS):
        total += jnp.sum(pred_recv[part].astype(F32), axis=0, keepdims=True)
    pmean = total * (1.0 / MEMBERS)
    pull = weights * (values - pmean)
    for part in range(PARTS):
        rows = slice(LOCAL * part, LOCAL * part + LOCAL)
        ppert = pred_recv[part].astype(F32) - pmean
        ymat[rows, :] = (ppert * weights).astype(BF16)
        zmat[rows, :] = ppert.astype(BF16)
        drive[rows, :] = jnp.sum(ppert * pull, axis=1, keepdims=True) * (1.0 / (MEMBERS - 1.0))
    gram = lax.dot_general(
        zmat[...], ymat[...], (((1,), (1,)), ((), ())), preferred_element_type=F32
    )
    eye = jnp.where(
        lax.broadcasted_iota(jnp.int32, (MEMBERS, MEMBERS), 0)
        == lax.broadcasted_iota(jnp.int32, (MEMBERS, MEMBERS), 1),
        1.0,
        0.0,
    )
    root[...] = gram * (1.0 / (MEMBERS - 1.0)) + eye
    small = jnp.where(
        lax.broadcasted_iota(jnp.int32, (LANES, LANES), 0)
        == lax.broadcasted_iota(jnp.int32, (LANES, LANES), 1),
        1.0,
        0.0,
    )
    trace = jnp.zeros((1, 1), F32)
    for block in range(MEMBERS // LANES):
        part = slice(LANES * block, LANES * block + LANES)
        diagonal = jnp.sum(root[part, part] * small, axis=1, keepdims=True)
        trace += jnp.sum(diagonal, axis=0, keepdims=True)
    scale = trace * (3.0 / MEMBERS)
    first = (root[...] * (1.0 / scale)).astype(BF16)
    ymat[...] = first
    mmat[...] = (1.5 * eye - 0.5 * first.astype(F32)).astype(BF16)
    zmat[...] = mmat[...]
    ymat[...] = jnp.dot(mmat[...], first, preferred_element_type=F32).astype(BF16)

    def newton(step, carry):
        product = jnp.dot(ymat[...], zmat[...], preferred_element_type=F32)
        mmat[...] = (1.5 * eye - 0.5 * product).astype(BF16)
        ynext = jnp.dot(mmat[...], ymat[...], preferred_element_type=F32).astype(BF16)
        znext = jnp.dot(zmat[...], mmat[...], preferred_element_type=F32).astype(BF16)
        ymat[...] = ynext
        zmat[...] = znext
        return carry

    lax.fori_loop(0, ITERS - 2, newton, 0)
    product = jnp.dot(ymat[...], zmat[...], preferred_element_type=F32)
    mmat[...] = (1.5 * eye - 0.5 * product).astype(BF16)
    root[...] = jnp.dot(zmat[...], mmat[...], preferred_element_type=F32) * (
        1.0 / jnp.sqrt(scale)
    )
    across = jnp.sum(root[...] * drive[...], axis=0, keepdims=True)
    wmean = jnp.zeros((1, MEMBERS), F32)
    for block in range(MEMBERS // LANES):
        part = slice(LANES * block, LANES * block + LANES)
        down = jnp.sum(across[:, part] * small, axis=1, keepdims=True)
        wmean += jnp.sum(root[part, :] * down, axis=0, keepdims=True)
    ymat[...] = (root[...] + wmean).astype(BF16)

    for chunk in range(CHUNKS):
        each(lambda offset: cell_copy(chunk, offset).wait())
        total = jnp.zeros((1, WIDE), F32)
        for part in range(PARTS):
            total += jnp.sum(cell_recv[chunk, part].astype(F32), axis=0, keepdims=True)
        xmean = total * (1.0 / MEMBERS)
        for part in range(PARTS):
            zmat[LOCAL * part : LOCAL * part + LOCAL, 0:WIDE] = (
                cell_recv[chunk, part].astype(F32) - xmean
            ).astype(BF16)
        update = jnp.dot(ymat[...], zmat[:, 0:WIDE], preferred_element_type=F32) + xmean
        for part in range(PARTS):
            back_send[chunk, part] = update[LOCAL * part : LOCAL * part + LOCAL].astype(BF16)
        each(lambda offset: back_copy(chunk, offset).start())
        back_recv[chunk, me] = back_send[chunk, me]

    for chunk in range(CHUNKS):
        each(lambda offset: back_copy(chunk, offset).wait())

        def from_cells(part, carry):
            for half in range(SPAN):
                first = pl.multiple_of((part * 8 + SPAN * chunk + half) * PITCH, 8)
                turn[pl.ds(first, LOCAL), :] = back_recv[
                    chunk, part, :, half * LANES : (half + 1) * LANES
                ].astype(F32)
            return carry

        lax.fori_loop(0, PARTS, from_cells, 0)

    def to_states(member, carry):
        for part in range(PARTS):
            out_ref[member, part // 4, (part % 4) * 8 : (part % 4) * 8 + 8, :] = turn[
                pl.ds(part * 8 * PITCH + member, 8, stride=PITCH), :
            ]
        return carry

    lax.fori_loop(0, LOCAL, to_states, 0)


def on_device(ensemble, diffusion, obs_cells, obs_values, obs_weights):
    vmem = pl.BlockSpec(memory_space=pltpu.VMEM)
    dma = pltpu.SemaphoreType.DMA
    halo = pltpu.VMEM((LOCAL // 2 + 1, 24, LANES), F32)
    square = pltpu.VMEM((MEMBERS, MEMBERS), BF16)
    return pl.pallas_call(
        kernel,
        name="cycle",
        out_shape=pltpu.VMEM(ensemble.shape, F32),
        in_specs=[pl.BlockSpec(memory_space=pl.ANY)] * 5,
        out_specs=vmem,
        scratch_shapes=[
            pltpu.VMEM(ensemble.shape, F32),
            pltpu.VMEM(diffusion.shape, F32),
            pltpu.VMEM(obs_cells.shape, jnp.int32),
            pltpu.VMEM(obs_values.shape, F32),
            pltpu.VMEM(obs_weights.shape, F32),
            halo, halo, halo, halo,
            pltpu.VMEM((5, LEVELS, ROWS, LANES), F32),
            pltpu.VMEM((5, LEVELS, 16, LANES), F32),
            pltpu.VMEM((LEVELS, 16, LANES), F32),
            pltpu.VMEM((LEVELS * ROWS * PITCH, LANES), F32),
            pltpu.VMEM((PARTS, 1, NOBS), jnp.int32),
            pltpu.VMEM((PARTS, HOT, NOBS), BF16),
            pltpu.VMEM((PARTS, CHUNKS, LOCAL, WIDE), BF16),
            pltpu.VMEM((CHUNKS, PARTS, LOCAL, WIDE), BF16),
            pltpu.VMEM((PARTS, LOCAL, NOBS), BF16),
            pltpu.VMEM((PARTS, LOCAL, NOBS), BF16),
            square, square, square,
            pltpu.VMEM((MEMBERS, MEMBERS), F32),
            pltpu.VMEM((MEMBERS, 1), F32),
            pltpu.VMEM((CHUNKS, PARTS, LOCAL, WIDE), BF16),
            pltpu.VMEM((CHUNKS, PARTS, LOCAL, WIDE), BF16),
            dma((6,)), dma((4, 2)), dma((4, 2)),
            dma((PARTS,)), dma((PARTS,)), dma((PARTS,)), dma((PARTS,)),
            dma((CHUNKS, PARTS)), dma((CHUNKS, PARTS)),
            dma((CHUNKS, PARTS)), dma((CHUNKS, PARTS)),
        ],
        compiler_params=pltpu.CompilerParams(
            collective_id=0, has_side_effects=True, vmem_limit_bytes=56 * 1024 * 1024
        ),
    )(ensemble, diffusion, obs_cells, obs_values, obs_weights)


def solution(mesh):
    return jax.shard_map(
        on_device,
        mesh=mesh,
        in_specs=(
            P("mem", None, "tile", None),
            P(None, "tile", None),
            P("tile", "mem", None),
            P("tile", "mem", None),
            P("tile", "mem", None),
        ),
        out_specs=P("mem", None, "tile", None),
        check_vma=False,
    )
```
